256 devices in a mesh: px: 32 (over x, y, core), py: 8 (over z).
Axes of the slice: x: 4, y: 4, z: 8, core: 2. Of those that a mesh axis runs over, the one named last changes fastest.
Arguments:
- cell_ids: int32 [32, 5120, 128], P('px', 'py'), may hold values from 0 to 32767, as said below
- offset_x: bfloat16 [32, 5120, 128], P('px', 'py'), may hold values from 0 to 1
- offset_y: bfloat16 [32, 5120, 128], P('px', 'py'), may hold values from 0 to 1
- mass: bfloat16 [32, 5120, 128], P('px', 'py'), may hold values from 0.25 to 4
- live: int32 [32, 5120, 128], P('px', 'py'), may hold values from 0 to 1, as said below
- tile_owner: int32 [32, 5120], P('px', 'py'), may hold values from 0 to 31, as said below
- counts: int32 [32, 8, 256], P('px', 'py'), may hold values from 0 to 7680, as said below
Outputs:
- spectrum: float32 [2, 8, 1024, 1024], P(None, None, ('px', 'py'))
- bucket_start: int32 [32, 8, 256], P('px', 'py')
The draws below stay inside these ranges and needn't reach their ends.
Inputs may be any that keep to these rules, and one draw needn't show every extreme that they name: A device's tiles stand in order of bucket, bucket = tile_owner * 8 + plane. One device has at most 60 tiles of one owner; in every draw, in each column of py, one owner has exactly 60 tiles on every device of that column. `cell_ids`: cell = (plane * 32 + row) * 128 + column, with row inside the owner's block of rows and column inside the device's block of columns; all slots of a tile, padded ones too, carry the tile's plane. In a tile the live particles come first; only the last tile of a bucket on a device has padded slots. counts[i, j, b] is the number of live particles in the tiles of bucket b on device (i, j); in every draw some bucket of every device holds 7680.
All inputs are finite; a program needn't handle non-finite values.
Results may differ from the reference program's by a relative error of at most 0.0003.
The reference program's roundings to bfloat16 on the way (of `weights`, `weight_x` and `weight_y`) count: a program that leaves them out, or rounds other values in their place, can miss the bound.
Values may be sent and summed in bfloat16 or wider, within the bound.
A program may use at most 128 MiB of HBM per device.

```python
import math
import jax
import jax.numpy as jnp
from jax import lax

NX = 1024
NY = 1024
PLANES = 8
TILE = 128
TILES_DEV = 640
RX = 32
RY = 128
CAP = 60
BUCKETS = 256
N_PX = 32
N_PY = 8


def tile_layout(key):
    base_key = jax.random.fold_in(key, 7001)
    key_hot, key_jitter, key_plane, key_fill = jax.random.split(base_key, 4)
    hot_owner = jax.random.randint(key_hot, (N_PY,), 0, N_PX)
    owner_ids = jnp.arange(N_PX, dtype=jnp.int32)
    is_hot = jnp.broadcast_to(owner_ids[None, None, :] == hot_owner[None, :, None], (N_PX, N_PY, N_PX))
    jitter = jax.random.randint(key_jitter, (N_PX, N_PY, N_PX), 1, 3)
    weights = jnp.where(is_hot, 0, (N_PX - 1 + 2 * owner_ids)[None, None, :] * jitter)
    remain = TILES_DEV - CAP
    shares = remain * weights // jnp.sum(weights, axis=-1, keepdims=True)
    leftover = remain - jnp.sum(shares, axis=-1, keepdims=True)
    order_rank = jnp.cumsum(jnp.where(is_hot, 0, 1), axis=-1) - 1
    shares = shares + jnp.where(jnp.logical_not(is_hot) & (order_rank < leftover), 1, 0)
    run_length = jnp.where(is_hot, CAP, shares)
    run_end = jnp.cumsum(run_length, axis=-1)
    tile_index = jnp.arange(TILES_DEV, dtype=jnp.int32)
    owner_of = jnp.sum((tile_index[None, None, :, None] >= run_end[:, :, None, :]).astype(jnp.int32), axis=-1)
    hot_of = jnp.broadcast_to(hot_owner[None, :, None], (N_PX, N_PY, TILES_DEV))
    tile_is_hot = owner_of == hot_of
    plane_draw = jax.random.randint(key_plane, (N_PX, N_PY, TILES_DEV), 0, PLANES)
    plane_draw = jnp.where(tile_is_hot, 0, plane_draw)
    sort_key = jnp.sort((owner_of * PLANES + plane_draw).astype(jnp.int32), axis=-1)
    closing = jnp.full((N_PX, N_PY, 1), -1, jnp.int32)
    is_last = sort_key != jnp.concatenate([sort_key[..., 1:], closing], axis=-1)
    sorted_hot = sort_key // PLANES == hot_of
    fill_count = jax.random.randint(key_fill, (N_PX, N_PY, TILES_DEV), 1, TILE + 1)
    live_count = jnp.where(is_last & jnp.logical_not(sorted_hot), fill_count, TILE)
    return (sort_key, live_count)


def bucket_tally(keys_row, live_row):
    return jax.ops.segment_sum(live_row, keys_row, num_segments=BUCKETS)


def draw_tile_owner(key, part):
    sort_key, live_count = tile_layout(key)
    return (sort_key // PLANES).reshape(N_PX, N_PY * TILES_DEV).astype(jnp.int32)


def draw_live(key, part):
    sort_key, live_count = tile_layout(key)
    slot_index = jnp.arange(TILE, dtype=jnp.int32)
    flags = (slot_index[None, None, None, :] < live_count[..., None]).astype(jnp.int32)
    return flags.reshape(N_PX, N_PY * TILES_DEV, TILE)


def draw_counts(key, part):
    sort_key, live_count = tile_layout(key)
    bucket_sums = jax.vmap(bucket_tally)(sort_key.reshape(-1, TILES_DEV), live_count.reshape(-1, TILES_DEV))
    return bucket_sums.reshape(N_PX, N_PY, BUCKETS).astype(jnp.int32)


def draw_cell_ids(key, part):
    sort_key, live_count = tile_layout(key)
    plane_ids = sort_key % PLANES
    key_x, key_y = jax.random.split(jax.random.fold_in(key, 7002))
    local_x = jax.random.randint(key_x, (N_PX, N_PY, TILES_DEV, TILE), 0, RX)
    local_y = jax.random.randint(key_y, (N_PX, N_PY, TILES_DEV, TILE), 0, RY)
    cells_all = (plane_ids[..., None] * RX + local_x) * RY + local_y
    return cells_all.reshape(N_PX, N_PY * TILES_DEV, TILE).astype(jnp.int32)


def steps_of(stream_key, shape, cuts, low, top_value):
    def one(dim, shards_of):
        steps = jax.random.uniform(jax.random.fold_in(jax.random.fold_in(stream_key, 6), dim), (shards_of,), jnp.float32, low / len(cuts), top_value / len(cuts))
        return jnp.repeat(jnp.exp(steps), shape[dim] // shards_of).reshape((-1,) + (1,) * (len(shape) - dim - 1))

    factor_of = one(*cuts[0])
    for cut in cuts[1:]:
        factor_of = factor_of * one(*cut)
    return factor_of


def setup_inputs(seed: int = 0) -> dict:
    keys = jax.random.split(jax.random.key(seed), 8)
    return {
        "cell_ids": draw_cell_ids(jax.random.fold_in(keys[7], 71), 0),
        "offset_x": jnp.clip(1.0 * jax.random.uniform(keys[1], (N_PX, N_PY * TILES_DEV, TILE), jnp.float32) ** steps_of(keys[1], (N_PX, N_PY * TILES_DEV, TILE), ((0, 32), (1, 8)), -0.2, 0.2), 0.0, 1.0).astype(jnp.bfloat16),
        "offset_y": jnp.clip(1.0 * jax.random.uniform(keys[2], (N_PX, N_PY * TILES_DEV, TILE), jnp.float32) ** steps_of(keys[2], (N_PX, N_PY * TILES_DEV, TILE), ((0, 32), (1, 8)), -0.2, 0.2), 0.0, 1.0).astype(jnp.bfloat16),
        "mass": jnp.clip(jnp.exp(math.log(4.0) - 2.7725887 * jax.random.uniform(keys[3], (N_PX, N_PY * TILES_DEV, TILE), jnp.float32) ** steps_of(keys[3], (N_PX, N_PY * TILES_DEV, TILE), ((0, 32), (1, 8)), -0.2, 0.2)), 0.25, 4.0).astype(jnp.bfloat16),
        "live": draw_live(jax.random.fold_in(keys[7], 71), 0),
        "tile_owner": draw_tile_owner(jax.random.fold_in(keys[7], 71), 0),
        "counts": draw_counts(jax.random.fold_in(keys[7], 71), 0),
    }


BETA = 18.4

def kernel(spread_at):
    return jnp.exp(BETA * (jnp.sqrt(1.0 - spread_at * spread_at) - 1.0))

def reference(cell_ids, offset_x, offset_y, mass, live, tile_owner, counts):
    tile_shape = (N_PX, N_PY, TILES_DEV, TILE)
    tile_cells = cell_ids.reshape(tile_shape)
    frac_x = offset_x.reshape(tile_shape).astype(jnp.float32)
    frac_y = offset_y.reshape(tile_shape).astype(jnp.float32)
    masses = jnp.where(live == 1, mass, jnp.zeros_like(mass)).reshape(tile_shape).astype(jnp.float32)
    owners = tile_owner.reshape(N_PX, N_PY, TILES_DEV)
    offset_steps = jnp.arange(-3, 5, dtype=jnp.int32)
    step_values = offset_steps.astype(jnp.float32)
    column_base = (jnp.arange(N_PY, dtype=jnp.int32) * RY)[:, None, None]

    def deposit_rows(density_flat, source_rows):
        row_cells, row_x, row_y, row_mass, row_owner = source_rows
        local_y = row_cells % RY
        local_x = row_cells // RY % RX
        plane_ids = row_cells // (RY * RX)
        global_x = row_owner[:, :, None] * RX + local_x
        global_y = column_base + local_y
        weight_x = kernel((step_values - row_x[..., None]) / 4.0).astype(jnp.bfloat16)
        weight_y = (kernel((step_values - row_y[..., None]) / 4.0) * row_mass[..., None]).astype(jnp.bfloat16)
        weight_x, weight_y = lax.optimization_barrier((weight_x, weight_y))
        values = weight_x.astype(jnp.float32)[..., :, None] * weight_y.astype(jnp.float32)[..., None, :]
        rows_at = (global_x[..., None] + offset_steps) % NX
        columns_at = (global_y[..., None] + offset_steps) % NY
        flat_index = (plane_ids[..., None, None] * NX + rows_at[..., :, None]) * NY + columns_at[..., None, :]
        return (density_flat.at[flat_index.reshape(-1)].add(values.reshape(-1)), None)
    initial = jnp.zeros((PLANES * NX * NY,), jnp.float32)
    density_flat = lax.scan(deposit_rows, initial, (tile_cells, frac_x, frac_y, masses, owners))[0]
    density = density_flat.reshape(PLANES, NX, NY)
    mean_density = jnp.sum(density) / (PLANES * NX * NY)
    contrast = density / mean_density - 1.0
    transform = jnp.fft.fft2(contrast, axes=(1, 2)) / math.sqrt(NX * NY)
    transform = jnp.transpose(transform, (0, 2, 1))
    spectrum = jnp.stack([jnp.real(transform), jnp.imag(transform)]).astype(jnp.float32)
    column_totals = lax.optimization_barrier(jnp.sum(counts, axis=0))
    preceding = jnp.cumsum(column_totals, axis=-1) - column_totals
    earlier = jnp.cumsum(counts, axis=0) - counts
    bucket_start = (preceding[None] + earlier).astype(jnp.int32)
    return (spectrum, bucket_start)
```

```python
import functools
import math

import jax
import jax.numpy as jnp
import numpy as np
from jax import lax
from jax.experimental import pallas as pl
from jax.experimental.pallas import tpu as pltpu
from jax.sharding import Mesh
from jax.sharding import PartitionSpec as P

NX = 1024
NY = 1024
PLANES = 8
BETA = 18.4
OWNERS = 32
RX = 32
TILE = 128
NT = (((1,), (1,)), ((), ()))


def tap_values(step, fraction):
    z = (step.astype(jnp.float32) - fraction) * 0.25
    return jnp.exp(BETA * (jnp.sqrt(1.0 - z * z) - 1.0))


def spread_kernel(
    bucket_ref, cell_ref, fx_ref, fy_ref, mass_ref, live_ref,
    main_ref, rim_ref, total_ref,
    grid_acc, rim_acc, lx_s, ly_s, fx_s, fy_s, w_s,
):
    tiles = cell_ref.shape[0]
    zero = jnp.zeros((8, TILE), jnp.float32)

    def clear(i, _):
        for p in range(PLANES):
            grid_acc[p, pl.ds(pl.multiple_of(i * 8, 8), 8), :] = zero
        return 0

    lax.fori_loop(0, grid_acc.shape[1] // 8, clear, 0)

    def clear_rim(i, _):
        for p in range(8):
            rim_acc[i * 8 + p] = zero
        return 0

    lax.fori_loop(0, OWNERS, clear_rim, 0)

    def prepare(i, _):
        rows = pl.ds(pl.multiple_of(i * 16, 16), 16)
        cell = cell_ref[rows, :]
        ly_s[rows, :] = cell & 127
        lx_s[rows, :] = (cell >> 7) & 31
        fx_s[rows, :] = fx_ref[rows, :].astype(jnp.float32)
        fy_s[rows, :] = fy_ref[rows, :].astype(jnp.float32)
        w_s[rows, :] = jnp.where(live_ref[rows, :] == 1, mass_ref[rows, :].astype(jnp.float32), 0.0)
        return 0

    lax.fori_loop(0, tiles // 16, prepare, 0)

    sub = lax.broadcasted_iota(jnp.int32, (8, TILE), 0)

    def row(ref, t):
        return jnp.broadcast_to(ref[pl.ds(t, 1), :], (8, TILE))

    def one_tile(t):
        lx, ly = row(lx_s, t), row(ly_s, t)
        jx = (sub - lx + 3) & 7
        jy = (sub - ly + 3) & 7
        tx = tap_values(jx - 3, row(fx_s, t))
        ty = tap_values(jy - 3, row(fy_s, t)) * row(w_s, t)
        gx = (lx + jx + 5) >> 3
        gy = (ly + jy - 3) >> 3
        gy = jnp.where(gy < 0, 16, gy)
        wx = jnp.concatenate([jnp.where(gx == g, tx, 0.0) for g in range(6)]).astype(jnp.bfloat16)
        wy = jnp.concatenate([jnp.where(gy == g, ty, 0.0) for g in range(16)]).astype(jnp.bfloat16)
        wr = jnp.concatenate([jnp.where(gy == 16, ty, 0.0), zero]).astype(jnp.bfloat16)
        main = lax.dot_general(wx, wy, NT, preferred_element_type=jnp.float32)
        rim = lax.dot_general(wr, wx, NT, preferred_element_type=jnp.float32)
        return main, rim[:8]

    unroll = 8

    def add_tiles(i, _):
        results = [one_tile(i * unroll + k) for k in range(unroll)]
        for k in range(unroll):
            bucket = bucket_ref[i * unroll + k]
            owner, plane = bucket >> 3, bucket & 7
            main, rim = results[k]
            rows = pl.ds(pl.multiple_of(owner * RX, RX), 48)
            grid_acc[plane, rows, :] = grid_acc[plane, rows, :] + main
            rim_acc[bucket, :, :48] = rim_acc[bucket, :, :48] + rim
        return 0

    lax.fori_loop(0, tiles // unroll, add_tiles, 0)

    for p in range(PLANES):
        grid_acc[p, 1024:1032, :] = grid_acc[p, 1024:1032, :] + grid_acc[p, 0:8, :]
        grid_acc[p, 8:16, :] = grid_acc[p, 8:16, :] + grid_acc[p, 1032:1040, :]

    lane = lax.broadcasted_iota(jnp.int32, (8, TILE), 1)

    def write_out(i, total):
        rows = pl.ds(pl.multiple_of(i * RX + 8, 8), RX)
        for p in range(PLANES):
            block = grid_acc[p, rows, :]
            main_ref[p, i // 2, i % 2] = block
            for k in range(RX // 8):
                total = total + block[8 * k : 8 * k + 8, :]
        before, after = (i + OWNERS - 1) % OWNERS, (i + 1) % OWNERS
        for q in range(2):
            out = zero
            for k in range(4):
                p = 4 * q + k
                own = pltpu.roll(rim_acc[i * 8 + p], (32 * k - 8) % 128, 1)
                low = pltpu.roll(rim_acc[before * 8 + p], (32 * k - 40) % 128, 1)
                high = pltpu.roll(rim_acc[after * 8 + p], (32 * k + 24) % 128, 1)
                spot = lane - 32 * k
                out = jnp.where((spot >= 0) & (spot < 32), own, out)
                out = out + jnp.where((spot >= 0) & (spot < 8), low, 0.0)
                out = out + jnp.where((spot >= 24) & (spot < 32), high, 0.0)
            rim_ref[q, i // 2, i % 2] = out
            total = total + out
        return total

    total_ref[...] = lax.fori_loop(0, OWNERS, write_out, zero)


def spread(buckets, cells, fx, fy, mass, live):
    tiles = cells.shape[0]
    vmem = pl.BlockSpec(memory_space=pltpu.VMEM)
    return pl.pallas_call(
        spread_kernel,
        out_shape=(
            jax.ShapeDtypeStruct((PLANES, 16, 2, RX, TILE), jnp.float32),
            jax.ShapeDtypeStruct((2, 16, 2, 8, TILE), jnp.float32),
            jax.ShapeDtypeStruct((8, TILE), jnp.float32),
        ),
        in_specs=[pl.BlockSpec(memory_space=pltpu.SMEM)] + [vmem] * 5,
        out_specs=(vmem, vmem, vmem),
        scratch_shapes=[
            pltpu.VMEM((PLANES, NX + 16, TILE), jnp.float32),
            pltpu.VMEM((OWNERS * PLANES, 8, TILE), jnp.float32),
            pltpu.VMEM((tiles, TILE), jnp.int32),
            pltpu.VMEM((tiles, TILE), jnp.int32),
            pltpu.VMEM((tiles, TILE), jnp.float32),
            pltpu.VMEM((tiles, TILE), jnp.float32),
            pltpu.VMEM((tiles, TILE), jnp.float32),
        ],
        name="spread",
    )(buckets, cells, fx, fy, mass, live)


COORDS = ("px_0", "px_1", "px_2")


def near(v):
    return v + 1 - 2 * (v % 2)


def far(v):
    return 3 - v


ROUTES = (("x", "near"), ("x", "far"), ("y", "near"), ("y", "far"))


def reduce_kernel(
    main_ref, rim_ref, total_ref, counts_ref,
    main_out, rim_out, total_out, start_out,
    main0, rim0, main1, rim1, main2, rim2, main3, rim3, main4, rim4,
    note, notes, note_send, note_recv, send, recv,
):
    x, y, c = (lax.axis_index(a) for a in COORDS)
    me = (x * 4 + y) * 2 + c
    barrier = pltpu.get_barrier_semaphore()

    def place(index):
        return {"px_0": index // 8, "px_1": index // 2 % 4, "px_2": index % 2}

    def greet(k, _):
        pl.semaphore_signal(
            barrier, inc=1, device_id=place((me + k) % OWNERS), device_id_type=pl.DeviceIdType.MESH
        )
        return 0

    lax.fori_loop(1, OWNERS, greet, 0)
    note[0:1, :] = counts_ref[0, :, 0:TILE].astype(jnp.float32)
    note[1:2, :] = counts_ref[0, :, TILE:].astype(jnp.float32)
    note[2:3, :] = jnp.sum(total_ref[...], axis=0, keepdims=True)
    note[3:8, :] = jnp.zeros((5, TILE), jnp.float32)
    notes[me] = note[...]
    pl.semaphore_wait(barrier, OWNERS - 1)

    def remote(src, dst, slot, where):
        copy = pltpu.make_async_remote_copy(
            src_ref=src, dst_ref=dst, send_sem=send.at[slot], recv_sem=recv.at[slot],
            device_id=where, device_id_type=pl.DeviceIdType.MESH,
        )
        copy.start()
        return copy

    chunks = []
    for k in range(10):
        if k < 8:
            refs = (main_ref.at[k], *(r.at[k] for r in (main0, main1, main2, main3, main4)), main_out.at[k])
        else:
            refs = (rim_ref.at[k - 8], *(r.at[k - 8] for r in (rim0, rim1, rim2, rim3, rim4)), rim_out.at[k - 8])
        chunks.append((*refs, k % 4 if k < 8 else 2 * (k - 8)))

    def leg(first, kind):
        v = x if first == "x" else y
        if kind == "near":
            low = (v + 1) // 2 % 2
            keep, give = (low, 3 - low), (1 - low, 2 + low)
            partner, other = near(v), far(v)
        else:
            low = 2 * (v // 2)
            keep, give = (low, low + 1), (2 - low, 3 - low)
            partner, other = far(v), near(v)
        axis = "px_0" if first == "x" else "px_1"
        return keep, give, {axis: partner}, other, {axis: other}

    pending = {}
    for k, (src, b0, *_) in enumerate(chunks):
        pending[k] = [remote(src.at[:, :, 1 - c], b0, 6 * k, {"px_2": 1 - c})]

    def tell(k, _):
        peer = (me + k) % OWNERS
        pltpu.make_async_remote_copy(
            src_ref=note, dst_ref=notes.at[me], send_sem=note_send.at[peer], recv_sem=note_recv.at[me],
            device_id=place(peer), device_id_type=pl.DeviceIdType.MESH,
        ).start()
        return 0

    lax.fori_loop(1, OWNERS, tell, 0)
    sent = []

    def arrive(k):
        for copy in pending[k]:
            copy.wait_recv()
        sent.extend(pending[k])

    for k, (src, b0, b1, b2, b3, b4, out, route) in enumerate(chunks):
        arrive(k)

        def add0(i, _, src=src, b0=b0):
            for j in range(4):
                b0[i, j] = b0[i, j] + src[i, j, c]
            return 0

        lax.fori_loop(0, 4, add0, 0)
        first, kind = ROUTES[route]
        _, give, where, _, _ = leg(first, kind)
        pending[k] = []
        for n in range(2):
            block = b0.at[give[n]] if first == "x" else b0.at[:, give[n]]
            pending[k].append(remote(block, b1.at[n], 6 * k + 1 + n, where))

    for k, (src, b0, b1, b2, b3, b4, out, route) in enumerate(chunks):
        arrive(k)
        first, kind = ROUTES[route]
        keep, _, _, other, where = leg(first, kind)
        for n in range(2):
            for j in range(4):
                at = (keep[n], j) if first == "x" else (j, keep[n])
                b0[at] = b0[at] + b1[n, j]
        block = b0.at[other] if first == "x" else b0.at[:, other]
        pending[k] = [remote(block, b2, 6 * k + 3, where)]

    for k, (src, b0, b1, b2, b3, b4, out, route) in enumerate(chunks):
        arrive(k)
        first, kind = ROUTES[route]
        for j in range(4):
            at = (x, j) if first == "x" else (j, y)
            b0[at] = b0[at] + b2[j]
        second = "y" if first == "x" else "x"
        _, give, where, _, _ = leg(second, kind)
        pending[k] = []
        for n in range(2):
            block = b0.at[x, give[n]] if first == "x" else b0.at[give[n], y]
            pending[k].append(remote(block, b3.at[n], 6 * k + 4 + n, where))

    last = 6 * len(chunks)
    for k, (src, b0, b1, b2, b3, b4, out, route) in enumerate(chunks):
        arrive(k)
        first, kind = ROUTES[route]
        second = "y" if first == "x" else "x"
        keep, _, _, other, where = leg(second, kind)
        for n in range(2):
            at = (x, keep[n]) if first == "x" else (keep[n], y)
            b0[at] = b0[at] + b3[n]
        block = b0.at[x, other] if first == "x" else b0.at[other, y]
        pending[k] = [remote(block, b4, last + k, where)]

    def heard(k, _):
        peer = (me + k) % OWNERS
        copy = pltpu.make_async_remote_copy(
            src_ref=note, dst_ref=notes.at[peer], send_sem=note_send.at[peer], recv_sem=note_recv.at[peer],
            device_id=place(peer), device_id_type=pl.DeviceIdType.MESH,
        )
        copy.wait_send()
        copy.wait_recv()
        return 0

    lax.fori_loop(1, OWNERS, heard, 0)
    everyone = jnp.zeros((8, TILE), jnp.float32)
    earlier = jnp.zeros((8, TILE), jnp.float32)
    for i in range(OWNERS):
        part = notes[i]
        everyone = everyone + part
        earlier = earlier + jnp.where(i < me, part, 0.0)
    lane = lax.broadcasted_iota(jnp.int32, (8, TILE), 1)
    running = everyone
    for shift in (1, 2, 4, 8, 16, 32, 64):
        running = running + jnp.where(lane >= shift, pltpu.roll(running, shift, 1), 0.0)
    begin = running - everyone + earlier
    whole = jnp.sum(everyone[0:1, :], axis=1, keepdims=True)
    start_out[0, :, 0:TILE] = begin[0:1, :].astype(jnp.int32)
    start_out[0, :, TILE:] = (begin[1:2, :] + whole).astype(jnp.int32)
    total_out[...] = jnp.broadcast_to(everyone[2:3, :], (8, TILE))

    for k, (src, b0, b1, b2, b3, b4, out, route) in enumerate(chunks):
        arrive(k)
        out[...] = b0[x, y] + b4[...]
    for copy in sent:
        copy.wait_send()


def reduce_rows(main, rim, total, counts):
    vmem = pl.BlockSpec(memory_space=pltpu.VMEM)
    f32 = jnp.float32

    def both(*lead):
        return [pltpu.VMEM((PLANES, *lead, RX, TILE), f32), pltpu.VMEM((2, *lead, 8, TILE), f32)]

    return pl.pallas_call(
        reduce_kernel,
        out_shape=(
            jax.ShapeDtypeStruct((PLANES, RX, TILE), f32),
            jax.ShapeDtypeStruct((2, 8, TILE), f32),
            jax.ShapeDtypeStruct((8, TILE), f32),
            jax.ShapeDtypeStruct((1, 1, 2 * TILE), jnp.int32),
        ),
        in_specs=[vmem] * 4,
        out_specs=(vmem,) * 4,
        scratch_shapes=[
            *both(4, 4), *both(2, 4), *both(4), *both(2), *both(),
            pltpu.VMEM((8, TILE), f32),
            pltpu.VMEM((OWNERS, 8, TILE), f32),
            pltpu.SemaphoreType.DMA((OWNERS,)),
            pltpu.SemaphoreType.DMA((OWNERS,)),
            pltpu.SemaphoreType.DMA((70,)),
            pltpu.SemaphoreType.DMA((70,)),
        ],
        compiler_params=pltpu.CompilerParams(collective_id=0, has_side_effects=True),
        name="reduce_rows",
    )(main, rim, total, counts)


PX = ("px_0", "px_1", "px_2")
PX_PY = ("px_0", "px_1", "px_2", "py")


def passed_along(value, axis, steps):
    count = lax.axis_size(axis)
    pairs = [(source, (source + steps) % count) for source in range(count)]
    return lax.ppermute(value, axis, pairs)


def in_blocks(value, dim, devices):
    before, after = (value.shape[:dim], value.shape[dim + 1 :])
    return jnp.moveaxis(value.reshape(*before, devices, -1, *after), dim, 0)


def laid_out(parts, dim):
    lengths = list(parts.shape[1:])
    lengths[dim] *= parts.shape[0]
    return jnp.moveaxis(parts, 0, dim).reshape(lengths)


def one_exchange(value, axis, axes, splits, concats):
    sizes = [lax.axis_size(a) for a in axes]
    parts = in_blocks(value, splits[0], sizes[0])
    parts = jnp.moveaxis(in_blocks(parts, splits[1] + 1, sizes[1]), 0, 1)
    inside = parts.shape[2:]
    parts = parts.reshape(-1, *inside)
    parts = lax.all_to_all(parts, axis, split_axis=0, concat_axis=0, tiled=True)
    parts = laid_out(parts.reshape(*sizes, *inside), concats[0] + 1)
    return laid_out(parts, concats[1])


def fold_columns(extended, col_count):
    core = extended[:, :, 4 : col_count + 4]
    for direction in (1, -1):
        if direction == 1:
            rim_cells = extended[:, :, col_count + 4 :]
        else:
            rim_cells = extended[:, :, :4]
        moved = passed_along(rim_cells, "py", direction)
        if direction == 1:
            core = core.at[:, :, :4].add(moved)
        else:
            core = core.at[:, :, col_count - 4 :].add(moved)
    return core


def project(data_block, table):
    return jnp.einsum("pqy,qk->pyk", data_block, table, precision=lax.Precision.HIGHEST)


def local(cell_ids, offset_x, offset_y, mass, live, tile_owner, counts):
    px_count = lax.axis_size(PX)
    py_count = lax.axis_size("py")
    row_count = NX // px_count
    col_count = NY // py_count
    tile_cells = cell_ids[0]
    buckets = tile_owner[0] * PLANES + tile_cells[:, 0] // 4096
    main, rim, total = spread(buckets, tile_cells, offset_x[0], offset_y[0], mass[0], live[0])
    main, rim, total, bucket_start = reduce_rows(
        main.reshape(PLANES, 4, 4, 2, row_count, col_count), rim.reshape(2, 4, 4, 2, 8, 128), total, counts
    )
    rim = rim.reshape(2, 8, 4, 32).transpose(0, 2, 3, 1).reshape(PLANES, row_count, 8)
    left = jnp.concatenate([jnp.zeros_like(rim[:, :, :5]), rim[:, :, 5:]], axis=2)[:, :, 4:]
    density = fold_columns(jnp.concatenate([left, main, rim[:, :, :4]], axis=2), col_count)
    grand_total = lax.psum(jnp.sum(total[0]), "py")
    contrast = density / (grand_total / (PLANES * NX * NY)) - 1.0
    by_rows = lax.all_to_all(contrast, "py", split_axis=1, concat_axis=2, tiled=True)
    part_rows = by_rows.shape[1]
    freq_y = jnp.arange(NY, dtype=jnp.int32)
    angle_y = 2.0 * math.pi / NY * (freq_y[:, None] * freq_y[None, :] % NY).astype(jnp.float32)
    flat_rows = by_rows.reshape(-1, NY)
    real_y = jnp.dot(flat_rows, jnp.cos(angle_y), precision=lax.Precision.HIGHEST).reshape(
        by_rows.shape
    )
    imag_y = -jnp.dot(flat_rows, jnp.sin(angle_y), precision=lax.Precision.HIGHEST).reshape(
        by_rows.shape
    )
    real_cols, imag_cols = (
        one_exchange(real_y, PX_PY, (PX, "py"), (2, 2), (1, 1)),
        one_exchange(imag_y, PX_PY, (PX, "py"), (2, 2), (1, 1)),
    )
    row_order = jnp.arange(NX, dtype=jnp.int32)
    within = row_order % part_rows
    from_px = row_order // part_rows % px_count
    from_py = row_order // (part_rows * px_count)
    true_x = from_px * row_count + from_py * part_rows + within
    angle_x = 2.0 * math.pi / NX * (true_x[:, None] * row_order[None, :] % NX).astype(jnp.float32)
    cos_x = jnp.cos(angle_x)
    sin_x = jnp.sin(angle_x)
    out_real = project(real_cols, cos_x) + project(imag_cols, sin_x)
    out_imag = project(imag_cols, cos_x) - project(real_cols, sin_x)
    spectrum = jnp.stack([out_real, out_imag]) * (1.0 / math.sqrt(NX * NY))
    return (spectrum, bucket_start)


def solution(mesh):
    torus = Mesh(mesh.devices.reshape(4, 4, 2, mesh.shape["py"]), ("px_0", "px_1", "px_2", "py"))
    return jax.shard_map(
        local,
        mesh=torus,
        in_specs=(
            P(PX, "py", None),
            P(PX, "py", None),
            P(PX, "py", None),
            P(PX, "py", None),
            P(PX, "py", None),
            P(PX, "py"),
            P(PX, "py", None),
        ),
        out_specs=(P(None, None, PX_PY, None), P(PX, "py", None)),
        check_vma=False,
    )
```

```python
import functools
import math

import jax
import jax.numpy as jnp
import numpy as np
from jax import lax
from jax.experimental import pallas as pl
from jax.experimental.pallas import tpu as pltpu
from jax.sharding import Mesh
from jax.sharding import PartitionSpec as P

NX = 1024
NY = 1024
PLANES = 8
BETA = 18.4
OWNERS = 32
RX = 32
TILE = 128
NT = (((1,), (1,)), ((), ()))


def tap_values(step, fraction):
    z = (step.astype(jnp.float32) - fraction) * 0.25
    return jnp.exp(BETA * (jnp.sqrt(1.0 - z * z) - 1.0))


def spread_kernel(
    bucket_ref, cell_ref, fx_ref, fy_ref, mass_ref, live_ref,
    main_ref, rim_ref, total_ref,
    grid_acc, rim_acc, lx_s, ly_s, fx_s, fy_s, w_s,
):
    tiles = cell_ref.shape[0]
    zero = jnp.zeros((8, TILE), jnp.float32)

    def clear(i, _):
        for p in range(PLANES):
            grid_acc[p, pl.ds(pl.multiple_of(i * 8, 8), 8), :] = zero
        return 0

    lax.fori_loop(0, grid_acc.shape[1] // 8, clear, 0)

    def clear_rim(i, _):
        for p in range(8):
            rim_acc[i * 8 + p] = zero
        return 0

    lax.fori_loop(0, OWNERS, clear_rim, 0)

    def prepare(i, _):
        rows = pl.ds(pl.multiple_of(i * 16, 16), 16)
        cell = cell_ref[rows, :]
        ly_s[rows, :] = cell & 127
        lx_s[rows, :] = (cell >> 7) & 31
        fx_s[rows, :] = fx_ref[rows, :].astype(jnp.float32)
        fy_s[rows, :] = fy_ref[rows, :].astype(jnp.float32)
        w_s[rows, :] = jnp.where(live_ref[rows, :] == 1, mass_ref[rows, :].astype(jnp.float32), 0.0)
        return 0

    lax.fori_loop(0, tiles // 16, prepare, 0)

    sub = lax.broadcasted_iota(jnp.int32, (8, TILE), 0)

    def row(ref, t):
        return jnp.broadcast_to(ref[pl.ds(t, 1), :], (8, TILE))

    def one_tile(t):
        lx, ly = row(lx_s, t), row(ly_s, t)
        jx = (sub - lx + 3) & 7
        jy = (sub - ly + 3) & 7
        tx = tap_values(jx - 3, row(fx_s, t))
        ty = tap_values(jy - 3, row(fy_s, t)) * row(w_s, t)
        gx = (lx + jx + 5) >> 3
        gy = (ly + jy - 3) >> 3
        gy = jnp.where(gy < 0, 16, gy)
        wx = jnp.concatenate([jnp.where(gx == g, tx, 0.0) for g in range(6)]).astype(jnp.bfloat16)
        wy = jnp.concatenate([jnp.where(gy == g, ty, 0.0) for g in range(16)]).astype(jnp.bfloat16)
        wr = jnp.concatenate([jnp.where(gy == 16, ty, 0.0), zero]).astype(jnp.bfloat16)
        main = lax.dot_general(wx, wy, NT, preferred_element_type=jnp.float32)
        rim = lax.dot_general(wr, wx, NT, preferred_element_type=jnp.float32)
        return main, rim[:8]

    unroll = 8

    def add_tiles(i, _):
        results = [one_tile(i * unroll + k) for k in range(unroll)]
        for k in range(unroll):
            bucket = bucket_ref[i * unroll + k]
            owner, plane = bucket >> 3, bucket & 7
            main, rim = results[k]
            rows = pl.ds(pl.multiple_of(owner * RX, RX), 48)
            grid_acc[plane, rows, :] = grid_acc[plane, rows, :] + main
            rim_acc[bucket, :, :48] = rim_acc[bucket, :, :48] + rim
        return 0

    lax.fori_loop(0, tiles // unroll, add_tiles, 0)

    for p in range(PLANES):
        grid_acc[p, 1024:1032, :] = grid_acc[p, 1024:1032, :] + grid_acc[p, 0:8, :]
        grid_acc[p, 8:16, :] = grid_acc[p, 8:16, :] + grid_acc[p, 1032:1040, :]

    lane = lax.broadcasted_iota(jnp.int32, (8, TILE), 1)

    def write_out(i, total):
        rows = pl.ds(pl.multiple_of(i * RX + 8, 8), RX)
        for p in range(PLANES):
            block = grid_acc[p, rows, :]
            main_ref[p, i // 2, i % 2] = block
            for k in range(RX // 8):
                total = total + block[8 * k : 8 * k + 8, :]
        before, after = (i + OWNERS - 1) % OWNERS, (i + 1) % OWNERS
        for q in range(2):
            out = zero
            for k in range(4):
                p = 4 * q + k
                own = pltpu.roll(rim_acc[i * 8 + p], (32 * k - 8) % 128, 1)
                low = pltpu.roll(rim_acc[before * 8 + p], (32 * k - 40) % 128, 1)
                high = pltpu.roll(rim_acc[after * 8 + p], (32 * k + 24) % 128, 1)
                spot = lane - 32 * k
                out = jnp.where((spot >= 0) & (spot < 32), own, out)
                out = out + jnp.where((spot >= 0) & (spot < 8), low, 0.0)
                out = out + jnp.where((spot >= 24) & (spot < 32), high, 0.0)
            rim_ref[q, i // 2, i % 2] = out
            total = total + out
        return total

    total_ref[...] = lax.fori_loop(0, OWNERS, write_out, zero)


def spread(buckets, cells, fx, fy, mass, live):
    tiles = cells.shape[0]
    vmem = pl.BlockSpec(memory_space=pltpu.VMEM)
    return pl.pallas_call(
        spread_kernel,
        out_shape=(
            jax.ShapeDtypeStruct((PLANES, 16, 2, RX, TILE), jnp.float32),
            jax.ShapeDtypeStruct((2, 16, 2, 8, TILE), jnp.float32),
            jax.ShapeDtypeStruct((8, TILE), jnp.float32),
        ),
        in_specs=[pl.BlockSpec(memory_space=pltpu.SMEM)] + [vmem] * 5,
        out_specs=(vmem, vmem, vmem),
        scratch_shapes=[
            pltpu.VMEM((PLANES, NX + 16, TILE), jnp.float32),
            pltpu.VMEM((OWNERS * PLANES, 8, TILE), jnp.float32),
            pltpu.VMEM((tiles, TILE), jnp.int32),
            pltpu.VMEM((tiles, TILE), jnp.int32),
            pltpu.VMEM((tiles, TILE), jnp.float32),
            pltpu.VMEM((tiles, TILE), jnp.float32),
            pltpu.VMEM((tiles, TILE), jnp.float32),
        ],
        name="spread",
    )(buckets, cells, fx, fy, mass, live)


COORDS = ("px_0", "px_1", "px_2")


def near(v):
    return v + 1 - 2 * (v % 2)


def far(v):
    return 3 - v


ROUTES = (("x", "near"), ("x", "far"), ("y", "near"), ("y", "far"))


def reduce_kernel(
    main_ref, rim_ref, total_ref, counts_ref,
    pack_out, start_out,
    main0, rim0, main1, rim1, main2, rim2, main3, rim3, main4, rim4,
    note, notes, note_send, note_recv, send, recv,
):
    x, y, c = (lax.axis_index(a) for a in COORDS)
    me = (x * 4 + y) * 2 + c
    barrier = pltpu.get_barrier_semaphore()

    def place(index):
        return {"px_0": index // 8, "px_1": index // 2 % 4, "px_2": index % 2}

    def greet(k, _):
        pl.semaphore_signal(
            barrier, inc=1, device_id=place((me + k) % OWNERS), device_id_type=pl.DeviceIdType.MESH
        )
        return 0

    lax.fori_loop(1, OWNERS, greet, 0)
    note[0:1, :] = counts_ref[0, :, 0:TILE].astype(jnp.float32)
    note[1:2, :] = counts_ref[0, :, TILE:].astype(jnp.float32)
    note[2:3, :] = jnp.sum(total_ref[...], axis=0, keepdims=True)
    note[3:8, :] = jnp.zeros((5, TILE), jnp.float32)
    notes[me] = note[...]
    pl.semaphore_wait(barrier, OWNERS - 1)

    def remote(src, dst, slot, where):
        copy = pltpu.make_async_remote_copy(
            src_ref=src, dst_ref=dst, send_sem=send.at[slot], recv_sem=recv.at[slot],
            device_id=where, device_id_type=pl.DeviceIdType.MESH,
        )
        copy.start()
        return copy

    chunks = []
    for k in range(10):
        if k < 8:
            refs = (main_ref.at[k], *(r.at[k] for r in (main0, main1, main2, main3, main4)), pack_out.at[k, 0:RX])
        else:
            refs = (rim_ref.at[k - 8], *(r.at[k - 8] for r in (rim0, rim1, rim2, rim3, rim4)), None)
        chunks.append((*refs, k % 4 if k < 8 else 2 * (k - 8)))

    def leg(first, kind):
        v = x if first == "x" else y
        if kind == "near":
            low = (v + 1) // 2 % 2
            keep, give = (low, 3 - low), (1 - low, 2 + low)
            partner, other = near(v), far(v)
        else:
            low = 2 * (v // 2)
            keep, give = (low, low + 1), (2 - low, 3 - low)
            partner, other = far(v), near(v)
        axis = "px_0" if first == "x" else "px_1"
        return keep, give, {axis: partner}, other, {axis: other}

    pending = {}
    for k, (src, b0, *_) in enumerate(chunks):
        pending[k] = [remote(src.at[:, :, 1 - c], b0, 6 * k, {"px_2": 1 - c})]

    def tell(k, _):
        peer = (me + k) % OWNERS
        pltpu.make_async_remote_copy(
            src_ref=note, dst_ref=notes.at[me], send_sem=note_send.at[peer], recv_sem=note_recv.at[me],
            device_id=place(peer), device_id_type=pl.DeviceIdType.MESH,
        ).start()
        return 0

    lax.fori_loop(1, OWNERS, tell, 0)
    sent = []

    def arrive(k):
        for copy in pending[k]:
            copy.wait_recv()
        sent.extend(pending[k])

    for k, (src, b0, b1, b2, b3, b4, out, route) in enumerate(chunks):
        arrive(k)

        def add0(i, _, src=src, b0=b0):
            for j in range(4):
                b0[i, j] = b0[i, j] + src[i, j, c]
            return 0

        lax.fori_loop(0, 4, add0, 0)
        first, kind = ROUTES[route]
        _, give, where, _, _ = leg(first, kind)
        pending[k] = []
        for n in range(2):
            block = b0.at[give[n]] if first == "x" else b0.at[:, give[n]]
            pending[k].append(remote(block, b1.at[n], 6 * k + 1 + n, where))

    for k, (src, b0, b1, b2, b3, b4, out, route) in enumerate(chunks):
        arrive(k)
        first, kind = ROUTES[route]
        keep, _, _, other, where = leg(first, kind)
        for n in range(2):
            for j in range(4):
                at = (keep[n], j) if first == "x" else (j, keep[n])
                b0[at] = b0[at] + b1[n, j]
        block = b0.at[other] if first == "x" else b0.at[:, other]
        pending[k] = [remote(block, b2, 6 * k + 3, where)]

    for k, (src, b0, b1, b2, b3, b4, out, route) in enumerate(chunks):
        arrive(k)
        first, kind = ROUTES[route]
        for j in range(4):
            at = (x, j) if first == "x" else (j, y)
            b0[at] = b0[at] + b2[j]
        second = "y" if first == "x" else "x"
        _, give, where, _, _ = leg(second, kind)
        pending[k] = []
        for n in range(2):
            block = b0.at[x, give[n]] if first == "x" else b0.at[give[n], y]
            pending[k].append(remote(block, b3.at[n], 6 * k + 4 + n, where))

    last = 6 * len(chunks)
    for k, (src, b0, b1, b2, b3, b4, out, route) in enumerate(chunks):
        arrive(k)
        first, kind = ROUTES[route]
        second = "y" if first == "x" else "x"
        keep, _, _, other, where = leg(second, kind)
        for n in range(2):
            at = (x, keep[n]) if first == "x" else (keep[n], y)
            b0[at] = b0[at] + b3[n]
        block = b0.at[x, other] if first == "x" else b0.at[other, y]
        pending[k] = [remote(block, b4, last + k, where)]

    def heard(k, _):
        peer = (me + k) % OWNERS
        copy = pltpu.make_async_remote_copy(
            src_ref=note, dst_ref=notes.at[peer], send_sem=note_send.at[peer], recv_sem=note_recv.at[peer],
            device_id=place(peer), device_id_type=pl.DeviceIdType.MESH,
        )
        copy.wait_send()
        copy.wait_recv()
        return 0

    lax.fori_loop(1, OWNERS, heard, 0)
    everyone = jnp.zeros((8, TILE), jnp.float32)
    earlier = jnp.zeros((8, TILE), jnp.float32)
    for i in range(OWNERS):
        part = notes[i]
        everyone = everyone + part
        earlier = earlier + jnp.where(i < me, part, 0.0)
    lane = lax.broadcasted_iota(jnp.int32, (8, TILE), 1)
    running = everyone
    for shift in (1, 2, 4, 8, 16, 32, 64):
        running = running + jnp.where(lane >= shift, pltpu.roll(running, shift, 1), 0.0)
    begin = running - everyone + earlier
    whole = jnp.sum(everyone[0:1, :], axis=1, keepdims=True)
    start_out[0, :, 0:TILE] = begin[0:1, :].astype(jnp.int32)
    start_out[0, :, TILE:] = (begin[1:2, :] + whole).astype(jnp.int32)
    for p in range(PLANES):
        pack_out[p, 40:48, :] = jnp.broadcast_to(everyone[2:3, :], (8, TILE))

    for k, (src, b0, b1, b2, b3, b4, out, route) in enumerate(chunks):
        arrive(k)
        block = b0[x, y] + b4[...]
        if k < 8:
            pack_out[k, 0:RX, :] = block
        else:
            for p in range(4):
                pack_out[4 * (k - 8) + p, RX : RX + 8, :] = block
    for copy in sent:
        copy.wait_send()


def reduce_rows(main, rim, total, counts):
    vmem = pl.BlockSpec(memory_space=pltpu.VMEM)
    f32 = jnp.float32

    def both(*lead):
        return [pltpu.VMEM((PLANES, *lead, RX, TILE), f32), pltpu.VMEM((2, *lead, 8, TILE), f32)]

    return pl.pallas_call(
        reduce_kernel,
        out_shape=(
            jax.ShapeDtypeStruct((PLANES, RX + 16, TILE), f32),
            jax.ShapeDtypeStruct((1, 1, 2 * TILE), jnp.int32),
        ),
        in_specs=[vmem] * 4,
        out_specs=(vmem, vmem),
        scratch_shapes=[
            *both(4, 4), *both(2, 4), *both(4), *both(2), *both(),
            pltpu.VMEM((8, TILE), f32),
            pltpu.VMEM((OWNERS, 8, TILE), f32),
            pltpu.SemaphoreType.DMA((OWNERS,)),
            pltpu.SemaphoreType.DMA((OWNERS,)),
            pltpu.SemaphoreType.DMA((70,)),
            pltpu.SemaphoreType.DMA((70,)),
        ],
        compiler_params=pltpu.CompilerParams(collective_id=0, has_side_effects=True),
        name="reduce_rows",
    )(main, rim, total, counts)


DEVICES = 256


def split_bf16(value):
    high = value.astype(jnp.bfloat16)
    return high, (value - high.astype(jnp.float32)).astype(jnp.bfloat16)


def np_split(value):
    high = np.asarray(value, np.float32).astype(jnp.bfloat16)
    low = (np.asarray(value, np.float64) - high.astype(np.float64)).astype(jnp.bfloat16)
    return high, low


def tables():
    k = np.arange(TILE)
    turn_y = 2 * np.pi / NY * (np.arange(8)[:, None] * k[None, :])
    twist_y = np.stack([np.cos(turn_y), -np.sin(turn_y)]).astype(np.float32)
    theta = 2 * np.pi / TILE * (k[:, None] * k[None, :] % TILE)
    wave_y = np.zeros((TILE, 2, 2, TILE))
    wave_y[:, 0, 0], wave_y[:, 0, 1] = np.cos(theta), np.sin(theta)
    wave_y[:, 1, 0], wave_y[:, 1, 1] = -np.sin(theta), np.cos(theta)
    y_high, y_low = np_split(wave_y.reshape(2 * TILE, 2 * TILE))
    phase = 2 * np.pi / OWNERS * (np.arange(OWNERS)[:, None] * k[None, :] % OWNERS)
    block = np.zeros((OWNERS, 2, 2, TILE))
    block[:, 0, 0], block[:, 1, 0] = np.cos(phase), np.sin(phase)
    block[:, 0, 1], block[:, 1, 1] = -np.sin(phase), np.cos(phase)
    wave_x = np.kron(np.eye(2), block.reshape(2 * OWNERS, 2 * TILE))
    x_high, x_low = np_split(wave_x)
    turn_x = 2 * np.pi / NX * (np.arange(RX)[:, None] * k[None, :])
    scale = 1.0 / math.sqrt(NX * NY)
    twist_x = (scale * np.stack([np.cos(turn_x), -np.sin(turn_x)])).astype(np.float32)
    return twist_y, y_high, y_low, np.concatenate([x_high, x_high]), x_low, twist_x


HALF = math.sqrt(0.5)


def real_eighths(d):
    s = [d[k] + d[k + 4] for k in range(4)]
    e = [d[k] - d[k + 4] for k in range(4)]
    near_sum, far_sum = s[0] + s[2], s[1] + s[3]
    a0, a4 = near_sum + far_sum, near_sum - far_sum
    re2, im2 = s[0] - s[2], s[3] - s[1]
    tilt, lean = (e[1] - e[3]) * HALF, (e[1] + e[3]) * HALF
    re1, im1 = e[0] + tilt, -e[2] - lean
    re3, im3 = e[0] - tilt, e[2] - lean
    zero = jnp.zeros_like(a0)
    return [(a0, zero), (re1, im1), (re2, im2), (re3, im3), (a4, zero), (re3, -im3), (re2, -im2), (re1, -im1)]


def fourths(t):
    def add(p, q):
        return p[0] + q[0], p[1] + q[1]

    def less(p, q):
        return p[0] - q[0], p[1] - q[1]

    e0, e1 = add(t[0], t[2]), less(t[0], t[2])
    f0, g = add(t[1], t[3]), less(t[1], t[3])
    f1 = (g[1], -g[0])
    return [add(e0, f0), add(e1, f1), less(e0, f0), less(e1, f1)]


def eighths(z):
    s = [(z[k][0] + z[k + 4][0], z[k][1] + z[k + 4][1]) for k in range(4)]
    d = [(z[k][0] - z[k + 4][0], z[k][1] - z[k + 4][1]) for k in range(4)]
    turned = [
        d[0],
        ((d[1][0] + d[1][1]) * HALF, (d[1][1] - d[1][0]) * HALF),
        (d[2][1], -d[2][0]),
        ((d[3][1] - d[3][0]) * HALF, -(d[3][0] + d[3][1]) * HALF),
    ]
    even, odd = fourths(s), fourths(turned)
    return [even[0], odd[0], even[1], odd[1], even[2], odd[2], even[3], odd[3]]


def fourier_kernel(
    pack_ref, twist_y, y_high, y_low, x_both, x_low, twist_x,
    out_ref,
    got, waves, columns, send, recv, wave_send, wave_recv,
):
    x, y, c = (lax.axis_index(a) for a in COORDS)
    j = lax.axis_index("py")
    i = (x * 4 + y) * 2 + c
    me = i * 8 + j
    barrier = pltpu.get_barrier_semaphore()

    def place(index):
        row = index // 8
        return {"px_0": row // 8, "px_1": row // 2 % 4, "px_2": row % 2, "py": index % 8}

    def greet(k, _):
        pl.semaphore_signal(
            barrier, inc=1, device_id=place((me + k) % DEVICES), device_id_type=pl.DeviceIdType.MESH
        )
        return 0

    lax.fori_loop(1, DEVICES, greet, 0)
    got[j] = pack_ref[j]
    pl.semaphore_wait(barrier, DEVICES - 1)

    moves = []
    for k in range(1, 8):
        peer = (j + k) % 8
        copy = pltpu.make_async_remote_copy(
            src_ref=pack_ref.at[peer], dst_ref=got.at[j], send_sem=send.at[k], recv_sem=recv.at[k],
            device_id={"py": peer}, device_id_type=pl.DeviceIdType.MESH,
        )
        copy.start()
        moves.append(copy)
    for copy in moves:
        copy.wait()

    lane = lax.broadcasted_iota(jnp.int32, (RX, TILE), 1)
    rims = jnp.concatenate([got[s, 32:40, :] for s in range(8)])
    rims = pltpu.roll(rims, (TILE - 32 * (j % 4)) % TILE, 1)
    rims = jnp.concatenate([rims, jnp.zeros((64, TILE), jnp.float32)])
    rims = jnp.transpose(rims)[:RX]
    amount = got[0, 40:41, :]
    for s in range(1, 8):
        amount = amount + got[s, 40:41, :]
    inverse = float(PLANES * NX * NY) / jnp.sum(amount, axis=1, keepdims=True)
    blocks = []
    for s in range(8):
        right = pltpu.roll(rims, (-8 * ((s + 7) % 8)) % TILE, 1)
        left = pltpu.roll(rims, (120 - 8 * ((s + 1) % 8)) % TILE, 1)
        value = got[s, 0:32, :] + jnp.where(lane < 4, right, 0.0) + jnp.where(lane >= 125, left, 0.0)
        blocks.append(value * inverse - 1.0)
    turned = []
    for k, (re, im) in enumerate(real_eighths(blocks)):
        tr, ti = twist_y[0, k : k + 1, :], twist_y[1, k : k + 1, :]
        turned.append(jnp.concatenate([re * tr - im * ti, re * ti + im * tr], axis=1))
    high, low = split_bf16(jnp.concatenate(turned))

    def times(a, b):
        return lax.dot_general(a, b, NT, preferred_element_type=jnp.float32)

    wave = times(y_high[...], low) + times(y_low[...], high) + times(y_high[...], high)
    for h in range(2):
        for k in range(TILE):
            waves[k, h] = wave[2 * k : 2 * k + 2, TILE * h : TILE * h + TILE]

    columns[j * 32 + i] = waves[me // 2, me % 2]

    def hand_out(k, _):
        peer = (me + k) % DEVICES
        pltpu.make_async_remote_copy(
            src_ref=waves.at[peer // 2, peer % 2], dst_ref=columns.at[j * 32 + i],
            send_sem=wave_send, recv_sem=wave_recv,
            device_id=place(peer), device_id_type=pl.DeviceIdType.MESH,
        ).start()
        return 0

    lax.fori_loop(1, DEVICES, hand_out, 0)
    others = columns.at[pl.ds(0, DEVICES - 1)]
    pltpu.make_async_copy(others, others, wave_recv).wait()

    for g in range(4):
        pair = columns[64 * g : 64 * g + 64].reshape(TILE, TILE)
        high, low = split_bf16(jnp.transpose(pair))
        both = jnp.concatenate([high, low], axis=1)
        sums = jnp.dot(both, x_both[...], preferred_element_type=jnp.float32)
        sums = sums + jnp.dot(high, x_low[...], preferred_element_type=jnp.float32)
        parts = [[], []]
        for p in range(2):
            for w in range(4):
                re_sum = im_sum = None
                for q in range(4):
                    rows = slice(32 * w + 8 * q, 32 * w + 8 * q + 8)
                    re = sums[rows, 256 * p : 256 * p + 128]
                    im = sums[rows, 256 * p + 128 : 256 * p + 256]
                    tr, ti = twist_x[0, 8 * q : 8 * q + 8, :], twist_x[1, 8 * q : 8 * q + 8, :]
                    re_part, im_part = re * tr - im * ti, re * ti + im * tr
                    re_sum = re_part if q == 0 else re_sum + re_part
                    im_sum = im_part if q == 0 else im_sum + im_part
                parts[0].append(re_sum)
                parts[1].append(im_sum)
        re, im = (jnp.transpose(jnp.stack(part), (1, 0, 2)) for part in parts)
        for a, value in enumerate(eighths([(re[k], im[k]) for k in range(8)])):
            for n in range(2):
                for p in range(2):
                    out_ref[n, 2 * g + p, :, TILE * a : TILE * a + TILE] = value[n][4 * p : 4 * p + 4]

    pltpu.make_async_copy(others, others, wave_send).wait()


def fourier(pack):
    vmem = pl.BlockSpec(memory_space=pltpu.VMEM)
    f32 = jnp.float32
    return pl.pallas_call(
        fourier_kernel,
        out_shape=jax.ShapeDtypeStruct((2, PLANES, 4, NX), f32),
        in_specs=[vmem] * 7,
        out_specs=vmem,
        scratch_shapes=[
            pltpu.VMEM((8, 48, TILE), f32),
            pltpu.VMEM((TILE, 2, 2, TILE), f32),
            pltpu.VMEM((DEVICES, 2, TILE), f32),
            pltpu.SemaphoreType.DMA((8,)),
            pltpu.SemaphoreType.DMA((8,)),
            pltpu.SemaphoreType.DMA,
            pltpu.SemaphoreType.DMA,
        ],
        compiler_params=pltpu.CompilerParams(collective_id=1, has_side_effects=True),
        name="fourier",
    )(pack, *tables())


PX = ("px_0", "px_1", "px_2")
PX_PY = ("px_0", "px_1", "px_2", "py")


def local(cell_ids, offset_x, offset_y, mass, live, tile_owner, counts):
    cells = cell_ids[0]
    buckets = tile_owner[0] * PLANES + cells[:, 0] // 4096
    main, rim, total = spread(buckets, cells, offset_x[0], offset_y[0], mass[0], live[0])
    pack, bucket_start = reduce_rows(
        main.reshape(PLANES, 4, 4, 2, RX, TILE), rim.reshape(2, 4, 4, 2, 8, TILE), total, counts
    )
    return fourier(pack), bucket_start


def solution(mesh):
    torus = Mesh(mesh.devices.reshape(4, 4, 2, mesh.shape["py"]), ("px_0", "px_1", "px_2", "py"))
    return jax.shard_map(
        local,
        mesh=torus,
        in_specs=(
            P(PX, "py", None),
            P(PX, "py", None),
            P(PX, "py", None),
            P(PX, "py", None),
            P(PX, "py", None),
            P(PX, "py"),
            P(PX, "py", None),
        ),
        out_specs=(P(None, None, PX_PY, None), P(PX, "py", None)),
        check_vma=False,
    )
```

```python
import functools
import math

import jax
import jax.numpy as jnp
import numpy as np
from jax import lax
from jax.experimental import pallas as pl
from jax.experimental.pallas import tpu as pltpu
from jax.sharding import Mesh
from jax.sharding import PartitionSpec as P

NX = 1024
NY = 1024
PLANES = 8
BETA = 18.4
OWNERS = 32
RX = 32
TILE = 128
NT = (((1,), (1,)), ((), ()))


def tap_values(step, fraction):
    z = (step.astype(jnp.float32) - fraction) * 0.25
    return jnp.exp(BETA * (jnp.sqrt(1.0 - z * z) - 1.0))


def spread_kernel(
    owner_ref, cell_ref, fx_ref, fy_ref, mass_ref, live_ref,
    main_ref, rim_ref, total_ref,
    grid_acc, rim_acc, lx_s, ly_s, fx_s, fy_s, w_s,
):
    tiles = cell_ref.shape[0]
    zero = jnp.zeros((8, TILE), jnp.float32)

    def clear(i, _):
        for p in range(PLANES):
            grid_acc[p, pl.ds(pl.multiple_of(i * 8, 8), 8), :] = zero
        return 0

    lax.fori_loop(0, grid_acc.shape[1] // 8, clear, 0)

    def clear_rim(i, _):
        for p in range(8):
            rim_acc[i * 8 + p] = zero
        return 0

    lax.fori_loop(0, OWNERS, clear_rim, 0)

    def prepare(i, _):
        rows = pl.ds(pl.multiple_of(i * 16, 16), 16)
        cell = cell_ref[rows, :]
        ly_s[rows, :] = cell & 127
        lx_s[rows, :] = (cell >> 7) & 31
        fx_s[rows, :] = fx_ref[rows, :].astype(jnp.float32)
        fy_s[rows, :] = fy_ref[rows, :].astype(jnp.float32)
        w_s[rows, :] = jnp.where(live_ref[rows, :] == 1, mass_ref[rows, :].astype(jnp.float32), 0.0)
        return 0

    lax.fori_loop(0, tiles // 16, prepare, 0)

    sub = lax.broadcasted_iota(jnp.int32, (8, TILE), 0)

    def row(ref, t):
        return jnp.broadcast_to(ref[pl.ds(t, 1), :], (8, TILE))

    def one_tile(t):
        lx, ly = row(lx_s, t), row(ly_s, t)
        jx = (sub - lx + 3) & 7
        jy = (sub - ly + 3) & 7
        tx = tap_values(jx - 3, row(fx_s, t))
        ty = tap_values(jy - 3, row(fy_s, t)) * row(w_s, t)
        gx = (lx + jx + 5) >> 3
        gy = (ly + jy - 3) >> 3
        gy = jnp.where(gy < 0, 16, gy)
        wx = jnp.concatenate([jnp.where(gx == g, tx, 0.0) for g in range(6)]).astype(jnp.bfloat16)
        wy = jnp.concatenate([jnp.where(gy == g, ty, 0.0) for g in range(16)]).astype(jnp.bfloat16)
        wr = jnp.concatenate([jnp.where(gy == 16, ty, 0.0), zero]).astype(jnp.bfloat16)
        main = lax.dot_general(wx, wy, NT, preferred_element_type=jnp.float32)
        rim = lax.dot_general(wr, wx, NT, preferred_element_type=jnp.float32)
        return main, rim[:8]

    unroll = 32

    def add_tiles(i, _):
        results = [one_tile(i * unroll + k) for k in range(unroll)]
        for k in range(unroll):
            owner = owner_ref[0, i * unroll + k]
            plane = cell_ref[pl.ds(i * unroll + k, 1), :][0, 0] >> 12
            bucket = owner * 8 + plane
            main, rim = results[k]
            rows = pl.ds(pl.multiple_of(owner * RX, RX), 48)
            grid_acc[plane, rows, :] = grid_acc[plane, rows, :] + main
            rim_acc[bucket, :, :48] = rim_acc[bucket, :, :48] + rim
        return 0

    lax.fori_loop(0, tiles // unroll, add_tiles, 0)

    for p in range(PLANES):
        grid_acc[p, 1024:1032, :] = grid_acc[p, 1024:1032, :] + grid_acc[p, 0:8, :]
        grid_acc[p, 8:16, :] = grid_acc[p, 8:16, :] + grid_acc[p, 1032:1040, :]

    lane = lax.broadcasted_iota(jnp.int32, (8, TILE), 1)

    def write_out(i, total):
        rows = pl.ds(pl.multiple_of(i * RX + 8, 8), RX)
        for p in range(PLANES):
            block = grid_acc[p, rows, :]
            main_ref[p, i // 2, i % 2] = block
            for k in range(RX // 8):
                total = total + block[8 * k : 8 * k + 8, :]
        before, after = (i + OWNERS - 1) % OWNERS, (i + 1) % OWNERS
        for q in range(2):
            out = zero
            for k in range(4):
                p = 4 * q + k
                own = pltpu.roll(rim_acc[i * 8 + p], (32 * k - 8) % 128, 1)
                low = pltpu.roll(rim_acc[before * 8 + p], (32 * k - 40) % 128, 1)
                high = pltpu.roll(rim_acc[after * 8 + p], (32 * k + 24) % 128, 1)
                spot = lane - 32 * k
                out = jnp.where((spot >= 0) & (spot < 32), own, out)
                out = out + jnp.where((spot >= 0) & (spot < 8), low, 0.0)
                out = out + jnp.where((spot >= 24) & (spot < 32), high, 0.0)
            rim_ref[q, i // 2, i % 2] = out
            total = total + out
        return total

    total_ref[...] = lax.fori_loop(0, OWNERS, write_out, zero)


def spread(owners, cells, fx, fy, mass, live):
    tiles = cells.shape[0]
    vmem = pl.BlockSpec(memory_space=pltpu.VMEM)
    return pl.pallas_call(
        spread_kernel,
        out_shape=(
            jax.ShapeDtypeStruct((PLANES, 16, 2, RX, TILE), jnp.float32),
            jax.ShapeDtypeStruct((2, 16, 2, 8, TILE), jnp.float32),
            jax.ShapeDtypeStruct((8, TILE), jnp.float32),
        ),
        in_specs=[pl.BlockSpec(memory_space=pltpu.SMEM)] + [vmem] * 5,
        out_specs=(vmem, vmem, vmem),
        scratch_shapes=[
            pltpu.VMEM((PLANES, NX + 16, TILE), jnp.float32),
            pltpu.VMEM((OWNERS * PLANES, 8, TILE), jnp.float32),
            pltpu.VMEM((tiles, TILE), jnp.int32),
            pltpu.VMEM((tiles, TILE), jnp.int32),
            pltpu.VMEM((tiles, TILE), jnp.float32),
            pltpu.VMEM((tiles, TILE), jnp.float32),
            pltpu.VMEM((tiles, TILE), jnp.float32),
        ],
        compiler_params=pltpu.CompilerParams(vmem_limit_bytes=24 << 20),
        name="spread",
    )(owners, cells, fx, fy, mass, live)


COORDS = ("px_0", "px_1", "px_2")
DEVICES = 256


def split_bf16(value):
    high = value.astype(jnp.bfloat16)
    return high, (value - high.astype(jnp.float32)).astype(jnp.bfloat16)


def np_split(value):
    high = np.asarray(value, np.float32).astype(jnp.bfloat16)
    low = (np.asarray(value, np.float64) - high.astype(np.float64)).astype(jnp.bfloat16)
    return high, low


def tables():
    k = np.arange(TILE)
    turn_y = 2 * np.pi / NY * (np.arange(8)[:, None] * k[None, :])
    twist_y = np.stack([np.cos(turn_y), -np.sin(turn_y)]).astype(np.float32)
    theta = 2 * np.pi / TILE * (k[:, None] * k[None, :] % TILE)
    wave_y = np.zeros((TILE, 2, 2, TILE))
    wave_y[:, 0, 0], wave_y[:, 0, 1] = np.cos(theta), np.sin(theta)
    wave_y[:, 1, 0], wave_y[:, 1, 1] = -np.sin(theta), np.cos(theta)
    y_high, y_low = np_split(wave_y.reshape(2 * TILE, 2 * TILE))
    phase = 2 * np.pi / OWNERS * (np.arange(OWNERS)[:, None] * k[None, :] % OWNERS)
    block = np.zeros((OWNERS, 2, 2, TILE))
    block[:, 0, 0], block[:, 1, 0] = np.cos(phase), np.sin(phase)
    block[:, 0, 1], block[:, 1, 1] = -np.sin(phase), np.cos(phase)
    wave_x = np.kron(np.eye(2), block.reshape(2 * OWNERS, 2 * TILE))
    x_high, x_low = np_split(wave_x)
    turn_x = 2 * np.pi / NX * (np.arange(RX)[:, None] * k[None, :])
    scale = 1.0 / math.sqrt(NX * NY)
    twist_x = (scale * np.stack([np.cos(turn_x), -np.sin(turn_x)])).astype(np.float32)
    return (twist_y, y_high, y_low), (np.concatenate([x_high, x_high]), x_low, twist_x)


HALF = math.sqrt(0.5)


def real_eighths(d):
    s = [d[k] + d[k + 4] for k in range(4)]
    e = [d[k] - d[k + 4] for k in range(4)]
    near_sum, far_sum = s[0] + s[2], s[1] + s[3]
    a0, a4 = near_sum + far_sum, near_sum - far_sum
    re2, im2 = s[0] - s[2], s[3] - s[1]
    tilt, lean = (e[1] - e[3]) * HALF, (e[1] + e[3]) * HALF
    re1, im1 = e[0] + tilt, -e[2] - lean
    re3, im3 = e[0] - tilt, e[2] - lean
    zero = jnp.zeros_like(a0)
    return [(a0, zero), (re1, im1), (re2, im2), (re3, im3), (a4, zero), (re3, -im3), (re2, -im2), (re1, -im1)]


def fourths(t):
    def add(p, q):
        return p[0] + q[0], p[1] + q[1]

    def less(p, q):
        return p[0] - q[0], p[1] - q[1]

    e0, e1 = add(t[0], t[2]), less(t[0], t[2])
    f0, g = add(t[1], t[3]), less(t[1], t[3])
    f1 = (g[1], -g[0])
    return [add(e0, f0), add(e1, f1), less(e0, f0), less(e1, f1)]


def eighths(z):
    s = [(z[k][0] + z[k + 4][0], z[k][1] + z[k + 4][1]) for k in range(4)]
    d = [(z[k][0] - z[k + 4][0], z[k][1] - z[k + 4][1]) for k in range(4)]
    turned = [
        d[0],
        ((d[1][0] + d[1][1]) * HALF, (d[1][1] - d[1][0]) * HALF),
        (d[2][1], -d[2][0]),
        ((d[3][1] - d[3][0]) * HALF, -(d[3][0] + d[3][1]) * HALF),
    ]
    even, odd = fourths(s), fourths(turned)
    return [even[0], odd[0], even[1], odd[1], even[2], odd[2], even[3], odd[3]]


def near(v):
    return v + 1 - 2 * lax.rem(v, 2)


def far(v):
    return 3 - v


ROUTES = (("x", "near"), ("x", "far"), ("y", "near"), ("y", "far"))
MESH = pl.DeviceIdType.MESH


def place(index):
    row = index // 8
    return {"px_0": row // 8, "px_1": lax.rem(row // 2, 4), "px_2": lax.rem(row, 2), "py": lax.rem(index, 8)}


def transform_kernel(
    main_ref, rim_ref, total_ref, counts_ref, twist_y, y_high, y_low,
    columns, begin_out,
    main0, rim0, main1, rim1, main2, rim2, main3, rim3, main4, rim4,
    note, notes, pack, got, waves,
    note_send, note_recv, send, recv, py_send, py_recv, wave_send, wave_recv,
):
    x, y, c = (lax.axis_index(a) for a in COORDS)
    j = lax.axis_index("py")
    i = (x * 4 + y) * 2 + c
    me = i * 8 + j
    barrier = pltpu.get_barrier_semaphore()

    def device(x, y, c):
        return ((x * 4 + y) * 2 + c) * 8 + j

    for k in range(1, OWNERS):
        pl.semaphore_signal(barrier, inc=1, device_id=place(lax.rem(me + 8 * k, DEVICES)), device_id_type=MESH)
    for k in range(1, 8):
        pl.semaphore_signal(barrier, inc=1, device_id=place(i * 8 + lax.rem(j + k, 8)), device_id_type=MESH)
    note[0:1, :] = counts_ref[0, :, 0:TILE].astype(jnp.float32)
    note[1:2, :] = counts_ref[0, :, TILE:].astype(jnp.float32)
    note[2:3, :] = jnp.sum(total_ref[...], axis=0, keepdims=True)
    note[3:8, :] = jnp.zeros((5, TILE), jnp.float32)
    notes[i] = note[...]
    pl.semaphore_wait(barrier, OWNERS - 1 + 7)

    def remote(src, dst, slot, where):
        copy = pltpu.make_async_remote_copy(
            src_ref=src, dst_ref=dst, send_sem=send.at[slot], recv_sem=recv.at[slot],
            device_id=place(where), device_id_type=MESH,
        )
        copy.start()
        return copy

    chunks = {}
    for k in (8, 9, *range(8)):
        if k < 8:
            refs = (main_ref.at[k], *(r.at[k] for r in (main0, main1, main2, main3, main4)))
        else:
            refs = (rim_ref.at[k - 8], *(r.at[k - 8] for r in (rim0, rim1, rim2, rim3, rim4)))
        chunks[k] = (*refs, k % 4 if k < 8 else 2 * (k - 8))

    def leg(first, kind):
        v = x if first == "x" else y
        if kind == "near":
            low = lax.rem((v + 1) // 2, 2)
            keep, give = (low, 3 - low), (1 - low, 2 + low)
            partner, other = near(v), far(v)
        else:
            low = 2 * (v // 2)
            keep, give = (low, low + 1), (2 - low, 3 - low)
            partner, other = far(v), near(v)
        if first == "x":
            return keep, give, device(partner, y, c), other, device(other, y, c)
        return keep, give, device(x, partner, c), other, device(x, other, c)

    pending = {}
    for k, (src, b0, *_) in chunks.items():
        pending[k] = [remote(src.at[:, :, 1 - c], b0, 7 * k, device(x, y, 1 - c))]

    def note_copy(k):
        peer = lax.rem(i + k, OWNERS)
        return pltpu.make_async_remote_copy(
            src_ref=note, dst_ref=notes.at[i], send_sem=note_send.at[peer], recv_sem=note_recv.at[i],
            device_id=place(peer * 8 + j), device_id_type=MESH,
        )

    for k in range(1, OWNERS):
        note_copy(k).start()
    sent = []

    def arrive(k):
        for copy in pending[k]:
            copy.wait_recv()
        sent.extend(pending[k])

    for k, (src, b0, b1, b2, b3, b4, route) in chunks.items():
        arrive(k)

        def add0(n, _, src=src, b0=b0):
            for m in range(4):
                b0[n, m] = b0[n, m] + src[n, m, c]
            return 0

        lax.fori_loop(0, 4, add0, 0)
        first, kind = ROUTES[route]
        _, give, where, _, _ = leg(first, kind)
        pending[k] = []
        for n in range(2):
            block = b0.at[give[n]] if first == "x" else b0.at[:, give[n]]
            pending[k].append(remote(block, b1.at[n], 7 * k + 1 + n, where))

    for k, (src, b0, b1, b2, b3, b4, route) in chunks.items():
        arrive(k)
        first, kind = ROUTES[route]
        keep, _, _, other, where = leg(first, kind)
        for n in range(2):
            for m in range(4):
                at = (keep[n], m) if first == "x" else (m, keep[n])
                b0[at] = b0[at] + b1[n, m]
        block = b0.at[other] if first == "x" else b0.at[:, other]
        pending[k] = [remote(block, b2, 7 * k + 3, where)]

    for k, (src, b0, b1, b2, b3, b4, route) in chunks.items():
        arrive(k)
        first, kind = ROUTES[route]
        for m in range(4):
            at = (x, m) if first == "x" else (m, y)
            b0[at] = b0[at] + b2[m]
        second = "y" if first == "x" else "x"
        _, give, where, _, _ = leg(second, kind)
        pending[k] = []
        for n in range(2):
            block = b0.at[x, give[n]] if first == "x" else b0.at[give[n], y]
            pending[k].append(remote(block, b3.at[n], 7 * k + 4 + n, where))

    for k, (src, b0, b1, b2, b3, b4, route) in chunks.items():
        arrive(k)
        first, kind = ROUTES[route]
        second = "y" if first == "x" else "x"
        keep, _, _, other, where = leg(second, kind)
        for n in range(2):
            at = (x, keep[n]) if first == "x" else (keep[n], y)
            b0[at] = b0[at] + b3[n]
        block = b0.at[x, other] if first == "x" else b0.at[other, y]
        pending[k] = [remote(block, b4, 7 * k + 6, where)]

    for k in range(1, OWNERS):
        peer = lax.rem(i + k, OWNERS)
        copy = pltpu.make_async_remote_copy(
            src_ref=note, dst_ref=notes.at[peer], send_sem=note_send.at[peer], recv_sem=note_recv.at[peer],
            device_id=place(peer * 8 + j), device_id_type=MESH,
        )
        copy.wait_send()
        copy.wait_recv()
    everyone = notes[0]
    for k in range(1, OWNERS):
        everyone = everyone + notes[k]
    amount = jnp.broadcast_to(everyone[2:3, :], (8, TILE))

    def plane_copy(k, source):
        return pltpu.make_async_remote_copy(
            src_ref=pack.at[k], dst_ref=got.at[source], send_sem=py_send.at[k], recv_sem=py_recv.at[source],
            device_id=place(i * 8 + k), device_id_type=MESH,
        )

    for k, (src, b0, b1, b2, b3, b4, route) in chunks.items():
        arrive(k)
        block = b0[x, y] + b4[...]
        if k >= 8:
            for p in range(4):
                pack[4 * (k - 8) + p, RX : RX + 8, :] = block
                pack[4 * (k - 8) + p, RX + 8 :, :] = amount
            continue
        pack[k, 0:RX, :] = block

        @pl.when(k != j)
        def _():
            plane_copy(k, j).start()

        @pl.when(k == j)
        def _():
            got[k] = pack[k]

    earlier = jnp.zeros((8, TILE), jnp.float32)
    for k in range(OWNERS):
        earlier = earlier + jnp.where(k < i, notes[k], 0.0)
    spot = lax.broadcasted_iota(jnp.int32, (8, TILE), 1)
    running = everyone
    for shift in (1, 2, 4, 8, 16, 32, 64):
        running = running + jnp.where(spot >= shift, pltpu.roll(running, shift, 1), 0.0)
    begin = running - everyone + earlier
    whole = jnp.sum(everyone[0:1, :], axis=1, keepdims=True)
    begin_out[0:1, :] = begin[0:1, :]
    begin_out[1:2, :] = begin[1:2, :] + whole
    begin_out[2:8, :] = jnp.zeros((6, TILE), jnp.float32)

    for k in range(1, 8):
        peer = lax.rem(j + k, 8)
        plane_copy(peer, j).wait_send()
        plane_copy(peer, peer).wait_recv()

    lane = lax.broadcasted_iota(jnp.int32, (RX, TILE), 1)
    rims = jnp.concatenate([got[s, 32:40, :] for s in range(8)])
    rims = pltpu.roll(rims, (TILE - 32 * (j % 4)) % TILE, 1)
    rims = jnp.concatenate([rims, jnp.zeros((64, TILE), jnp.float32)])
    rims = jnp.transpose(rims)[:RX]
    mass_sum = got[0, 40:41, :]
    for s in range(1, 8):
        mass_sum = mass_sum + got[s, 40:41, :]
    inverse = float(PLANES * NX * NY) / jnp.sum(mass_sum, axis=1, keepdims=True)
    blocks = []
    for s in range(8):
        right = pltpu.roll(rims, (-8 * ((s + 7) % 8)) % TILE, 1)
        left = pltpu.roll(rims, (120 - 8 * ((s + 1) % 8)) % TILE, 1)
        value = got[s, 0:32, :] + jnp.where(lane < 4, right, 0.0) + jnp.where(lane >= 125, left, 0.0)
        blocks.append(value * inverse - 1.0)
    turned = []
    for k, (re, im) in enumerate(real_eighths(blocks)):
        tr, ti = twist_y[0, k : k + 1, :], twist_y[1, k : k + 1, :]
        turned.append(jnp.concatenate([re * tr - im * ti, re * ti + im * tr], axis=1))
    high, low = split_bf16(jnp.concatenate(turned))

    def times(a, b):
        return lax.dot_general(a, b, NT, preferred_element_type=jnp.float32)

    wave = times(y_high[...], low) + times(y_low[...], high) + times(y_high[...], high)
    for h in range(2):
        for k in range(TILE):
            waves[2 * k + h] = wave[2 * k : 2 * k + 2, TILE * h : TILE * h + TILE]

    columns[j * 32 + i] = waves[me]

    def hand_out(k, _):
        for n in range(5):
            peer = lax.rem(me + 5 * k + n + 1, DEVICES)
            pltpu.make_async_remote_copy(
                src_ref=waves.at[peer], dst_ref=columns.at[j * 32 + i],
                send_sem=wave_send, recv_sem=wave_recv,
                device_id=place(peer), device_id_type=MESH,
            ).start()
        return 0

    lax.fori_loop(0, (DEVICES - 1) // 5, hand_out, 0)
    for copy in sent:
        copy.wait_send()
    others = columns.at[pl.ds(0, DEVICES - 1)]
    pltpu.make_async_copy(others, others, wave_recv).wait()
    pltpu.make_async_copy(others, others, wave_send).wait()


def transform(main, rim, total, counts, wave_tables):
    vmem = pl.BlockSpec(memory_space=pltpu.VMEM)
    f32 = jnp.float32

    def both(*lead):
        return [pltpu.VMEM((PLANES, *lead, RX, TILE), f32), pltpu.VMEM((2, *lead, 8, TILE), f32)]

    dma = pltpu.SemaphoreType.DMA
    return pl.pallas_call(
        transform_kernel,
        out_shape=(
            jax.ShapeDtypeStruct((DEVICES, 2, TILE), f32),
            jax.ShapeDtypeStruct((8, TILE), f32),
        ),
        in_specs=[vmem] * 7,
        out_specs=(vmem, vmem),
        scratch_shapes=[
            *both(4, 4), *both(2, 4), *both(4), *both(2), *both(),
            pltpu.VMEM((8, TILE), f32),
            pltpu.VMEM((OWNERS, 8, TILE), f32),
            pltpu.VMEM((PLANES, RX + 16, TILE), f32),
            pltpu.VMEM((PLANES, RX + 16, TILE), f32),
            pltpu.VMEM((DEVICES, 2, TILE), f32),
            dma((OWNERS,)), dma((OWNERS,)), dma((70,)), dma((70,)), dma((8,)), dma((8,)), dma, dma,
        ],
        compiler_params=pltpu.CompilerParams(
            collective_id=0, has_side_effects=True, vmem_limit_bytes=24 << 20
        ),
        name="transform",
    )(main, rim, total, counts, *wave_tables)


def finish_kernel(columns, begin_ref, x_both, x_low, twist_x, out_ref, start_ref):
    start_ref[0, :, 0:TILE] = begin_ref[0:1, :].astype(jnp.int32)
    start_ref[0, :, TILE:] = begin_ref[1:2, :].astype(jnp.int32)
    for g in range(4):
        pair = columns[64 * g : 64 * g + 64].reshape(TILE, TILE)
        high, low = split_bf16(jnp.transpose(pair))
        both = jnp.concatenate([high, low], axis=1)
        sums = jnp.dot(both, x_both[...], preferred_element_type=jnp.float32)
        sums = sums + jnp.dot(high, x_low[...], preferred_element_type=jnp.float32)
        parts = [[], []]
        for p in range(2):
            for w in range(4):
                re_sum = im_sum = None
                for q in range(4):
                    rows = slice(32 * w + 8 * q, 32 * w + 8 * q + 8)
                    re = sums[rows, 256 * p : 256 * p + 128]
                    im = sums[rows, 256 * p + 128 : 256 * p + 256]
                    tr, ti = twist_x[0, 8 * q : 8 * q + 8, :], twist_x[1, 8 * q : 8 * q + 8, :]
                    re_part, im_part = re * tr - im * ti, re * ti + im * tr
                    re_sum = re_part if q == 0 else re_sum + re_part
                    im_sum = im_part if q == 0 else im_sum + im_part
                parts[0].append(re_sum)
                parts[1].append(im_sum)
        re, im = (jnp.transpose(jnp.stack(part), (1, 0, 2)) for part in parts)
        for a, value in enumerate(eighths([(re[k], im[k]) for k in range(8)])):
            for n in range(2):
                for p in range(2):
                    out_ref[n, 2 * g + p, :, TILE * a : TILE * a + TILE] = value[n][4 * p : 4 * p + 4]


def finish(columns, begin, wave_tables):
    vmem = pl.BlockSpec(memory_space=pltpu.VMEM)
    return pl.pallas_call(
        finish_kernel,
        out_shape=(
            jax.ShapeDtypeStruct((2, PLANES, 4, NX), jnp.float32),
            jax.ShapeDtypeStruct((1, 1, 2 * TILE), jnp.int32),
        ),
        in_specs=[vmem] * 5,
        out_specs=(vmem, vmem),
        compiler_params=pltpu.CompilerParams(vmem_limit_bytes=24 << 20),
        name="finish",
    )(columns, begin, *wave_tables)


PX = ("px_0", "px_1", "px_2")
PX_PY = ("px_0", "px_1", "px_2", "py")


def local(cell_ids, offset_x, offset_y, mass, live, tile_owner, counts):
    main, rim, total = spread(tile_owner, cell_ids[0], offset_x[0], offset_y[0], mass[0], live[0])
    y_tables, x_tables = tables()
    columns, begin = transform(
        main.reshape(PLANES, 4, 4, 2, RX, TILE), rim.reshape(2, 4, 4, 2, 8, TILE), total, counts, y_tables
    )
    return finish(columns, begin, x_tables)


def solution(mesh):
    torus = Mesh(mesh.devices.reshape(4, 4, 2, mesh.shape["py"]), ("px_0", "px_1", "px_2", "py"))
    return jax.shard_map(
        local,
        mesh=torus,
        in_specs=(
            P(PX, "py", None),
            P(PX, "py", None),
            P(PX, "py", None),
            P(PX, "py", None),
            P(PX, "py", None),
            P(PX, "py"),
            P(PX, "py", None),
        ),
        out_specs=(P(None, None, PX_PY, None), P(PX, "py", None)),
        check_vma=False,
    )
```

```python
import functools
import math

import jax
import jax.numpy as jnp
import numpy as np
from jax import lax
from jax.experimental import pallas as pl
from jax.experimental.pallas import tpu as pltpu
from jax.sharding import Mesh
from jax.sharding import PartitionSpec as P

NX = 1024
NY = 1024
PLANES = 8
BETA = 18.4
OWNERS = 32
RX = 32
TILE = 128
NT = (((1,), (1,)), ((), ()))


def tap_values(step, fraction):
    z = (step.astype(jnp.float32) - fraction) * 0.25
    return jnp.exp(BETA * (jnp.sqrt(1.0 - z * z) - 1.0))


def spread_kernel(
    owner_hbm, cell_hbm, fx_hbm, fy_hbm, mass_hbm, live_hbm,
    main_ref, rim_ref, total_ref,
    owner_ref, cell_ref, fx_ref, fy_ref, mass_ref, live_ref, in_sem,
    grid_acc, rim_acc, lx_s, ly_s, fx_s, fy_s, w_s,
):
    tiles = cell_ref.shape[0]
    sources = (owner_hbm, cell_hbm, fx_hbm, fy_hbm, mass_hbm, live_hbm)
    homes = (owner_ref, cell_ref, fx_ref, fy_ref, mass_ref, live_ref)
    arrivals = [
        pltpu.make_async_copy(source, home, in_sem.at[k]) for k, (source, home) in enumerate(zip(sources, homes))
    ]
    for copy in arrivals:
        copy.start()
    zero = jnp.zeros((8, TILE), jnp.float32)

    def clear(i, _):
        for p in range(PLANES):
            grid_acc[p, pl.ds(pl.multiple_of(i * 8, 8), 8), :] = zero
        return 0

    lax.fori_loop(0, grid_acc.shape[1] // 8, clear, 0)

    def clear_rim(i, _):
        for p in range(8):
            rim_acc[i * 8 + p] = zero
        return 0

    lax.fori_loop(0, OWNERS, clear_rim, 0)

    for copy in arrivals:
        copy.wait()

    def prepare(i, _):
        rows = pl.ds(pl.multiple_of(i * 16, 16), 16)
        cell = cell_ref[rows, :]
        ly_s[rows, :] = cell & 127
        lx_s[rows, :] = (cell >> 7) & 31
        fx_s[rows, :] = fx_ref[rows, :].astype(jnp.float32)
        fy_s[rows, :] = fy_ref[rows, :].astype(jnp.float32)
        w_s[rows, :] = jnp.where(live_ref[rows, :] == 1, mass_ref[rows, :].astype(jnp.float32), 0.0)
        return 0

    lax.fori_loop(0, tiles // 16, prepare, 0)

    sub = lax.broadcasted_iota(jnp.int32, (8, TILE), 0)

    def row(ref, t):
        return jnp.broadcast_to(ref[pl.ds(t, 1), :], (8, TILE))

    def one_tile(t):
        lx, ly = row(lx_s, t), row(ly_s, t)
        jx = (sub - lx + 3) & 7
        jy = (sub - ly + 3) & 7
        tx = tap_values(jx - 3, row(fx_s, t))
        ty = tap_values(jy - 3, row(fy_s, t)) * row(w_s, t)
        gx = (lx + jx + 5) >> 3
        gy = (ly + jy - 3) >> 3
        gy = jnp.where(gy < 0, 16, gy)
        wx = jnp.concatenate([jnp.where(gx == g, tx, 0.0) for g in range(6)]).astype(jnp.bfloat16)
        wy = jnp.concatenate([jnp.where(gy == g, ty, 0.0) for g in range(16)]).astype(jnp.bfloat16)
        wr = jnp.concatenate([jnp.where(gy == 16, ty, 0.0), zero]).astype(jnp.bfloat16)
        main = lax.dot_general(wx, wy, NT, preferred_element_type=jnp.float32)
        rim = lax.dot_general(wr, wx, NT, preferred_element_type=jnp.float32)
        return main, rim[:8]

    unroll = 64

    def add_tiles(i, _):
        results = [one_tile(i * unroll + k) for k in range(unroll)]
        for k in range(unroll):
            owner = owner_ref[0, i * unroll + k]
            plane = cell_ref[pl.ds(i * unroll + k, 1), :][0, 0] >> 12
            bucket = owner * 8 + plane
            main, rim = results[k]
            rows = pl.ds(pl.multiple_of(owner * RX, RX), 48)
            grid_acc[plane, rows, :] = grid_acc[plane, rows, :] + main
            rim_acc[bucket, :, :48] = rim_acc[bucket, :, :48] + rim
        return 0

    lax.fori_loop(0, tiles // unroll, add_tiles, 0)

    for p in range(PLANES):
        grid_acc[p, 1024:1032, :] = grid_acc[p, 1024:1032, :] + grid_acc[p, 0:8, :]
        grid_acc[p, 8:16, :] = grid_acc[p, 8:16, :] + grid_acc[p, 1032:1040, :]

    lane = lax.broadcasted_iota(jnp.int32, (8, TILE), 1)

    def write_out(i, total):
        rows = pl.ds(pl.multiple_of(i * RX + 8, 8), RX)
        for p in range(PLANES):
            block = grid_acc[p, rows, :]
            main_ref[p, i // 2, i % 2] = block
            for k in range(RX // 8):
                total = total + block[8 * k : 8 * k + 8, :]
        before, after = (i + OWNERS - 1) % OWNERS, (i + 1) % OWNERS
        for q in range(2):
            out = zero
            for k in range(4):
                p = 4 * q + k
                own = pltpu.roll(rim_acc[i * 8 + p], (32 * k - 8) % 128, 1)
                low = pltpu.roll(rim_acc[before * 8 + p], (32 * k - 40) % 128, 1)
                high = pltpu.roll(rim_acc[after * 8 + p], (32 * k + 24) % 128, 1)
                spot = lane - 32 * k
                out = jnp.where((spot >= 0) & (spot < 32), own, out)
                out = out + jnp.where((spot >= 0) & (spot < 8), low, 0.0)
                out = out + jnp.where((spot >= 24) & (spot < 32), high, 0.0)
            rim_ref[q, i // 2, i % 2] = out
            total = total + out
        return total

    total_ref[...] = lax.fori_loop(0, OWNERS, write_out, zero)


def spread(owners, cells, fx, fy, mass, live):
    tiles = cells.shape[0]
    vmem = pl.BlockSpec(memory_space=pltpu.VMEM)
    return pl.pallas_call(
        spread_kernel,
        out_shape=(
            jax.ShapeDtypeStruct((PLANES, 16, 2, RX, TILE), jnp.float32),
            jax.ShapeDtypeStruct((2, 16, 2, 8, TILE), jnp.float32),
            jax.ShapeDtypeStruct((8, TILE), jnp.float32),
        ),
        in_specs=[pl.BlockSpec(memory_space=pltpu.HBM)] * 6,
        out_specs=(vmem, vmem, vmem),
        scratch_shapes=[
            pltpu.SMEM((1, tiles), jnp.int32),
            pltpu.VMEM((tiles, TILE), jnp.int32),
            pltpu.VMEM((tiles, TILE), jnp.bfloat16),
            pltpu.VMEM((tiles, TILE), jnp.bfloat16),
            pltpu.VMEM((tiles, TILE), jnp.bfloat16),
            pltpu.VMEM((tiles, TILE), jnp.int32),
            pltpu.SemaphoreType.DMA((6,)),
            pltpu.VMEM((PLANES, NX + 16, TILE), jnp.float32),
            pltpu.VMEM((OWNERS * PLANES, 8, TILE), jnp.float32),
            pltpu.VMEM((tiles, TILE), jnp.int32),
            pltpu.VMEM((tiles, TILE), jnp.int32),
            pltpu.VMEM((tiles, TILE), jnp.float32),
            pltpu.VMEM((tiles, TILE), jnp.float32),
            pltpu.VMEM((tiles, TILE), jnp.float32),
        ],
        compiler_params=pltpu.CompilerParams(vmem_limit_bytes=24 << 20),
        name="spread",
    )(*(pltpu.with_memory_space_constraint(a, pltpu.HBM) for a in (owners, cells, fx, fy, mass, live)))


COORDS = ("px_0", "px_1", "px_2")
DEVICES = 256


def split_bf16(value):
    high = value.astype(jnp.bfloat16)
    return high, (value - high.astype(jnp.float32)).astype(jnp.bfloat16)


def np_split(value):
    high = np.asarray(value, np.float32).astype(jnp.bfloat16)
    low = (np.asarray(value, np.float64) - high.astype(np.float64)).astype(jnp.bfloat16)
    return high, low


def tables():
    k = np.arange(TILE)
    turn_y = 2 * np.pi / NY * (np.arange(8)[:, None] * k[None, :])
    twist_y = np.stack([np.cos(turn_y), -np.sin(turn_y)]).astype(np.float32)
    theta = 2 * np.pi / TILE * (k[:, None] * k[None, :] % TILE)
    wave_y = np.zeros((TILE, 2, 2, TILE))
    wave_y[:, 0, 0], wave_y[:, 0, 1] = np.cos(theta), np.sin(theta)
    wave_y[:, 1, 0], wave_y[:, 1, 1] = -np.sin(theta), np.cos(theta)
    y_high, y_low = np_split(wave_y.reshape(2 * TILE, 2 * TILE))
    phase = 2 * np.pi / OWNERS * (np.arange(OWNERS)[:, None] * k[None, :] % OWNERS)
    block = np.zeros((OWNERS, 2, 2, TILE))
    block[:, 0, 0], block[:, 1, 0] = np.cos(phase), np.sin(phase)
    block[:, 0, 1], block[:, 1, 1] = -np.sin(phase), np.cos(phase)
    wave_x = np.kron(np.eye(2), block.reshape(2 * OWNERS, 2 * TILE))
    x_high, x_low = np_split(wave_x)
    turn_x = 2 * np.pi / NX * (np.arange(RX)[:, None] * k[None, :])
    scale = 1.0 / math.sqrt(NX * NY)
    twist_x = (scale * np.stack([np.cos(turn_x), -np.sin(turn_x)])).astype(np.float32)
    return (twist_y, y_high, y_low), (np.concatenate([x_high, x_high]), x_low, twist_x)


HALF = math.sqrt(0.5)


def real_eighths(d):
    s = [d[k] + d[k + 4] for k in range(4)]
    e = [d[k] - d[k + 4] for k in range(4)]
    near_sum, far_sum = s[0] + s[2], s[1] + s[3]
    a0, a4 = near_sum + far_sum, near_sum - far_sum
    re2, im2 = s[0] - s[2], s[3] - s[1]
    tilt, lean = (e[1] - e[3]) * HALF, (e[1] + e[3]) * HALF
    re1, im1 = e[0] + tilt, -e[2] - lean
    re3, im3 = e[0] - tilt, e[2] - lean
    zero = jnp.zeros_like(a0)
    return [(a0, zero), (re1, im1), (re2, im2), (re3, im3), (a4, zero), (re3, -im3), (re2, -im2), (re1, -im1)]


def fourths(t):
    def add(p, q):
        return p[0] + q[0], p[1] + q[1]

    def less(p, q):
        return p[0] - q[0], p[1] - q[1]

    e0, e1 = add(t[0], t[2]), less(t[0], t[2])
    f0, g = add(t[1], t[3]), less(t[1], t[3])
    f1 = (g[1], -g[0])
    return [add(e0, f0), add(e1, f1), less(e0, f0), less(e1, f1)]


def eighths(z):
    s = [(z[k][0] + z[k + 4][0], z[k][1] + z[k + 4][1]) for k in range(4)]
    d = [(z[k][0] - z[k + 4][0], z[k][1] - z[k + 4][1]) for k in range(4)]
    turned = [
        d[0],
        ((d[1][0] + d[1][1]) * HALF, (d[1][1] - d[1][0]) * HALF),
        (d[2][1], -d[2][0]),
        ((d[3][1] - d[3][0]) * HALF, -(d[3][0] + d[3][1]) * HALF),
    ]
    even, odd = fourths(s), fourths(turned)
    return [even[0], odd[0], even[1], odd[1], even[2], odd[2], even[3], odd[3]]


def near(v):
    return v + 1 - 2 * lax.rem(v, 2)


def far(v):
    return 3 - v


ROUTES = (("x", "near"), ("x", "far"), ("y", "near"), ("y", "far"))
MESH = pl.DeviceIdType.MESH


def transform_kernel(
    main_ref, rim_ref, total_ref, counts_hbm, twist_hbm, y_high_hbm, y_low_hbm,
    columns, begin_out,
    counts_ref, twist_y, y_high, y_low, table_sem,
    main0, rim0, main1, rim1, main2, rim2, main3, rim3, main4, rim4,
    note, notes, pack, got, waves,
    note_send, note_recv, send, recv, py_send, py_recv, wave_send, wave_recv,
):
    x, y, c = (lax.axis_index(a) for a in COORDS)
    j = lax.axis_index("py")
    i = (x * 4 + y) * 2 + c
    me = i * 8 + j
    barrier = pltpu.get_barrier_semaphore()

    def device(x, y, c):
        return {"px_0": x, "px_1": y, "px_2": c}

    tables_in = [
        pltpu.make_async_copy(table, spot, table_sem.at[k])
        for k, (table, spot) in enumerate(
            ((counts_hbm, counts_ref), (twist_hbm, twist_y), (y_high_hbm, y_high), (y_low_hbm, y_low))
        )
    ]
    for copy in tables_in:
        copy.start()
    xs = [x] + [lax.rem(x + k, 4) for k in range(1, 4)]
    ys = [y] + [lax.rem(y + k, 4) for k in range(1, 4)]
    js = [j] + [lax.rem(j + k, 8) for k in range(1, 8)]
    column = [(xs[a], ys[b], (c, 1 - c)[d]) for a in range(4) for b in range(4) for d in range(2)][1:]
    for peer in column:
        pl.semaphore_signal(barrier, inc=1, device_id=device(*peer), device_id_type=MESH)
    for k in range(1, 8):
        pl.semaphore_signal(barrier, inc=1, device_id={"py": js[k]}, device_id_type=MESH)
    tables_in[0].wait()
    note[0:1, :] = counts_ref[0, :, 0:TILE].astype(jnp.float32)
    note[1:2, :] = counts_ref[0, :, TILE:].astype(jnp.float32)
    note[2:3, :] = jnp.sum(total_ref[...], axis=0, keepdims=True)
    note[3:8, :] = jnp.zeros((5, TILE), jnp.float32)
    notes[i] = note[...]
    pl.semaphore_wait(barrier, OWNERS - 1 + 7)

    def remote(src, dst, slot, where):
        copy = pltpu.make_async_remote_copy(
            src_ref=src, dst_ref=dst, send_sem=send.at[slot], recv_sem=recv.at[slot],
            device_id=where, device_id_type=MESH,
        )
        copy.start()
        return copy

    chunks = {}
    for k in (8, 9, *range(8)):
        if k < 8:
            refs = (main_ref.at[k], *(r.at[k] for r in (main0, main1, main2, main3, main4)))
        else:
            refs = (rim_ref.at[k - 8], *(r.at[k - 8] for r in (rim0, rim1, rim2, rim3, rim4)))
        chunks[k] = (*refs, k % 4 if k < 8 else 2 * (k - 8))

    def leg(first, kind):
        v = x if first == "x" else y
        if kind == "near":
            low = lax.rem((v + 1) // 2, 2)
            keep, give = (low, 3 - low), (1 - low, 2 + low)
            partner, other = near(v), far(v)
        else:
            low = 2 * (v // 2)
            keep, give = (low, low + 1), (2 - low, 3 - low)
            partner, other = far(v), near(v)
        if first == "x":
            return keep, give, device(partner, y, c), other, device(other, y, c)
        return keep, give, device(x, partner, c), other, device(x, other, c)

    pending = {}
    for k, (src, b0, *_) in chunks.items():
        pending[k] = [remote(src.at[:, :, 1 - c], b0, 7 * k, device(x, y, 1 - c))]

    def note_copy(peer, slot, source):
        return pltpu.make_async_remote_copy(
            src_ref=note, dst_ref=notes.at[source], send_sem=note_send.at[slot], recv_sem=note_recv.at[source],
            device_id=device(*peer), device_id_type=MESH,
        )

    for k, peer in enumerate(column):
        note_copy(peer, k, i).start()
    sent = []

    def arrive(k):
        for copy in pending[k]:
            copy.wait_recv()
        sent.extend(pending[k])

    for k, (src, b0, b1, b2, b3, b4, route) in chunks.items():
        arrive(k)

        def add0(n, _, src=src, b0=b0):
            for m in range(4):
                b0[n, m] = b0[n, m] + src[n, m, c]
            return 0

        lax.fori_loop(0, 4, add0, 0)
        first, kind = ROUTES[route]
        _, give, where, _, _ = leg(first, kind)
        pending[k] = []
        for n in range(2):
            block = b0.at[give[n]] if first == "x" else b0.at[:, give[n]]
            pending[k].append(remote(block, b1.at[n], 7 * k + 1 + n, where))

    for k, (src, b0, b1, b2, b3, b4, route) in chunks.items():
        arrive(k)
        first, kind = ROUTES[route]
        keep, _, _, other, where = leg(first, kind)
        for n in range(2):
            for m in range(4):
                at = (keep[n], m) if first == "x" else (m, keep[n])
                b0[at] = b0[at] + b1[n, m]
        block = b0.at[other] if first == "x" else b0.at[:, other]
        pending[k] = [remote(block, b2, 7 * k + 3, where)]

    for k, (src, b0, b1, b2, b3, b4, route) in chunks.items():
        arrive(k)
        first, kind = ROUTES[route]
        for m in range(4):
            at = (x, m) if first == "x" else (m, y)
            b0[at] = b0[at] + b2[m]
        second = "y" if first == "x" else "x"
        _, give, where, _, _ = leg(second, kind)
        pending[k] = []
        for n in range(2):
            block = b0.at[x, give[n]] if first == "x" else b0.at[give[n], y]
            pending[k].append(remote(block, b3.at[n], 7 * k + 4 + n, where))

    for k, (src, b0, b1, b2, b3, b4, route) in chunks.items():
        arrive(k)
        first, kind = ROUTES[route]
        second = "y" if first == "x" else "x"
        keep, _, _, other, where = leg(second, kind)
        for n in range(2):
            at = (x, keep[n]) if first == "x" else (keep[n], y)
            b0[at] = b0[at] + b3[n]
        block = b0.at[x, other] if first == "x" else b0.at[other, y]
        pending[k] = [remote(block, b4, 7 * k + 6, where)]

    for k, peer in enumerate(column):
        copy = note_copy(peer, k, (peer[0] * 4 + peer[1]) * 2 + peer[2])
        copy.wait_send()
        copy.wait_recv()
    everyone = notes[0]
    for k in range(1, OWNERS):
        everyone = everyone + notes[k]
    amount = jnp.broadcast_to(everyone[2:3, :], (8, TILE))

    def plane_copy(k, source):
        return pltpu.make_async_remote_copy(
            src_ref=pack.at[k], dst_ref=got.at[source], send_sem=py_send.at[k], recv_sem=py_recv.at[source],
            device_id={"py": k}, device_id_type=MESH,
        )

    for k, (src, b0, b1, b2, b3, b4, route) in chunks.items():
        arrive(k)
        block = b0[x, y] + b4[...]
        if k >= 8:
            for p in range(4):
                pack[4 * (k - 8) + p, RX : RX + 8, :] = block
                pack[4 * (k - 8) + p, RX + 8 :, :] = amount
            continue
        pack[k, 0:RX, :] = block

        @pl.when(k != j)
        def _():
            plane_copy(k, j).start()

        @pl.when(k == j)
        def _():
            got[k] = pack[k]

    earlier = jnp.zeros((8, TILE), jnp.float32)
    for k in range(OWNERS):
        earlier = earlier + jnp.where(k < i, notes[k], 0.0)
    spot = lax.broadcasted_iota(jnp.int32, (8, TILE), 1)
    running = everyone
    for shift in (1, 2, 4, 8, 16, 32, 64):
        running = running + jnp.where(spot >= shift, pltpu.roll(running, shift, 1), 0.0)
    begin = running - everyone + earlier
    whole = jnp.sum(everyone[0:1, :], axis=1, keepdims=True)
    begin_out[0:1, :] = begin[0:1, :]
    begin_out[1:2, :] = begin[1:2, :] + whole
    begin_out[2:8, :] = jnp.zeros((6, TILE), jnp.float32)

    for k in range(1, 8):
        peer = js[k]
        plane_copy(peer, j).wait_send()
        plane_copy(peer, peer).wait_recv()

    for copy in tables_in[1:]:
        copy.wait()
    lane = lax.broadcasted_iota(jnp.int32, (RX, TILE), 1)
    rims = jnp.concatenate([got[s, 32:40, :] for s in range(8)])
    rims = pltpu.roll(rims, (TILE - 32 * (j % 4)) % TILE, 1)
    rims = jnp.concatenate([rims, jnp.zeros((64, TILE), jnp.float32)])
    rims = jnp.transpose(rims)[:RX]
    mass_sum = got[0, 40:41, :]
    for s in range(1, 8):
        mass_sum = mass_sum + got[s, 40:41, :]
    inverse = float(PLANES * NX * NY) / jnp.sum(mass_sum, axis=1, keepdims=True)
    blocks = []
    for s in range(8):
        right = pltpu.roll(rims, (-8 * ((s + 7) % 8)) % TILE, 1)
        left = pltpu.roll(rims, (120 - 8 * ((s + 1) % 8)) % TILE, 1)
        value = got[s, 0:32, :] + jnp.where(lane < 4, right, 0.0) + jnp.where(lane >= 125, left, 0.0)
        blocks.append(value * inverse - 1.0)
    turned = []
    for k, (re, im) in enumerate(real_eighths(blocks)):
        tr, ti = twist_y[0, k : k + 1, :], twist_y[1, k : k + 1, :]
        turned.append(jnp.concatenate([re * tr - im * ti, re * ti + im * tr], axis=1))
    high, low = split_bf16(jnp.concatenate(turned))

    def times(a, b):
        return lax.dot_general(a, b, NT, preferred_element_type=jnp.float32)

    wave = times(y_high[...], low) + times(y_low[...], high) + times(y_high[...], high)
    for h in range(2):
        for k in range(TILE):
            waves[2 * k + h] = wave[2 * k : 2 * k + 2, TILE * h : TILE * h + TILE]

    columns[j * 32 + i] = waves[me]

    def hand_out(row, place, n):
        pltpu.make_async_remote_copy(
            src_ref=waves.at[row * 8 + js[n]], dst_ref=columns.at[j * 32 + i],
            send_sem=wave_send, recv_sem=wave_recv,
            device_id={**place, "py": js[n]}, device_id_type=MESH,
        ).start()

    def hand_out_row(k, _):
        row = lax.rem(i + k, OWNERS)
        place = device(row // 8, lax.rem(row // 2, 4), lax.rem(row, 2))
        for n in range(8):
            hand_out(row, place, n)
        return 0

    lax.fori_loop(1, OWNERS, hand_out_row, 0)
    for n in range(1, 8):
        hand_out(i, {}, n)
    for copy in sent:
        copy.wait_send()
    others = columns.at[pl.ds(0, DEVICES - 1)]
    pltpu.make_async_copy(others, others, wave_recv).wait()
    pltpu.make_async_copy(others, others, wave_send).wait()


def transform(main, rim, total, counts, wave_tables):
    vmem = pl.BlockSpec(memory_space=pltpu.VMEM)
    f32 = jnp.float32

    def both(*lead):
        return [pltpu.VMEM((PLANES, *lead, RX, TILE), f32), pltpu.VMEM((2, *lead, 8, TILE), f32)]

    dma = pltpu.SemaphoreType.DMA
    return pl.pallas_call(
        transform_kernel,
        out_shape=(
            jax.ShapeDtypeStruct((DEVICES, 2, TILE), f32),
            jax.ShapeDtypeStruct((8, TILE), f32),
        ),
        in_specs=[vmem] * 3 + [pl.BlockSpec(memory_space=pltpu.HBM)] * 4,
        out_specs=(vmem, vmem),
        scratch_shapes=[
            pltpu.VMEM((1, 1, 2 * TILE), jnp.int32),
            pltpu.VMEM((2, 8, TILE), f32),
            pltpu.VMEM((2 * TILE, 2 * TILE), jnp.bfloat16),
            pltpu.VMEM((2 * TILE, 2 * TILE), jnp.bfloat16),
            dma((4,)),
            *both(4, 4), *both(2, 4), *both(4), *both(2), *both(),
            pltpu.VMEM((8, TILE), f32),
            pltpu.VMEM((OWNERS, 8, TILE), f32),
            pltpu.VMEM((PLANES, RX + 16, TILE), f32),
            pltpu.VMEM((PLANES, RX + 16, TILE), f32),
            pltpu.VMEM((DEVICES, 2, TILE), f32),
            dma((OWNERS,)), dma((OWNERS,)), dma((70,)), dma((70,)), dma((8,)), dma((8,)), dma, dma,
        ],
        compiler_params=pltpu.CompilerParams(
            collective_id=0, has_side_effects=True, vmem_limit_bytes=24 << 20
        ),
        name="transform",
    )(main, rim, total, *(pltpu.with_memory_space_constraint(a, pltpu.HBM) for a in (counts, *wave_tables)))


def finish_kernel(columns, begin_ref, x_both, x_low, twist_x, out_ref, start_ref):
    start_ref[0, :, 0:TILE] = begin_ref[0:1, :].astype(jnp.int32)
    start_ref[0, :, TILE:] = begin_ref[1:2, :].astype(jnp.int32)
    for g in range(4):
        pair = columns[64 * g : 64 * g + 64].reshape(TILE, TILE)
        high, low = split_bf16(jnp.transpose(pair))
        both = jnp.concatenate([high, low], axis=1)
        sums = jnp.dot(both, x_both[...], preferred_element_type=jnp.float32)
        sums = sums + jnp.dot(high, x_low[...], preferred_element_type=jnp.float32)
        parts = [[], []]
        for p in range(2):
            for w in range(4):
                re_sum = im_sum = None
                for q in range(4):
                    rows = slice(32 * w + 8 * q, 32 * w + 8 * q + 8)
                    re = sums[rows, 256 * p : 256 * p + 128]
                    im = sums[rows, 256 * p + 128 : 256 * p + 256]
                    tr, ti = twist_x[0, 8 * q : 8 * q + 8, :], twist_x[1, 8 * q : 8 * q + 8, :]
                    re_part, im_part = re * tr - im * ti, re * ti + im * tr
                    re_sum = re_part if q == 0 else re_sum + re_part
                    im_sum = im_part if q == 0 else im_sum + im_part
                parts[0].append(re_sum)
                parts[1].append(im_sum)
        re, im = (jnp.transpose(jnp.stack(part), (1, 0, 2)) for part in parts)
        for a, value in enumerate(eighths([(re[k], im[k]) for k in range(8)])):
            for n in range(2):
                for p in range(2):
                    out_ref[n, 2 * g + p, :, TILE * a : TILE * a + TILE] = value[n][4 * p : 4 * p + 4]


def finish(columns, begin, wave_tables):
    vmem = pl.BlockSpec(memory_space=pltpu.VMEM)
    return pl.pallas_call(
        finish_kernel,
        out_shape=(
            jax.ShapeDtypeStruct((2, PLANES, 4, NX), jnp.float32),
            jax.ShapeDtypeStruct((1, 1, 2 * TILE), jnp.int32),
        ),
        in_specs=[vmem] * 5,
        out_specs=(vmem, vmem),
        compiler_params=pltpu.CompilerParams(vmem_limit_bytes=24 << 20),
        name="finish",
    )(columns, begin, *wave_tables)


PX = ("px_0", "px_1", "px_2")
PX_PY = ("px_0", "px_1", "px_2", "py")


def local(cell_ids, offset_x, offset_y, mass, live, tile_owner, counts):
    main, rim, total = spread(tile_owner, cell_ids[0], offset_x[0], offset_y[0], mass[0], live[0])
    y_tables, x_tables = tables()
    columns, begin = transform(
        main.reshape(PLANES, 4, 4, 2, RX, TILE), rim.reshape(2, 4, 4, 2, 8, TILE), total, counts, y_tables
    )
    return finish(columns, begin, x_tables)


def solution(mesh):
    torus = Mesh(mesh.devices.reshape(4, 4, 2, mesh.shape["py"]), ("px_0", "px_1", "px_2", "py"))
    return jax.shard_map(
        local,
        mesh=torus,
        in_specs=(
            P(PX, "py", None),
            P(PX, "py", None),
            P(PX, "py", None),
            P(PX, "py", None),
            P(PX, "py", None),
            P(PX, "py"),
            P(PX, "py", None),
        ),
        out_specs=(P(None, None, PX_PY, None), P(PX, "py", None)),
        check_vma=False,
    )
```

```python
import functools
import math

import jax
import jax.numpy as jnp
import numpy as np
from jax import lax
from jax.experimental import pallas as pl
from jax.experimental.pallas import tpu as pltpu
from jax.sharding import Mesh
from jax.sharding import PartitionSpec as P

NX = 1024
NY = 1024
PLANES = 8
BETA = 18.4
OWNERS = 32
BLOCKS = OWNERS + 2
RX = 32
TILE = 128
NT = (((1,), (1,)), ((), ()))


def tap_values(step, fraction):
    z = (step.astype(jnp.float32) - fraction) * 0.25
    return jnp.exp(BETA * (jnp.sqrt(1.0 - z * z) - 1.0))


def spread_kernel(
    owner_hbm, cell_hbm, fx_hbm, fy_hbm, mass_hbm, live_hbm,
    main_ref, rim_ref, total_ref,
    owner_ref, cell_ref, fx_ref, fy_ref, mass_ref, live_ref, in_sem,
    rim_acc, lx_s, ly_s, fx_s, fy_s, w_s,
):
    tiles = cell_ref.shape[0]
    sources = (owner_hbm, cell_hbm, fx_hbm, fy_hbm, mass_hbm, live_hbm)
    homes = (owner_ref, cell_ref, fx_ref, fy_ref, mass_ref, live_ref)
    arrivals = [
        pltpu.make_async_copy(source, home, in_sem.at[k]) for k, (source, home) in enumerate(zip(sources, homes))
    ]
    for copy in arrivals:
        copy.start()
    zero = jnp.zeros((8, TILE), jnp.float32)

    def clear(i, _):
        for p in range(PLANES):
            for k in range(RX // 8):
                main_ref[i * PLANES + p, 8 * k : 8 * k + 8, :] = zero
        return 0

    lax.fori_loop(0, BLOCKS, clear, 0)

    def clear_rim(i, _):
        for p in range(8):
            rim_acc[i * 8 + p] = zero
        return 0

    lax.fori_loop(0, OWNERS, clear_rim, 0)

    for copy in arrivals:
        copy.wait()

    def prepare(i, _):
        rows = pl.ds(pl.multiple_of(i * 16, 16), 16)
        cell = cell_ref[rows, :]
        ly_s[rows, :] = cell & 127
        lx_s[rows, :] = (cell >> 7) & 31
        fx_s[rows, :] = fx_ref[rows, :].astype(jnp.float32)
        fy_s[rows, :] = fy_ref[rows, :].astype(jnp.float32)
        w_s[rows, :] = jnp.where(live_ref[rows, :] == 1, mass_ref[rows, :].astype(jnp.float32), 0.0)
        return 0

    lax.fori_loop(0, tiles // 16, prepare, 0)

    sub = lax.broadcasted_iota(jnp.int32, (8, TILE), 0)

    def row(ref, t):
        return jnp.broadcast_to(ref[pl.ds(t, 1), :], (8, TILE))

    def one_tile(t):
        lx, ly = row(lx_s, t), row(ly_s, t)
        jx = (sub - lx + 3) & 7
        jy = (sub - ly + 3) & 7
        tx = tap_values(jx - 3, row(fx_s, t))
        ty = tap_values(jy - 3, row(fy_s, t)) * row(w_s, t)
        gx = (lx + jx + 5) >> 3
        gy = (ly + jy - 3) >> 3
        gy = jnp.where(gy < 0, 16, gy)
        wx = jnp.concatenate([jnp.where(gx == g, tx, 0.0) for g in range(6)]).astype(jnp.bfloat16)
        wy = jnp.concatenate([jnp.where(gy == g, ty, 0.0) for g in range(16)]).astype(jnp.bfloat16)
        wr = jnp.concatenate([jnp.where(gy == 16, ty, 0.0), zero]).astype(jnp.bfloat16)
        main = lax.dot_general(wx, wy, NT, preferred_element_type=jnp.float32)
        rim = lax.dot_general(wr, wx, NT, preferred_element_type=jnp.float32)
        return main, rim[:8]

    unroll = 160

    def add_tiles(i, _):
        results = [one_tile(i * unroll + k) for k in range(unroll)]
        for k in range(unroll):
            owner = owner_ref[0, i * unroll + k]
            plane = cell_ref[pl.ds(i * unroll + k, 1), :][0, 0] >> 12
            bucket = owner * 8 + plane
            main, rim = results[k]
            spot = plane * BLOCKS + owner
            main_ref[spot, 24:32, :] = main_ref[spot, 24:32, :] + main[:8]
            main_ref[spot + 1] = main_ref[spot + 1] + main[8:40]
            main_ref[spot + 2, 0:8, :] = main_ref[spot + 2, 0:8, :] + main[40:]
            rim_acc[bucket, :, :48] = rim_acc[bucket, :, :48] + rim
        return 0

    lax.fori_loop(0, tiles // unroll, add_tiles, 0)

    for p in range(PLANES):
        first, last = p * BLOCKS, p * BLOCKS + OWNERS
        main_ref[last, 24:32, :] = main_ref[last, 24:32, :] + main_ref[first, 24:32, :]
        main_ref[first + 1, 0:8, :] = main_ref[first + 1, 0:8, :] + main_ref[last + 1, 0:8, :]

    lane = lax.broadcasted_iota(jnp.int32, (8, TILE), 1)

    def write_out(i, total):
        parts = [main_ref[p * BLOCKS + i + 1, 8 * k : 8 * k + 8, :] for p in range(PLANES) for k in range(RX // 8)]
        while len(parts) > 1:
            parts = [one + two for one, two in zip(parts[::2], parts[1::2])]
        total = total + parts[0]
        before, after = (i + OWNERS - 1) % OWNERS, (i + 1) % OWNERS
        for q in range(2):
            out = zero
            for k in range(4):
                p = 4 * q + k
                own = pltpu.roll(rim_acc[i * 8 + p], (32 * k - 8) % 128, 1)
                low = pltpu.roll(rim_acc[before * 8 + p], (32 * k - 40) % 128, 1)
                high = pltpu.roll(rim_acc[after * 8 + p], (32 * k + 24) % 128, 1)
                spot = lane - 32 * k
                out = jnp.where((spot >= 0) & (spot < 32), own, out)
                out = out + jnp.where((spot >= 0) & (spot < 8), low, 0.0)
                out = out + jnp.where((spot >= 24) & (spot < 32), high, 0.0)
            rim_ref[q, i // 2, i % 2] = out
            total = total + out
        return total

    total_ref[...] = lax.fori_loop(0, OWNERS, write_out, zero)


def spread(owners, cells, fx, fy, mass, live):
    tiles = cells.shape[0]
    vmem = pl.BlockSpec(memory_space=pltpu.VMEM)
    return pl.pallas_call(
        spread_kernel,
        out_shape=(
            jax.ShapeDtypeStruct((PLANES * BLOCKS, RX, TILE), jnp.float32),
            jax.ShapeDtypeStruct((2, 16, 2, 8, TILE), jnp.float32),
            jax.ShapeDtypeStruct((8, TILE), jnp.float32),
        ),
        in_specs=[pl.BlockSpec(memory_space=pltpu.HBM)] * 6,
        out_specs=(vmem, vmem, vmem),
        scratch_shapes=[
            pltpu.SMEM((1, tiles), jnp.int32),
            pltpu.VMEM((tiles, TILE), jnp.int32),
            pltpu.VMEM((tiles, TILE), jnp.bfloat16),
            pltpu.VMEM((tiles, TILE), jnp.bfloat16),
            pltpu.VMEM((tiles, TILE), jnp.bfloat16),
            pltpu.VMEM((tiles, TILE), jnp.int32),
            pltpu.SemaphoreType.DMA((6,)),
            pltpu.VMEM((OWNERS * PLANES, 8, TILE), jnp.float32),
            pltpu.VMEM((tiles, TILE), jnp.int32),
            pltpu.VMEM((tiles, TILE), jnp.int32),
            pltpu.VMEM((tiles, TILE), jnp.float32),
            pltpu.VMEM((tiles, TILE), jnp.float32),
            pltpu.VMEM((tiles, TILE), jnp.float32),
        ],
        compiler_params=pltpu.CompilerParams(vmem_limit_bytes=24 << 20),
        name="spread",
    )(*(pltpu.with_memory_space_constraint(a, pltpu.HBM) for a in (owners, cells, fx, fy, mass, live)))


COORDS = ("px_0", "px_1", "px_2")
DEVICES = 256


def split_bf16(value):
    high = value.astype(jnp.bfloat16)
    return high, (value - high.astype(jnp.float32)).astype(jnp.bfloat16)


def np_split(value):
    high = np.asarray(value, np.float32).astype(jnp.bfloat16)
    low = (np.asarray(value, np.float64) - high.astype(np.float64)).astype(jnp.bfloat16)
    return high, low


def tables():
    k = np.arange(TILE)
    turn_y = 2 * np.pi / NY * (np.arange(8)[:, None] * k[None, :])
    twist_y = np.stack([np.cos(turn_y), -np.sin(turn_y)]).astype(np.float32)
    theta = 2 * np.pi / TILE * (k[:, None] * k[None, :] % TILE)
    wave_y = np.zeros((TILE, 2, 2, TILE))
    wave_y[:, 0, 0], wave_y[:, 0, 1] = np.cos(theta), np.sin(theta)
    wave_y[:, 1, 0], wave_y[:, 1, 1] = -np.sin(theta), np.cos(theta)
    y_high, y_low = np_split(wave_y.reshape(2 * TILE, 2 * TILE))
    phase = 2 * np.pi / OWNERS * (np.arange(OWNERS)[:, None] * k[None, :] % OWNERS)
    block = np.zeros((OWNERS, 2, 2, TILE))
    block[:, 0, 0], block[:, 1, 0] = np.cos(phase), np.sin(phase)
    block[:, 0, 1], block[:, 1, 1] = -np.sin(phase), np.cos(phase)
    wave_x = np.kron(np.eye(2), block.reshape(2 * OWNERS, 2 * TILE))
    x_high, x_low = np_split(wave_x)
    turn_x = 2 * np.pi / NX * (np.arange(RX)[:, None] * k[None, :])
    scale = 1.0 / math.sqrt(NX * NY)
    twist_x = (scale * np.stack([np.cos(turn_x), -np.sin(turn_x)])).astype(np.float32)
    return (twist_y, y_high, y_low), (np.concatenate([x_high, x_high]), x_low, twist_x)


HALF = math.sqrt(0.5)


def real_eighths(d):
    s = [d[k] + d[k + 4] for k in range(4)]
    e = [d[k] - d[k + 4] for k in range(4)]
    near_sum, far_sum = s[0] + s[2], s[1] + s[3]
    a0, a4 = near_sum + far_sum, near_sum - far_sum
    re2, im2 = s[0] - s[2], s[3] - s[1]
    tilt, lean = (e[1] - e[3]) * HALF, (e[1] + e[3]) * HALF
    re1, im1 = e[0] + tilt, -e[2] - lean
    re3, im3 = e[0] - tilt, e[2] - lean
    zero = jnp.zeros_like(a0)
    return [(a0, zero), (re1, im1), (re2, im2), (re3, im3), (a4, zero), (re3, -im3), (re2, -im2), (re1, -im1)]


def fourths(t):
    def add(p, q):
        return p[0] + q[0], p[1] + q[1]

    def less(p, q):
        return p[0] - q[0], p[1] - q[1]

    e0, e1 = add(t[0], t[2]), less(t[0], t[2])
    f0, g = add(t[1], t[3]), less(t[1], t[3])
    f1 = (g[1], -g[0])
    return [add(e0, f0), add(e1, f1), less(e0, f0), less(e1, f1)]


def eighths(z):
    s = [(z[k][0] + z[k + 4][0], z[k][1] + z[k + 4][1]) for k in range(4)]
    d = [(z[k][0] - z[k + 4][0], z[k][1] - z[k + 4][1]) for k in range(4)]
    turned = [
        d[0],
        ((d[1][0] + d[1][1]) * HALF, (d[1][1] - d[1][0]) * HALF),
        (d[2][1], -d[2][0]),
        ((d[3][1] - d[3][0]) * HALF, -(d[3][0] + d[3][1]) * HALF),
    ]
    even, odd = fourths(s), fourths(turned)
    return [even[0], odd[0], even[1], odd[1], even[2], odd[2], even[3], odd[3]]


def near(v):
    return v + 1 - 2 * lax.rem(v, 2)


def far(v):
    return 3 - v


ROUTES = (("x", "near"), ("x", "far"), ("y", "near"), ("y", "far"))
MESH = pl.DeviceIdType.MESH


def hops(offset):
    a, b, d, e = offset
    return min(a, 4 - a) + min(b, 4 - b) + min(e, 8 - e)


FAR_FIRST = sorted(
    ((a, b, d, e) for a in range(4) for b in range(4) for e in range(8) for d in range(2) if (a, b, d, e) != (0, 0, 0, 0)),
    key=lambda o: (-hops(o), (7 * o[0] + 3 * o[1] + 5 * o[3]) % 11),
)


def transform_kernel(
    main_ref, rim_ref, total_ref, counts_hbm, twist_hbm, y_high_hbm, y_low_hbm,
    columns, begin_out,
    counts_ref, twist_y, y_high, y_low, table_sem,
    main0, rim0, main1, rim1, main2, rim2, main3, rim3, main4, rim4,
    note, notes, pack, got, waves,
    note_send, note_recv, send, recv, py_send, py_recv, wave_send, wave_recv,
):
    x, y, c = (lax.axis_index(a) for a in COORDS)
    j = lax.axis_index("py")
    i = (x * 4 + y) * 2 + c
    me = i * 8 + j
    barrier = pltpu.get_barrier_semaphore()

    def device(x, y, c):
        return {"px_0": x, "px_1": y, "px_2": c}

    tables_in = [
        pltpu.make_async_copy(table, spot, table_sem.at[k])
        for k, (table, spot) in enumerate(
            ((counts_hbm, counts_ref), (twist_hbm, twist_y), (y_high_hbm, y_high), (y_low_hbm, y_low))
        )
    ]
    for copy in tables_in:
        copy.start()
    xs = [x] + [lax.rem(x + k, 4) for k in range(1, 4)]
    ys = [y] + [lax.rem(y + k, 4) for k in range(1, 4)]
    js = [j] + [lax.rem(j + k, 8) for k in range(1, 8)]
    column = [(xs[a], ys[b], (c, 1 - c)[d]) for a in range(4) for b in range(4) for d in range(2)][1:]
    for peer in column:
        pl.semaphore_signal(barrier, inc=1, device_id=device(*peer), device_id_type=MESH)
    for k in range(1, 8):
        pl.semaphore_signal(barrier, inc=1, device_id={"py": js[k]}, device_id_type=MESH)
    tables_in[0].wait()
    note[0:1, :] = counts_ref[0, :, 0:TILE].astype(jnp.float32)
    note[1:2, :] = counts_ref[0, :, TILE:].astype(jnp.float32)
    note[2:3, :] = jnp.sum(total_ref[...], axis=0, keepdims=True)
    note[3:8, :] = jnp.zeros((5, TILE), jnp.float32)
    notes[i] = note[...]
    pl.semaphore_wait(barrier, OWNERS - 1 + 7)

    def remote(src, dst, slot, where):
        copy = pltpu.make_async_remote_copy(
            src_ref=src, dst_ref=dst, send_sem=send.at[slot], recv_sem=recv.at[slot],
            device_id=where, device_id_type=MESH,
        )
        copy.start()
        return copy

    chunks = {}
    for k in (8, 9, *range(8)):
        if k < 8:
            refs = (main_ref.at[k], *(r.at[k] for r in (main0, main1, main2, main3, main4)))
        else:
            refs = (rim_ref.at[k - 8], *(r.at[k - 8] for r in (rim0, rim1, rim2, rim3, rim4)))
        chunks[k] = (*refs, k % 4 if k < 8 else 2 * (k - 8))

    def leg(first, kind):
        v = x if first == "x" else y
        if kind == "near":
            low = lax.rem((v + 1) // 2, 2)
            keep, give = (low, 3 - low), (1 - low, 2 + low)
            partner, other = near(v), far(v)
        else:
            low = 2 * (v // 2)
            keep, give = (low, low + 1), (2 - low, 3 - low)
            partner, other = far(v), near(v)
        if first == "x":
            return keep, give, device(partner, y, c), other, device(other, y, c)
        return keep, give, device(x, partner, c), other, device(x, other, c)

    def core_copy(k, src, b0):
        where = device(x, y, 1 - c)
        if k >= 8:
            parts = [(src.at[:, :, 1 - c], b0)]
        else:
            parts = [(src.at[pl.ds(1 - c + 4 * n, 4), c], b0.at[n]) for n in range(4)]
        for one, two in parts:
            pltpu.make_async_remote_copy(
                src_ref=one, dst_ref=two, send_sem=send.at[7 * k], recv_sem=recv.at[7 * k],
                device_id=where, device_id_type=MESH,
            ).start()

    for k, (src, b0, *_) in chunks.items():
        core_copy(k, src, b0)
    pending = {}

    def note_copy(peer, slot, source):
        return pltpu.make_async_remote_copy(
            src_ref=note, dst_ref=notes.at[source], send_sem=note_send.at[slot], recv_sem=note_recv.at[source],
            device_id=device(*peer), device_id_type=MESH,
        )

    for k, peer in enumerate(column):
        note_copy(peer, k, i).start()
    sent = []

    def arrive(k):
        for copy in pending[k]:
            copy.wait_recv()
        sent.extend(pending[k])

    for k, (src, b0, b1, b2, b3, b4, route) in chunks.items():
        pltpu.make_async_copy(b0, b0, recv.at[7 * k]).wait()

        def add0(n, _, src=src, b0=b0, k=k):
            for m in range(4):
                own = src[c + 4 * n + m, 1 - c] if k < 8 else src[n, m, c]
                b0[n, m] = b0[n, m] + own
            return 0

        lax.fori_loop(0, 4, add0, 0)
        first, kind = ROUTES[route]
        _, give, where, _, _ = leg(first, kind)
        pending[k] = []
        for n in range(2):
            block = b0.at[give[n]] if first == "x" else b0.at[:, give[n]]
            pending[k].append(remote(block, b1.at[n], 7 * k + 1 + n, where))

    for k, (src, b0, b1, b2, b3, b4, route) in chunks.items():
        arrive(k)
        first, kind = ROUTES[route]
        keep, _, _, other, where = leg(first, kind)
        for n in range(2):
            for m in range(4):
                at = (keep[n], m) if first == "x" else (m, keep[n])
                b0[at] = b0[at] + b1[n, m]
        block = b0.at[other] if first == "x" else b0.at[:, other]
        pending[k] = [remote(block, b2, 7 * k + 3, where)]

    for k, (src, b0, b1, b2, b3, b4, route) in chunks.items():
        arrive(k)
        first, kind = ROUTES[route]
        for m in range(4):
            at = (x, m) if first == "x" else (m, y)
            b0[at] = b0[at] + b2[m]
        second = "y" if first == "x" else "x"
        _, give, where, _, _ = leg(second, kind)
        pending[k] = []
        for n in range(2):
            block = b0.at[x, give[n]] if first == "x" else b0.at[give[n], y]
            pending[k].append(remote(block, b3.at[n], 7 * k + 4 + n, where))

    for k, (src, b0, b1, b2, b3, b4, route) in chunks.items():
        arrive(k)
        first, kind = ROUTES[route]
        second = "y" if first == "x" else "x"
        keep, _, _, other, where = leg(second, kind)
        for n in range(2):
            at = (x, keep[n]) if first == "x" else (keep[n], y)
            b0[at] = b0[at] + b3[n]
        block = b0.at[x, other] if first == "x" else b0.at[other, y]
        pending[k] = [remote(block, b4, 7 * k + 6, where)]

    for k, peer in enumerate(column):
        copy = note_copy(peer, k, (peer[0] * 4 + peer[1]) * 2 + peer[2])
        copy.wait_send()
        copy.wait_recv()
    everyone = notes[0]
    for k in range(1, OWNERS):
        everyone = everyone + notes[k]
    amount = jnp.broadcast_to(everyone[2:3, :], (8, TILE))
    spare = lax.broadcasted_iota(jnp.int32, (8, TILE), 0) == 4

    def plane_copy(k, source):
        return pltpu.make_async_remote_copy(
            src_ref=pack.at[k], dst_ref=got.at[source], send_sem=py_send.at[k], recv_sem=py_recv.at[source],
            device_id={"py": k}, device_id_type=MESH,
        )

    for k, (src, b0, b1, b2, b3, b4, route) in chunks.items():
        arrive(k)
        block = b0[x, y] + b4[...]
        if k >= 8:
            block = jnp.where(spare, amount, block)
            for p in range(4):
                pack[4 * (k - 8) + p, RX:, :] = block
            continue
        pack[k, 0:RX, :] = block

        @pl.when(k != j)
        def _():
            plane_copy(k, j).start()

        @pl.when(k == j)
        def _():
            got[k] = pack[k]

    earlier = jnp.zeros((8, TILE), jnp.float32)
    for k in range(OWNERS):
        earlier = earlier + jnp.where(k < i, notes[k], 0.0)
    spot = lax.broadcasted_iota(jnp.int32, (8, TILE), 1)
    running = everyone
    for shift in (1, 2, 4, 8, 16, 32, 64):
        running = running + jnp.where(spot >= shift, pltpu.roll(running, shift, 1), 0.0)
    begin = running - everyone + earlier
    whole = jnp.sum(everyone[0:1, :], axis=1, keepdims=True)
    begin_out[0:1, :] = begin[0:1, :]
    begin_out[1:2, :] = begin[1:2, :] + whole
    begin_out[2:8, :] = jnp.zeros((6, TILE), jnp.float32)

    for k in range(1, 8):
        peer = js[k]
        plane_copy(peer, j).wait_send()
        plane_copy(peer, peer).wait_recv()

    for copy in tables_in[1:]:
        copy.wait()
    lane = lax.broadcasted_iota(jnp.int32, (RX, TILE), 1)
    rims = jnp.concatenate([got[s, 32:40, :] for s in range(8)])
    rims = pltpu.roll(rims, (TILE - 32 * (j % 4)) % TILE, 1)
    rims = jnp.concatenate([rims, jnp.zeros((64, TILE), jnp.float32)])
    rims = jnp.transpose(rims)[:RX]
    mass_sum = got[0, 36:37, :]
    for s in range(1, 8):
        mass_sum = mass_sum + got[s, 36:37, :]
    inverse = float(PLANES * NX * NY) / jnp.sum(mass_sum, axis=1, keepdims=True)
    blocks = []
    for s in range(8):
        right = pltpu.roll(rims, (-8 * ((s + 7) % 8)) % TILE, 1)
        left = pltpu.roll(rims, (120 - 8 * ((s + 1) % 8)) % TILE, 1)
        value = got[s, 0:32, :] + jnp.where(lane < 4, right, 0.0) + jnp.where(lane >= 125, left, 0.0)
        blocks.append(value * inverse - 1.0)
    turned = []
    for k, (re, im) in enumerate(real_eighths(blocks)):
        tr, ti = twist_y[0, k : k + 1, :], twist_y[1, k : k + 1, :]
        turned.append(jnp.concatenate([re * tr - im * ti, re * ti + im * tr], axis=1))
    high, low = split_bf16(jnp.concatenate(turned))

    def times(a, b):
        return lax.dot_general(a, b, NT, preferred_element_type=jnp.float32)

    wave = times(y_high[...], low) + times(y_low[...], high) + times(y_high[...], high)
    for h in range(2):
        for k in range(TILE):
            waves[2 * k + h] = wave[2 * k : 2 * k + 2, TILE * h : TILE * h + TILE]

    columns[j * 32 + i] = waves[me]

    cs = [c, 1 - c]
    for a, b, d, e in FAR_FIRST:
        pltpu.make_async_remote_copy(
            src_ref=waves.at[((xs[a] * 4 + ys[b]) * 2 + cs[d]) * 8 + js[e]], dst_ref=columns.at[j * 32 + i],
            send_sem=wave_send, recv_sem=wave_recv,
            device_id={"px_0": xs[a], "px_1": ys[b], "px_2": cs[d], "py": js[e]}, device_id_type=MESH,
        ).start()
    for copy in sent:
        copy.wait_send()
    for k, (src, b0, *_) in chunks.items():
        pltpu.make_async_copy(b0, b0, send.at[7 * k]).wait()
    others = columns.at[pl.ds(0, DEVICES - 1)]
    pltpu.make_async_copy(others, others, wave_recv).wait()
    pltpu.make_async_copy(others, others, wave_send).wait()


def transform(main, rim, total, counts, wave_tables):
    vmem = pl.BlockSpec(memory_space=pltpu.VMEM)
    f32 = jnp.float32

    def both(*lead):
        return [pltpu.VMEM((PLANES, *lead, RX, TILE), f32), pltpu.VMEM((2, *lead, 8, TILE), f32)]

    dma = pltpu.SemaphoreType.DMA
    return pl.pallas_call(
        transform_kernel,
        out_shape=(
            jax.ShapeDtypeStruct((DEVICES, 2, TILE), f32),
            jax.ShapeDtypeStruct((8, TILE), f32),
        ),
        in_specs=[vmem] * 3 + [pl.BlockSpec(memory_space=pltpu.HBM)] * 4,
        out_specs=(vmem, vmem),
        scratch_shapes=[
            pltpu.VMEM((1, 1, 2 * TILE), jnp.int32),
            pltpu.VMEM((2, 8, TILE), f32),
            pltpu.VMEM((2 * TILE, 2 * TILE), jnp.bfloat16),
            pltpu.VMEM((2 * TILE, 2 * TILE), jnp.bfloat16),
            dma((4,)),
            *both(4, 4), *both(2, 4), *both(4), *both(2), *both(),
            pltpu.VMEM((8, TILE), f32),
            pltpu.VMEM((OWNERS, 8, TILE), f32),
            pltpu.VMEM((PLANES, RX + 8, TILE), f32),
            pltpu.VMEM((PLANES, RX + 8, TILE), f32),
            pltpu.VMEM((DEVICES, 2, TILE), f32),
            dma((OWNERS,)), dma((OWNERS,)), dma((70,)), dma((70,)), dma((8,)), dma((8,)), dma, dma,
        ],
        compiler_params=pltpu.CompilerParams(
            collective_id=0, has_side_effects=True, vmem_limit_bytes=24 << 20
        ),
        name="transform",
    )(main, rim, total, *(pltpu.with_memory_space_constraint(a, pltpu.HBM) for a in (counts, *wave_tables)))


def finish_kernel(columns, begin_ref, x_both, x_low, twist_x, out_ref, start_ref):
    start_ref[0, :, 0:TILE] = begin_ref[0:1, :].astype(jnp.int32)
    start_ref[0, :, TILE:] = begin_ref[1:2, :].astype(jnp.int32)
    for g in range(4):
        pair = columns[64 * g : 64 * g + 64].reshape(TILE, TILE)
        high, low = split_bf16(jnp.transpose(pair))
        both = jnp.concatenate([high, low], axis=1)
        sums = jnp.dot(both, x_both[...], preferred_element_type=jnp.float32)
        sums = sums + jnp.dot(high, x_low[...], preferred_element_type=jnp.float32)
        parts = [[], []]
        for p in range(2):
            for w in range(4):
                re_sum = im_sum = None
                for q in range(4):
                    rows = slice(32 * w + 8 * q, 32 * w + 8 * q + 8)
                    re = sums[rows, 256 * p : 256 * p + 128]
                    im = sums[rows, 256 * p + 128 : 256 * p + 256]
                    tr, ti = twist_x[0, 8 * q : 8 * q + 8, :], twist_x[1, 8 * q : 8 * q + 8, :]
                    re_part, im_part = re * tr - im * ti, re * ti + im * tr
                    re_sum = re_part if q == 0 else re_sum + re_part
                    im_sum = im_part if q == 0 else im_sum + im_part
                parts[0].append(re_sum)
                parts[1].append(im_sum)
        re, im = (jnp.transpose(jnp.stack(part), (1, 0, 2)) for part in parts)
        for a, value in enumerate(eighths([(re[k], im[k]) for k in range(8)])):
            for n in range(2):
                for p in range(2):
                    out_ref[n, 2 * g + p, :, TILE * a : TILE * a + TILE] = value[n][4 * p : 4 * p + 4]


def finish(columns, begin, wave_tables):
    vmem = pl.BlockSpec(memory_space=pltpu.VMEM)
    return pl.pallas_call(
        finish_kernel,
        out_shape=(
            jax.ShapeDtypeStruct((2, PLANES, 4, NX), jnp.float32),
            jax.ShapeDtypeStruct((1, 1, 2 * TILE), jnp.int32),
        ),
        in_specs=[vmem] * 5,
        out_specs=(vmem, vmem),
        compiler_params=pltpu.CompilerParams(vmem_limit_bytes=24 << 20),
        name="finish",
    )(columns, begin, *wave_tables)


PX = ("px_0", "px_1", "px_2")
PX_PY = ("px_0", "px_1", "px_2", "py")


def local(cell_ids, offset_x, offset_y, mass, live, tile_owner, counts):
    main, rim, total = spread(tile_owner, cell_ids[0], offset_x[0], offset_y[0], mass[0], live[0])
    y_tables, x_tables = tables()
    columns, begin = transform(
        main.reshape(PLANES, BLOCKS // 2, 2, RX, TILE), rim.reshape(2, 4, 4, 2, 8, TILE), total, counts, y_tables
    )
    return finish(columns, begin, x_tables)


def solution(mesh):
    torus = Mesh(mesh.devices.reshape(4, 4, 2, mesh.shape["py"]), ("px_0", "px_1", "px_2", "py"))
    return jax.shard_map(
        local,
        mesh=torus,
        in_specs=(
            P(PX, "py", None),
            P(PX, "py", None),
            P(PX, "py", None),
            P(PX, "py", None),
            P(PX, "py", None),
            P(PX, "py"),
            P(PX, "py", None),
        ),
        out_specs=(P(None, None, PX_PY, None), P(PX, "py", None)),
        check_vma=False,
    )
```

```python
import functools
import math

import jax
import jax.numpy as jnp
import numpy as np
from jax import lax
from jax.experimental import pallas as pl
from jax.experimental.pallas import tpu as pltpu
from jax.sharding import Mesh
from jax.sharding import PartitionSpec as P

NX = 1024
NY = 1024
PLANES = 8
BETA = 18.4
OWNERS = 32
BLOCKS = OWNERS + 2
RX = 32
TILE = 128
NT = (((1,), (1,)), ((), ()))


def tap_values(step, fraction):
    z = (step.astype(jnp.float32) - fraction) * 0.25
    return jnp.exp(BETA * (jnp.sqrt(1.0 - z * z) - 1.0))


def spread_kernel(
    owner_hbm, cell_hbm, fx_hbm, fy_hbm, mass_hbm, live_hbm,
    main_ref, rim_ref, total_ref,
    owner_ref, cell_ref, fx_ref, fy_ref, mass_ref, live_ref, in_sem,
    rim_acc, lx_s, ly_s, fx_s, fy_s, w_s,
):
    tiles = cell_ref.shape[0]
    sources = (owner_hbm, cell_hbm, fx_hbm, fy_hbm, mass_hbm, live_hbm)
    homes = (owner_ref, cell_ref, fx_ref, fy_ref, mass_ref, live_ref)
    arrivals = [
        pltpu.make_async_copy(source, home, in_sem.at[k]) for k, (source, home) in enumerate(zip(sources, homes))
    ]
    for copy in arrivals:
        copy.start()
    zero = jnp.zeros((8, TILE), jnp.float32)

    def clear(i, _):
        for p in range(PLANES):
            for k in range(RX // 8):
                main_ref[i * PLANES + p, 8 * k : 8 * k + 8, :] = zero
        return 0

    lax.fori_loop(0, BLOCKS, clear, 0)

    def clear_rim(i, _):
        for p in range(8):
            rim_acc[i * 8 + p] = zero
        return 0

    lax.fori_loop(0, OWNERS, clear_rim, 0)

    for copy in arrivals:
        copy.wait()

    def prepare(i, _):
        rows = pl.ds(pl.multiple_of(i * 16, 16), 16)
        cell = cell_ref[rows, :]
        ly_s[rows, :] = cell & 127
        lx_s[rows, :] = (cell >> 7) & 31
        fx_s[rows, :] = fx_ref[rows, :].astype(jnp.float32)
        fy_s[rows, :] = fy_ref[rows, :].astype(jnp.float32)
        w_s[rows, :] = jnp.where(live_ref[rows, :] == 1, mass_ref[rows, :].astype(jnp.float32), 0.0)
        return 0

    lax.fori_loop(0, tiles // 16, prepare, 0)

    sub = lax.broadcasted_iota(jnp.int32, (8, TILE), 0)

    def row(ref, t):
        return jnp.broadcast_to(ref[pl.ds(t, 1), :], (8, TILE))

    def one_tile(t):
        lx, ly = row(lx_s, t), row(ly_s, t)
        jx = (sub - lx + 3) & 7
        jy = (sub - ly + 3) & 7
        tx = tap_values(jx - 3, row(fx_s, t))
        ty = tap_values(jy - 3, row(fy_s, t)) * row(w_s, t)
        gx = (lx + jx + 5) >> 3
        gy = (ly + jy - 3) >> 3
        gy = jnp.where(gy < 0, 16, gy)
        wx = jnp.concatenate([jnp.where(gx == g, tx, 0.0) for g in range(6)]).astype(jnp.bfloat16)
        wy = jnp.concatenate([jnp.where(gy == g, ty, 0.0) for g in range(16)]).astype(jnp.bfloat16)
        wr = jnp.concatenate([jnp.where(gy == 16, ty, 0.0), zero]).astype(jnp.bfloat16)
        main = lax.dot_general(wx, wy, NT, preferred_element_type=jnp.float32)
        rim = lax.dot_general(wr, wx, NT, preferred_element_type=jnp.float32)
        return main, rim[:8]

    unroll = 160

    def add_tiles(i, _):
        results = [one_tile(i * unroll + k) for k in range(unroll)]
        for k in range(unroll):
            owner = owner_ref[0, i * unroll + k]
            plane = cell_ref[pl.ds(i * unroll + k, 1), :][0, 0] >> 12
            bucket = owner * 8 + plane
            main, rim = results[k]
            spot = plane * BLOCKS + owner
            main_ref[spot, 24:32, :] = main_ref[spot, 24:32, :] + main[:8]
            main_ref[spot + 1] = main_ref[spot + 1] + main[8:40]
            main_ref[spot + 2, 0:8, :] = main_ref[spot + 2, 0:8, :] + main[40:]
            rim_acc[bucket, :, :48] = rim_acc[bucket, :, :48] + rim
        return 0

    lax.fori_loop(0, tiles // unroll, add_tiles, 0)

    for p in range(PLANES):
        first, last = p * BLOCKS, p * BLOCKS + OWNERS
        main_ref[last, 24:32, :] = main_ref[last, 24:32, :] + main_ref[first, 24:32, :]
        main_ref[first + 1, 0:8, :] = main_ref[first + 1, 0:8, :] + main_ref[last + 1, 0:8, :]

    lane = lax.broadcasted_iota(jnp.int32, (8, TILE), 1)

    def write_out(i, total):
        parts = [main_ref[p * BLOCKS + i + 1, 8 * k : 8 * k + 8, :] for p in range(PLANES) for k in range(RX // 8)]
        while len(parts) > 1:
            parts = [one + two for one, two in zip(parts[::2], parts[1::2])]
        total = total + parts[0]
        before, after = (i + OWNERS - 1) % OWNERS, (i + 1) % OWNERS
        for q in range(2):
            out = zero
            for k in range(4):
                p = 4 * q + k
                own = pltpu.roll(rim_acc[i * 8 + p], (32 * k - 8) % 128, 1)
                low = pltpu.roll(rim_acc[before * 8 + p], (32 * k - 40) % 128, 1)
                high = pltpu.roll(rim_acc[after * 8 + p], (32 * k + 24) % 128, 1)
                spot = lane - 32 * k
                out = jnp.where((spot >= 0) & (spot < 32), own, out)
                out = out + jnp.where((spot >= 0) & (spot < 8), low, 0.0)
                out = out + jnp.where((spot >= 24) & (spot < 32), high, 0.0)
            rim_ref[q, i // 2, i % 2] = out
            total = total + out
        return total

    total_ref[...] = lax.fori_loop(0, OWNERS, write_out, zero, unroll=8)


def spread(owners, cells, fx, fy, mass, live):
    tiles = cells.shape[0]
    vmem = pl.BlockSpec(memory_space=pltpu.VMEM)
    return pl.pallas_call(
        spread_kernel,
        out_shape=(
            jax.ShapeDtypeStruct((PLANES * BLOCKS, RX, TILE), jnp.float32),
            jax.ShapeDtypeStruct((2, 16, 2, 8, TILE), jnp.float32),
            jax.ShapeDtypeStruct((8, TILE), jnp.float32),
        ),
        in_specs=[pl.BlockSpec(memory_space=pltpu.HBM)] * 6,
        out_specs=(vmem, vmem, vmem),
        scratch_shapes=[
            pltpu.SMEM((1, tiles), jnp.int32),
            pltpu.VMEM((tiles, TILE), jnp.int32),
            pltpu.VMEM((tiles, TILE), jnp.bfloat16),
            pltpu.VMEM((tiles, TILE), jnp.bfloat16),
            pltpu.VMEM((tiles, TILE), jnp.bfloat16),
            pltpu.VMEM((tiles, TILE), jnp.int32),
            pltpu.SemaphoreType.DMA((6,)),
            pltpu.VMEM((OWNERS * PLANES, 8, TILE), jnp.float32),
            pltpu.VMEM((tiles, TILE), jnp.int32),
            pltpu.VMEM((tiles, TILE), jnp.int32),
            pltpu.VMEM((tiles, TILE), jnp.float32),
            pltpu.VMEM((tiles, TILE), jnp.float32),
            pltpu.VMEM((tiles, TILE), jnp.float32),
        ],
        compiler_params=pltpu.CompilerParams(vmem_limit_bytes=24 << 20),
        name="spread",
    )(*(pltpu.with_memory_space_constraint(a, pltpu.HBM) for a in (owners, cells, fx, fy, mass, live)))


COORDS = ("px_0", "px_1", "px_2")
DEVICES = 256


def split_bf16(value):
    high = value.astype(jnp.bfloat16)
    return high, (value - high.astype(jnp.float32)).astype(jnp.bfloat16)


def np_split(value):
    high = np.asarray(value, np.float32).astype(jnp.bfloat16)
    low = (np.asarray(value, np.float64) - high.astype(np.float64)).astype(jnp.bfloat16)
    return high, low


def tables():
    k = np.arange(TILE)
    turn_y = 2 * np.pi / NY * (np.arange(8)[:, None] * k[None, :])
    twist_y = np.stack([np.cos(turn_y), -np.sin(turn_y)]).astype(np.float32)
    theta = 2 * np.pi / TILE * (k[:, None] * k[None, :] % TILE)
    wave_y = np.zeros((TILE, 2, 2, TILE))
    wave_y[:, 0, 0], wave_y[:, 0, 1] = np.cos(theta), np.sin(theta)
    wave_y[:, 1, 0], wave_y[:, 1, 1] = -np.sin(theta), np.cos(theta)
    y_high, y_low = np_split(wave_y.reshape(2 * TILE, 2 * TILE))
    phase = 2 * np.pi / OWNERS * (np.arange(OWNERS)[:, None] * k[None, :] % OWNERS)
    block = np.zeros((OWNERS, 2, 2, TILE))
    block[:, 0, 0], block[:, 1, 0] = np.cos(phase), np.sin(phase)
    block[:, 0, 1], block[:, 1, 1] = -np.sin(phase), np.cos(phase)
    wave_x = np.kron(np.eye(2), block.reshape(2 * OWNERS, 2 * TILE))
    x_high, x_low = np_split(wave_x)
    turn_x = 2 * np.pi / NX * (np.arange(RX)[:, None] * k[None, :])
    scale = 1.0 / math.sqrt(NX * NY)
    twist_x = (scale * np.stack([np.cos(turn_x), -np.sin(turn_x)])).astype(np.float32)
    return (twist_y, y_high, y_low), (np.concatenate([x_high, x_high]), x_low, twist_x)


HALF = math.sqrt(0.5)


def real_eighths(d):
    s = [d[k] + d[k + 4] for k in range(4)]
    e = [d[k] - d[k + 4] for k in range(4)]
    near_sum, far_sum = s[0] + s[2], s[1] + s[3]
    a0, a4 = near_sum + far_sum, near_sum - far_sum
    re2, im2 = s[0] - s[2], s[3] - s[1]
    tilt, lean = (e[1] - e[3]) * HALF, (e[1] + e[3]) * HALF
    re1, im1 = e[0] + tilt, -e[2] - lean
    re3, im3 = e[0] - tilt, e[2] - lean
    zero = jnp.zeros_like(a0)
    return [(a0, zero), (re1, im1), (re2, im2), (re3, im3), (a4, zero), (re3, -im3), (re2, -im2), (re1, -im1)]


def fourths(t):
    def add(p, q):
        return p[0] + q[0], p[1] + q[1]

    def less(p, q):
        return p[0] - q[0], p[1] - q[1]

    e0, e1 = add(t[0], t[2]), less(t[0], t[2])
    f0, g = add(t[1], t[3]), less(t[1], t[3])
    f1 = (g[1], -g[0])
    return [add(e0, f0), add(e1, f1), less(e0, f0), less(e1, f1)]


def eighths(z):
    s = [(z[k][0] + z[k + 4][0], z[k][1] + z[k + 4][1]) for k in range(4)]
    d = [(z[k][0] - z[k + 4][0], z[k][1] - z[k + 4][1]) for k in range(4)]
    turned = [
        d[0],
        ((d[1][0] + d[1][1]) * HALF, (d[1][1] - d[1][0]) * HALF),
        (d[2][1], -d[2][0]),
        ((d[3][1] - d[3][0]) * HALF, -(d[3][0] + d[3][1]) * HALF),
    ]
    even, odd = fourths(s), fourths(turned)
    return [even[0], odd[0], even[1], odd[1], even[2], odd[2], even[3], odd[3]]


def near(v):
    return v + 1 - 2 * lax.rem(v, 2)


def far(v):
    return 3 - v


ROUTES = (("x", "near"), ("x", "far"), ("y", "near"), ("y", "far"))
MESH = pl.DeviceIdType.MESH


def hops(offset):
    a, b, d, e = offset
    return min(a, 4 - a) + min(b, 4 - b) + min(e, 8 - e)


FAR_FIRST = sorted(
    ((a, b, d, e) for a in range(4) for b in range(4) for e in range(8) for d in range(2) if (a, b, d, e) != (0, 0, 0, 0)),
    key=lambda o: (-hops(o), (7 * o[0] + 3 * o[1] + 5 * o[3]) % 11),
)


def transform_kernel(
    main_ref, rim_ref, total_ref, counts_hbm, twist_hbm, y_high_hbm, y_low_hbm,
    columns, begin_out,
    counts_ref, twist_y, y_high, y_low, table_sem,
    main0, rim0, main1, rim1, main2, rim2, main3, rim3, main4, rim4,
    tally, inbox, pack, got, waves,
    z_sem, note_send, note_recv, send, recv, py_send, py_recv, wave_send, wave_recv,
):
    x, y, c = (lax.axis_index(a) for a in COORDS)
    j = lax.axis_index("py")
    i = (x * 4 + y) * 2 + c
    me = i * 8 + j
    barrier = pltpu.get_barrier_semaphore()

    def device(x, y, c):
        return {"px_0": x, "px_1": y, "px_2": c}

    tables_in = [
        pltpu.make_async_copy(table, spot, table_sem.at[k])
        for k, (table, spot) in enumerate(
            ((counts_hbm, counts_ref), (twist_hbm, twist_y), (y_high_hbm, y_high), (y_low_hbm, y_low))
        )
    ]
    for copy in tables_in:
        copy.start()
    xs = [x] + [lax.rem(x + k, 4) for k in range(1, 4)]
    ys = [y] + [lax.rem(y + k, 4) for k in range(1, 4)]
    js = [j] + [lax.rem(j + k, 8) for k in range(1, 8)]
    kin = [
        (device(x, y, 1 - c), c == 1),
        (device(x, near(y), c), lax.rem(y, 2) == 1),
        (device(x, far(y), c), y >= 2),
        (device(near(x), y, c), lax.rem(x, 2) == 1),
        (device(far(x), y, c), x >= 2),
    ]
    above, below = {"py": js[1]}, {"py": js[7]}
    for peer in (*(peer for peer, _ in kin), above, below):
        pl.semaphore_signal(barrier, inc=1, device_id=peer, device_id_type=MESH)
    tables_in[0].wait()
    tally[0, 0:1, :] = counts_ref[0, :, 0:TILE].astype(jnp.float32)
    tally[0, 1:2, :] = counts_ref[0, :, TILE:].astype(jnp.float32)
    tally[0, 2:3, :] = jnp.sum(total_ref[...], axis=0, keepdims=True)
    tally[0, 3:8, :] = jnp.zeros((5, TILE), jnp.float32)
    pl.semaphore_wait(barrier, 7)

    def tell(n):
        if n < 3:
            pl.semaphore_signal(z_sem.at[n, 0], inc=1, device_id=above, device_id_type=MESH)
            pl.semaphore_signal(z_sem.at[n, 1], inc=1, device_id=below, device_id_type=MESH)
        copy = pltpu.make_async_remote_copy(
            src_ref=tally.at[n], dst_ref=inbox.at[n], send_sem=note_send.at[n], recv_sem=note_recv.at[n],
            device_id=kin[n][0], device_id_type=MESH,
        )
        copy.start()
        told.append(copy)

    def hear(n):
        if n < 3:
            pl.semaphore_wait(z_sem.at[n, 0], 1)
            pl.semaphore_wait(z_sem.at[n, 1], 1)
        told[n].wait_recv()
        tally[n + 1] = tally[n] + inbox[n]

    sent, told = [], []
    tell(0)

    def remote(src, dst, slot, where):
        copy = pltpu.make_async_remote_copy(
            src_ref=src, dst_ref=dst, send_sem=send.at[slot], recv_sem=recv.at[slot],
            device_id=where, device_id_type=MESH,
        )
        copy.start()
        return copy

    chunks = {}
    for k in (8, 9, *range(8)):
        if k < 8:
            refs = (main_ref.at[k], *(r.at[k] for r in (main0, main1, main2, main3, main4)))
        else:
            refs = (rim_ref.at[k - 8], *(r.at[k - 8] for r in (rim0, rim1, rim2, rim3, rim4)))
        chunks[k] = (*refs, k % 4 if k < 8 else 2 * (k - 8))

    def leg(first, kind):
        v = x if first == "x" else y
        if kind == "near":
            low = lax.rem((v + 1) // 2, 2)
            keep, give = (low, 3 - low), (1 - low, 2 + low)
            partner, other = near(v), far(v)
        else:
            low = 2 * (v // 2)
            keep, give = (low, low + 1), (2 - low, 3 - low)
            partner, other = far(v), near(v)
        if first == "x":
            return keep, give, device(partner, y, c), other, device(other, y, c)
        return keep, give, device(x, partner, c), other, device(x, other, c)

    def core_copy(k, src, b0):
        where = device(x, y, 1 - c)
        if k >= 8:
            parts = [(src.at[:, :, 1 - c], b0)]
        else:
            parts = [(src.at[pl.ds(1 - c + 4 * n, 4), c], b0.at[n]) for n in range(4)]
        for one, two in parts:
            pltpu.make_async_remote_copy(
                src_ref=one, dst_ref=two, send_sem=send.at[7 * k], recv_sem=recv.at[7 * k],
                device_id=where, device_id_type=MESH,
            ).start()

    for k, (src, b0, *_) in chunks.items():
        core_copy(k, src, b0)
    pending = {}

    hear(0)
    tell(1)

    def arrive(k):
        for copy in pending[k]:
            copy.wait_recv()
        sent.extend(pending[k])

    for k, (src, b0, b1, b2, b3, b4, route) in chunks.items():
        pltpu.make_async_copy(b0, b0, recv.at[7 * k]).wait()

        def add0(n, _, src=src, b0=b0, k=k):
            for m in range(4):
                own = src[c + 4 * n + m, 1 - c] if k < 8 else src[n, m, c]
                b0[n, m] = b0[n, m] + own
            return 0

        lax.fori_loop(0, 4, add0, 0)
        first, kind = ROUTES[route]
        _, give, where, _, _ = leg(first, kind)
        pending[k] = []
        for n in range(2):
            block = b0.at[give[n]] if first == "x" else b0.at[:, give[n]]
            pending[k].append(remote(block, b1.at[n], 7 * k + 1 + n, where))

    hear(1)
    tell(2)
    for k, (src, b0, b1, b2, b3, b4, route) in chunks.items():
        arrive(k)
        first, kind = ROUTES[route]
        keep, _, _, other, where = leg(first, kind)
        for n in range(2):
            for m in range(4):
                at = (keep[n], m) if first == "x" else (m, keep[n])
                b0[at] = b0[at] + b1[n, m]
        block = b0.at[other] if first == "x" else b0.at[:, other]
        pending[k] = [remote(block, b2, 7 * k + 3, where)]

    hear(2)
    tell(3)
    for k, (src, b0, b1, b2, b3, b4, route) in chunks.items():
        arrive(k)
        first, kind = ROUTES[route]
        for m in range(4):
            at = (x, m) if first == "x" else (m, y)
            b0[at] = b0[at] + b2[m]
        second = "y" if first == "x" else "x"
        _, give, where, _, _ = leg(second, kind)
        pending[k] = []
        for n in range(2):
            block = b0.at[x, give[n]] if first == "x" else b0.at[give[n], y]
            pending[k].append(remote(block, b3.at[n], 7 * k + 4 + n, where))

    hear(3)
    tell(4)
    for k, (src, b0, b1, b2, b3, b4, route) in chunks.items():
        arrive(k)
        first, kind = ROUTES[route]
        second = "y" if first == "x" else "x"
        keep, _, _, other, where = leg(second, kind)
        for n in range(2):
            at = (x, keep[n]) if first == "x" else (keep[n], y)
            b0[at] = b0[at] + b3[n]
        block = b0.at[x, other] if first == "x" else b0.at[other, y]
        pending[k] = [remote(block, b4, 7 * k + 6, where)]

    hear(4)
    everyone = tally[5]
    amount = jnp.broadcast_to(everyone[2:3, :], (8, TILE))
    spare = lax.broadcasted_iota(jnp.int32, (8, TILE), 0) == 4

    def plane_copy(k, source):
        return pltpu.make_async_remote_copy(
            src_ref=pack.at[k], dst_ref=got.at[source], send_sem=py_send.at[k], recv_sem=py_recv.at[source],
            device_id={"py": k}, device_id_type=MESH,
        )

    for k, (src, b0, b1, b2, b3, b4, route) in chunks.items():
        arrive(k)
        block = b0[x, y] + b4[...]
        if k >= 8:
            block = jnp.where(spare, amount, block)
            for p in range(4):
                pack[4 * (k - 8) + p, RX:, :] = block
            continue
        pack[k, 0:RX, :] = block

        @pl.when(k != j)
        def _():
            plane_copy(k, j).start()

        @pl.when(k == j)
        def _():
            got[k] = pack[k]

    earlier = jnp.zeros((8, TILE), jnp.float32)
    for n, (_, lower) in enumerate(kin):
        earlier = earlier + jnp.where(lower, inbox[n], 0.0)
    spot = lax.broadcasted_iota(jnp.int32, (8, TILE), 1)
    running = everyone
    for shift in (1, 2, 4, 8, 16, 32, 64):
        running = running + jnp.where(spot >= shift, pltpu.roll(running, shift, 1), 0.0)
    begin = running - everyone + earlier
    whole = jnp.sum(everyone[0:1, :], axis=1, keepdims=True)
    begin_out[0:1, :] = begin[0:1, :]
    begin_out[1:2, :] = begin[1:2, :] + whole
    begin_out[2:8, :] = jnp.zeros((6, TILE), jnp.float32)

    for k in range(1, 8):
        peer = js[k]
        plane_copy(peer, j).wait_send()
        plane_copy(peer, peer).wait_recv()

    for copy in tables_in[1:]:
        copy.wait()
    lane = lax.broadcasted_iota(jnp.int32, (RX, TILE), 1)
    rims = jnp.concatenate([got[s, 32:40, :] for s in range(8)])
    rims = pltpu.roll(rims, (TILE - 32 * (j % 4)) % TILE, 1)
    rims = jnp.concatenate([rims, jnp.zeros((64, TILE), jnp.float32)])
    rims = jnp.transpose(rims)[:RX]
    mass_sum = got[0, 36:37, :]
    for s in range(1, 8):
        mass_sum = mass_sum + got[s, 36:37, :]
    inverse = float(PLANES * NX * NY) / jnp.sum(mass_sum, axis=1, keepdims=True)
    blocks = []
    for s in range(8):
        right = pltpu.roll(rims, (-8 * ((s + 7) % 8)) % TILE, 1)
        left = pltpu.roll(rims, (120 - 8 * ((s + 1) % 8)) % TILE, 1)
        value = got[s, 0:32, :] + jnp.where(lane < 4, right, 0.0) + jnp.where(lane >= 125, left, 0.0)
        blocks.append(value * inverse - 1.0)
    turned = []
    for k, (re, im) in enumerate(real_eighths(blocks)):
        tr, ti = twist_y[0, k : k + 1, :], twist_y[1, k : k + 1, :]
        turned.append(jnp.concatenate([re * tr - im * ti, re * ti + im * tr], axis=1))
    high, low = split_bf16(jnp.concatenate(turned))

    def times(a, b):
        return lax.dot_general(a, b, NT, preferred_element_type=jnp.float32)

    wave = times(y_high[...], low) + times(y_low[...], high) + times(y_high[...], high)
    for h in range(2):
        for k in range(TILE):
            waves[2 * k + h] = wave[2 * k : 2 * k + 2, TILE * h : TILE * h + TILE]

    columns[j * 32 + i] = waves[me]

    cs = [c, 1 - c]
    for a, b, d, e in FAR_FIRST:
        pltpu.make_async_remote_copy(
            src_ref=waves.at[((xs[a] * 4 + ys[b]) * 2 + cs[d]) * 8 + js[e]], dst_ref=columns.at[j * 32 + i],
            send_sem=wave_send, recv_sem=wave_recv,
            device_id={"px_0": xs[a], "px_1": ys[b], "px_2": cs[d], "py": js[e]}, device_id_type=MESH,
        ).start()
    for copy in (*sent, *told):
        copy.wait_send()
    for k, (src, b0, *_) in chunks.items():
        pltpu.make_async_copy(b0, b0, send.at[7 * k]).wait()
    others = columns.at[pl.ds(0, DEVICES - 1)]
    pltpu.make_async_copy(others, others, wave_recv).wait()
    pltpu.make_async_copy(others, others, wave_send).wait()


def transform(main, rim, total, counts, wave_tables):
    vmem = pl.BlockSpec(memory_space=pltpu.VMEM)
    f32 = jnp.float32

    def both(*lead):
        return [pltpu.VMEM((PLANES, *lead, RX, TILE), f32), pltpu.VMEM((2, *lead, 8, TILE), f32)]

    dma = pltpu.SemaphoreType.DMA
    return pl.pallas_call(
        transform_kernel,
        out_shape=(
            jax.ShapeDtypeStruct((DEVICES, 2, TILE), f32),
            jax.ShapeDtypeStruct((8, TILE), f32),
        ),
        in_specs=[vmem] * 3 + [pl.BlockSpec(memory_space=pltpu.HBM)] * 4,
        out_specs=(vmem, vmem),
        scratch_shapes=[
            pltpu.VMEM((1, 1, 2 * TILE), jnp.int32),
            pltpu.VMEM((2, 8, TILE), f32),
            pltpu.VMEM((2 * TILE, 2 * TILE), jnp.bfloat16),
            pltpu.VMEM((2 * TILE, 2 * TILE), jnp.bfloat16),
            dma((4,)),
            *both(4, 4), *both(2, 4), *both(4), *both(2), *both(),
            pltpu.VMEM((6, 8, TILE), f32),
            pltpu.VMEM((5, 8, TILE), f32),
            pltpu.VMEM((PLANES, RX + 8, TILE), f32),
            pltpu.VMEM((PLANES, RX + 8, TILE), f32),
            pltpu.VMEM((DEVICES, 2, TILE), f32),
            pltpu.SemaphoreType.REGULAR((3, 2)), dma((5,)), dma((5,)), dma((70,)), dma((70,)), dma((8,)), dma((8,)), dma, dma,
        ],
        compiler_params=pltpu.CompilerParams(
            collective_id=0, has_side_effects=True, vmem_limit_bytes=24 << 20
        ),
        name="transform",
    )(main, rim, total, *(pltpu.with_memory_space_constraint(a, pltpu.HBM) for a in (counts, *wave_tables)))


def finish_kernel(columns, begin_ref, x_both, x_low, twist_x, out_ref, start_ref):
    start_ref[0, :, 0:TILE] = begin_ref[0:1, :].astype(jnp.int32)
    start_ref[0, :, TILE:] = begin_ref[1:2, :].astype(jnp.int32)
    for g in range(4):
        pair = columns[64 * g : 64 * g + 64].reshape(TILE, TILE)
        high, low = split_bf16(jnp.transpose(pair))
        both = jnp.concatenate([high, low], axis=1)
        sums = jnp.dot(both, x_both[...], preferred_element_type=jnp.float32)
        sums = sums + jnp.dot(high, x_low[...], preferred_element_type=jnp.float32)
        parts = [[], []]
        for p in range(2):
            for w in range(4):
                re_sum = im_sum = None
                for q in range(4):
                    rows = slice(32 * w + 8 * q, 32 * w + 8 * q + 8)
                    re = sums[rows, 256 * p : 256 * p + 128]
                    im = sums[rows, 256 * p + 128 : 256 * p + 256]
                    tr, ti = twist_x[0, 8 * q : 8 * q + 8, :], twist_x[1, 8 * q : 8 * q + 8, :]
                    re_part, im_part = re * tr - im * ti, re * ti + im * tr
                    re_sum = re_part if q == 0 else re_sum + re_part
                    im_sum = im_part if q == 0 else im_sum + im_part
                parts[0].append(re_sum)
                parts[1].append(im_sum)
        re, im = (jnp.transpose(jnp.stack(part), (1, 0, 2)) for part in parts)
        for a, value in enumerate(eighths([(re[k], im[k]) for k in range(8)])):
            for n in range(2):
                for p in range(2):
                    out_ref[n, 2 * g + p, :, TILE * a : TILE * a + TILE] = value[n][4 * p : 4 * p + 4]


def finish(columns, begin, wave_tables):
    vmem = pl.BlockSpec(memory_space=pltpu.VMEM)
    return pl.pallas_call(
        finish_kernel,
        out_shape=(
            jax.ShapeDtypeStruct((2, PLANES, 4, NX), jnp.float32),
            jax.ShapeDtypeStruct((1, 1, 2 * TILE), jnp.int32),
        ),
        in_specs=[vmem] * 5,
        out_specs=(vmem, vmem),
        compiler_params=pltpu.CompilerParams(vmem_limit_bytes=24 << 20),
        name="finish",
    )(columns, begin, *wave_tables)


PX = ("px_0", "px_1", "px_2")
PX_PY = ("px_0", "px_1", "px_2", "py")


def local(cell_ids, offset_x, offset_y, mass, live, tile_owner, counts):
    main, rim, total = spread(tile_owner, cell_ids[0], offset_x[0], offset_y[0], mass[0], live[0])
    y_tables, x_tables = tables()
    columns, begin = transform(
        main.reshape(PLANES, BLOCKS // 2, 2, RX, TILE), rim.reshape(2, 4, 4, 2, 8, TILE), total, counts, y_tables
    )
    return finish(columns, begin, x_tables)


def solution(mesh):
    torus = Mesh(mesh.devices.reshape(4, 4, 2, mesh.shape["py"]), ("px_0", "px_1", "px_2", "py"))
    return jax.shard_map(
        local,
        mesh=torus,
        in_specs=(
            P(PX, "py", None),
            P(PX, "py", None),
            P(PX, "py", None),
            P(PX, "py", None),
            P(PX, "py", None),
            P(PX, "py"),
            P(PX, "py", None),
        ),
        out_specs=(P(None, None, PX_PY, None), P(PX, "py", None)),
        check_vma=False,
    )
```

```python
import functools
import math

import jax
import jax.numpy as jnp
import numpy as np
from jax import lax
from jax.experimental import pallas as pl
from jax.experimental.pallas import tpu as pltpu
from jax.sharding import Mesh
from jax.sharding import PartitionSpec as P

NX = 1024
NY = 1024
PLANES = 8
BETA = 18.4
OWNERS = 32
BLOCKS = OWNERS + 2
RX = 32
TILE = 128
NT = (((1,), (1,)), ((), ()))


def tap_values(step, fraction):
    z = (step.astype(jnp.float32) - fraction) * 0.25
    return jnp.exp(BETA * (jnp.sqrt(1.0 - z * z) - 1.0))


def spread_kernel(
    owner_hbm, cell_hbm, fx_hbm, fy_hbm, mass_hbm, live_hbm,
    main_ref, rim_ref, total_ref,
    owner_ref, cell_ref, fx_ref, fy_ref, mass_ref, live_ref, in_sem,
    rim_acc, lx_s, ly_s, fx_s, fy_s, w_s,
):
    tiles = cell_ref.shape[0]
    sources = (owner_hbm, cell_hbm, fx_hbm, fy_hbm, mass_hbm, live_hbm)
    homes = (owner_ref, cell_ref, fx_ref, fy_ref, mass_ref, live_ref)
    arrivals = [
        pltpu.make_async_copy(source, home, in_sem.at[k]) for k, (source, home) in enumerate(zip(sources, homes))
    ]
    for copy in arrivals:
        copy.start()
    zero = jnp.zeros((8, TILE), jnp.float32)

    def clear(i, _):
        for p in range(PLANES):
            for k in range(RX // 8):
                main_ref[i * PLANES + p, 8 * k : 8 * k + 8, :] = zero
        for k in range(RX // 8):
            rim_acc[i, 8 * k : 8 * k + 8, :] = zero
        return 0

    lax.fori_loop(0, BLOCKS, clear, 0)

    for copy in arrivals:
        copy.wait()

    def prepare(i, _):
        rows = pl.ds(pl.multiple_of(i * 16, 16), 16)
        cell = cell_ref[rows, :]
        ly_s[rows, :] = cell & 127
        lx_s[rows, :] = (cell >> 7) & 31
        fx_s[rows, :] = fx_ref[rows, :].astype(jnp.float32)
        fy_s[rows, :] = fy_ref[rows, :].astype(jnp.float32)
        w_s[rows, :] = jnp.where(live_ref[rows, :] == 1, mass_ref[rows, :].astype(jnp.float32), 0.0)
        return 0

    lax.fori_loop(0, tiles // 16, prepare, 0)

    sub = lax.broadcasted_iota(jnp.int32, (8, TILE), 0)

    def row(ref, t):
        return jnp.broadcast_to(ref[pl.ds(t, 1), :], (8, TILE))

    def one_tile(t):
        lx, ly = row(lx_s, t), row(ly_s, t)
        jx = (sub - lx + 3) & 7
        jy = (sub - ly + 3) & 7
        tx = tap_values(jx - 3, row(fx_s, t))
        ty = tap_values(jy - 3, row(fy_s, t)) * row(w_s, t)
        gx = (lx + jx + 5) >> 3
        gy = (ly + jy - 3) >> 3
        gy = jnp.where(gy < 0, 16, gy)
        wx = jnp.concatenate([jnp.where(gx == g, tx, 0.0) for g in range(6)]).astype(jnp.bfloat16)
        wy = jnp.concatenate([*(jnp.where(gy == g, ty, 0.0) for g in range(17)), zero]).astype(jnp.bfloat16)
        return lax.dot_general(wx, wy, NT, preferred_element_type=jnp.float32)

    blank = jnp.zeros((48, TILE - 8), jnp.float32)

    unroll = 320

    def add_tiles(i, _):
        results = [one_tile(i * unroll + k) for k in range(unroll)]
        for k in range(unroll):
            owner = owner_ref[0, i * unroll + k]
            plane = cell_ref[pl.ds(i * unroll + k, 1), :][0, 0] >> 12
            main, rim = results[k][:, :TILE], results[k][:, TILE : TILE + 8]
            rim = pltpu.roll(jnp.concatenate([rim, blank], axis=1), 8 * plane, 1)
            for blocks, spot, part in ((main_ref, plane * BLOCKS + owner, main), (rim_acc, owner, rim)):
                blocks[spot, 24:32, :] = blocks[spot, 24:32, :] + part[:8]
                blocks[spot + 1] = blocks[spot + 1] + part[8:40]
                blocks[spot + 2, 0:8, :] = blocks[spot + 2, 0:8, :] + part[40:]
        return 0

    lax.fori_loop(0, tiles // unroll, add_tiles, 0)

    for blocks, start in ((rim_acc, 0), *((main_ref, p * BLOCKS) for p in range(PLANES))):
        first, last = start, start + OWNERS
        blocks[last, 24:32, :] = blocks[last, 24:32, :] + blocks[first, 24:32, :]
        blocks[first + 1, 0:8, :] = blocks[first + 1, 0:8, :] + blocks[last + 1, 0:8, :]

    def write_out(i, total):
        parts = [main_ref[p * BLOCKS + i + 1, 8 * k : 8 * k + 8, :] for p in range(PLANES) for k in range(RX // 8)]
        while len(parts) > 1:
            parts = [one + two for one, two in zip(parts[::2], parts[1::2])]
        total = total + parts[0]
        for q in range(2):
            near_rows, far_rows = rim_acc[i + 1, 8 * q : 8 * q + 8, :], rim_acc[i + 1, 8 * q + 16 : 8 * q + 24, :]
            out = near_rows + pltpu.roll(far_rows, 64, 1)
            rim_ref[q, i // 2, i % 2] = out
            total = total + out
        return total

    total_ref[...] = lax.fori_loop(0, OWNERS, write_out, zero, unroll=8)


def spread(owners, cells, fx, fy, mass, live):
    tiles = cells.shape[0]
    vmem = pl.BlockSpec(memory_space=pltpu.VMEM)
    return pl.pallas_call(
        spread_kernel,
        out_shape=(
            jax.ShapeDtypeStruct((PLANES * BLOCKS, RX, TILE), jnp.float32),
            jax.ShapeDtypeStruct((2, 16, 2, 8, TILE), jnp.float32),
            jax.ShapeDtypeStruct((8, TILE), jnp.float32),
        ),
        in_specs=[pl.BlockSpec(memory_space=pltpu.HBM)] * 6,
        out_specs=(vmem, vmem, vmem),
        scratch_shapes=[
            pltpu.SMEM((1, tiles), jnp.int32),
            pltpu.VMEM((tiles, TILE), jnp.int32),
            pltpu.VMEM((tiles, TILE), jnp.bfloat16),
            pltpu.VMEM((tiles, TILE), jnp.bfloat16),
            pltpu.VMEM((tiles, TILE), jnp.bfloat16),
            pltpu.VMEM((tiles, TILE), jnp.int32),
            pltpu.SemaphoreType.DMA((6,)),
            pltpu.VMEM((BLOCKS, RX, TILE), jnp.float32),
            pltpu.VMEM((tiles, TILE), jnp.int32),
            pltpu.VMEM((tiles, TILE), jnp.int32),
            pltpu.VMEM((tiles, TILE), jnp.float32),
            pltpu.VMEM((tiles, TILE), jnp.float32),
            pltpu.VMEM((tiles, TILE), jnp.float32),
        ],
        compiler_params=pltpu.CompilerParams(vmem_limit_bytes=24 << 20),
        name="spread",
    )(*(pltpu.with_memory_space_constraint(a, pltpu.HBM) for a in (owners, cells, fx, fy, mass, live)))


COORDS = ("px_0", "px_1", "px_2")
DEVICES = 256


def split_bf16(value):
    high = value.astype(jnp.bfloat16)
    return high, (value - high.astype(jnp.float32)).astype(jnp.bfloat16)


def np_split(value):
    high = np.asarray(value, np.float32).astype(jnp.bfloat16)
    low = (np.asarray(value, np.float64) - high.astype(np.float64)).astype(jnp.bfloat16)
    return high, low


def tables():
    k = np.arange(TILE)
    turn_y = 2 * np.pi / NY * (np.arange(8)[:, None] * k[None, :])
    twist_y = np.stack([np.cos(turn_y), -np.sin(turn_y)]).astype(np.float32)
    theta = 2 * np.pi / TILE * (k[:, None] * k[None, :] % TILE)
    wave_y = np.zeros((TILE, 2, 2, TILE))
    wave_y[:, 0, 0], wave_y[:, 0, 1] = np.cos(theta), np.sin(theta)
    wave_y[:, 1, 0], wave_y[:, 1, 1] = -np.sin(theta), np.cos(theta)
    y_high, y_low = np_split(wave_y.reshape(2 * TILE, 2 * TILE))
    phase = 2 * np.pi / OWNERS * (np.arange(OWNERS)[:, None] * k[None, :] % OWNERS)
    block = np.zeros((OWNERS, 2, 2, TILE))
    block[:, 0, 0], block[:, 1, 0] = np.cos(phase), np.sin(phase)
    block[:, 0, 1], block[:, 1, 1] = -np.sin(phase), np.cos(phase)
    wave_x = np.kron(np.eye(2), block.reshape(2 * OWNERS, 2 * TILE))
    x_high, x_low = np_split(wave_x)
    turn_x = 2 * np.pi / NX * (np.arange(RX)[:, None] * k[None, :])
    scale = 1.0 / math.sqrt(NX * NY)
    twist_x = (scale * np.stack([np.cos(turn_x), -np.sin(turn_x)])).astype(np.float32)
    return (twist_y, y_high, y_low), (np.concatenate([x_high, x_high]), x_low, twist_x)


HALF = math.sqrt(0.5)


def real_eighths(d):
    s = [d[k] + d[k + 4] for k in range(4)]
    e = [d[k] - d[k + 4] for k in range(4)]
    near_sum, far_sum = s[0] + s[2], s[1] + s[3]
    a0, a4 = near_sum + far_sum, near_sum - far_sum
    re2, im2 = s[0] - s[2], s[3] - s[1]
    tilt, lean = (e[1] - e[3]) * HALF, (e[1] + e[3]) * HALF
    re1, im1 = e[0] + tilt, -e[2] - lean
    re3, im3 = e[0] - tilt, e[2] - lean
    zero = jnp.zeros_like(a0)
    return [(a0, zero), (re1, im1), (re2, im2), (re3, im3), (a4, zero), (re3, -im3), (re2, -im2), (re1, -im1)]


def fourths(t):
    def add(p, q):
        return p[0] + q[0], p[1] + q[1]

    def less(p, q):
        return p[0] - q[0], p[1] - q[1]

    e0, e1 = add(t[0], t[2]), less(t[0], t[2])
    f0, g = add(t[1], t[3]), less(t[1], t[3])
    f1 = (g[1], -g[0])
    return [add(e0, f0), add(e1, f1), less(e0, f0), less(e1, f1)]


def eighths(z):
    s = [(z[k][0] + z[k + 4][0], z[k][1] + z[k + 4][1]) for k in range(4)]
    d = [(z[k][0] - z[k + 4][0], z[k][1] - z[k + 4][1]) for k in range(4)]
    turned = [
        d[0],
        ((d[1][0] + d[1][1]) * HALF, (d[1][1] - d[1][0]) * HALF),
        (d[2][1], -d[2][0]),
        ((d[3][1] - d[3][0]) * HALF, -(d[3][0] + d[3][1]) * HALF),
    ]
    even, odd = fourths(s), fourths(turned)
    return [even[0], odd[0], even[1], odd[1], even[2], odd[2], even[3], odd[3]]


def near(v):
    return v + 1 - 2 * lax.rem(v, 2)


def far(v):
    return 3 - v


ROUTES = (("x", "near"), ("x", "far"), ("y", "near"), ("y", "far"))
MESH = pl.DeviceIdType.MESH


def hops(offset):
    a, b, d, e = offset
    return min(a, 4 - a) + min(b, 4 - b) + min(e, 8 - e)


FAR_FIRST = sorted(
    ((a, b, d, e) for a in range(4) for b in range(4) for e in range(8) for d in range(2) if (a, b, d, e) != (0, 0, 0, 0)),
    key=lambda o: (-hops(o), (7 * o[0] + 3 * o[1] + 5 * o[3]) % 11),
)


def transform_kernel(
    main_ref, rim_ref, total_ref, counts_hbm, twist_hbm, y_high_hbm, y_low_hbm,
    columns, begin_out,
    counts_ref, twist_y, y_high, y_low, table_sem,
    main0, rim0, main1, rim1, main2, rim2, main3, rim3, main4, rim4,
    tally, inbox, pack, got, waves,
    z_sem, note_send, note_recv, send, recv, py_send, py_recv, wave_send, wave_recv,
):
    x, y, c = (lax.axis_index(a) for a in COORDS)
    j = lax.axis_index("py")
    i = (x * 4 + y) * 2 + c
    me = i * 8 + j
    barrier = pltpu.get_barrier_semaphore()

    def device(x, y, c):
        return {"px_0": x, "px_1": y, "px_2": c}

    tables_in = [
        pltpu.make_async_copy(table, spot, table_sem.at[k])
        for k, (table, spot) in enumerate(
            ((counts_hbm, counts_ref), (twist_hbm, twist_y), (y_high_hbm, y_high), (y_low_hbm, y_low))
        )
    ]
    for copy in tables_in:
        copy.start()
    xs = [x] + [lax.rem(x + k, 4) for k in range(1, 4)]
    ys = [y] + [lax.rem(y + k, 4) for k in range(1, 4)]
    js = [j] + [lax.rem(j + k, 8) for k in range(1, 8)]
    kin = [
        (device(x, y, 1 - c), c == 1),
        (device(x, near(y), c), lax.rem(y, 2) == 1),
        (device(x, far(y), c), y >= 2),
        (device(near(x), y, c), lax.rem(x, 2) == 1),
        (device(far(x), y, c), x >= 2),
    ]
    above, below = {"py": js[1]}, {"py": js[7]}
    for peer in (*(peer for peer, _ in kin), above, below):
        pl.semaphore_signal(barrier, inc=1, device_id=peer, device_id_type=MESH)
    tables_in[0].wait()
    tally[0, 0:1, :] = counts_ref[0, :, 0:TILE].astype(jnp.float32)
    tally[0, 1:2, :] = counts_ref[0, :, TILE:].astype(jnp.float32)
    tally[0, 2:3, :] = jnp.sum(total_ref[...], axis=0, keepdims=True)
    tally[0, 3:8, :] = jnp.zeros((5, TILE), jnp.float32)
    pl.semaphore_wait(barrier, 7)

    def tell(n):
        if n < 3:
            pl.semaphore_signal(z_sem.at[n, 0], inc=1, device_id=above, device_id_type=MESH)
            pl.semaphore_signal(z_sem.at[n, 1], inc=1, device_id=below, device_id_type=MESH)
        copy = pltpu.make_async_remote_copy(
            src_ref=tally.at[n], dst_ref=inbox.at[n], send_sem=note_send.at[n], recv_sem=note_recv.at[n],
            device_id=kin[n][0], device_id_type=MESH,
        )
        copy.start()
        told.append(copy)

    def hear(n):
        if n < 3:
            pl.semaphore_wait(z_sem.at[n, 0], 1)
            pl.semaphore_wait(z_sem.at[n, 1], 1)
        told[n].wait_recv()
        tally[n + 1] = tally[n] + inbox[n]

    sent, told = [], []
    tell(0)

    def remote(src, dst, slot, where):
        copy = pltpu.make_async_remote_copy(
            src_ref=src, dst_ref=dst, send_sem=send.at[slot], recv_sem=recv.at[slot],
            device_id=where, device_id_type=MESH,
        )
        copy.start()
        return copy

    chunks = {}
    for k in (8, 9, *range(8)):
        if k < 8:
            refs = (main_ref.at[k], *(r.at[k] for r in (main0, main1, main2, main3, main4)))
        else:
            refs = (rim_ref.at[k - 8], *(r.at[k - 8] for r in (rim0, rim1, rim2, rim3, rim4)))
        chunks[k] = (*refs, k % 4 if k < 8 else 2 * (k - 8))

    def leg(first, kind):
        v = x if first == "x" else y
        if kind == "near":
            low = lax.rem((v + 1) // 2, 2)
            keep, give = (low, 3 - low), (1 - low, 2 + low)
            partner, other = near(v), far(v)
        else:
            low = 2 * (v // 2)
            keep, give = (low, low + 1), (2 - low, 3 - low)
            partner, other = far(v), near(v)
        if first == "x":
            return keep, give, device(partner, y, c), other, device(other, y, c)
        return keep, give, device(x, partner, c), other, device(x, other, c)

    def core_copy(k, src, b0):
        where = device(x, y, 1 - c)
        if k >= 8:
            parts = [(src.at[:, :, 1 - c], b0)]
        else:
            parts = [(src.at[pl.ds(1 - c + 4 * n, 4), c], b0.at[n]) for n in range(4)]
        for one, two in parts:
            pltpu.make_async_remote_copy(
                src_ref=one, dst_ref=two, send_sem=send.at[7 * k], recv_sem=recv.at[7 * k],
                device_id=where, device_id_type=MESH,
            ).start()

    for k, (src, b0, *_) in chunks.items():
        core_copy(k, src, b0)
    pending = {}

    hear(0)
    tell(1)

    def arrive(k):
        for copy in pending[k]:
            copy.wait_recv()
        sent.extend(pending[k])

    for k, (src, b0, b1, b2, b3, b4, route) in chunks.items():
        pltpu.make_async_copy(b0, b0, recv.at[7 * k]).wait()

        def add0(n, _, src=src, b0=b0, k=k):
            for m in range(4):
                own = src[c + 4 * n + m, 1 - c] if k < 8 else src[n, m, c]
                b0[n, m] = b0[n, m] + own
            return 0

        lax.fori_loop(0, 4, add0, 0)
        first, kind = ROUTES[route]
        _, give, where, _, _ = leg(first, kind)
        pending[k] = []
        for n in range(2):
            block = b0.at[give[n]] if first == "x" else b0.at[:, give[n]]
            pending[k].append(remote(block, b1.at[n], 7 * k + 1 + n, where))

    hear(1)
    tell(2)
    for k, (src, b0, b1, b2, b3, b4, route) in chunks.items():
        arrive(k)
        first, kind = ROUTES[route]
        keep, _, _, other, where = leg(first, kind)
        for n in range(2):
            for m in range(4):
                at = (keep[n], m) if first == "x" else (m, keep[n])
                b0[at] = b0[at] + b1[n, m]
        block = b0.at[other] if first == "x" else b0.at[:, other]
        pending[k] = [remote(block, b2, 7 * k + 3, where)]

    hear(2)
    tell(3)
    for k, (src, b0, b1, b2, b3, b4, route) in chunks.items():
        arrive(k)
        first, kind = ROUTES[route]
        for m in range(4):
            at = (x, m) if first == "x" else (m, y)
            b0[at] = b0[at] + b2[m]
        second = "y" if first == "x" else "x"
        _, give, where, _, _ = leg(second, kind)
        pending[k] = []
        for n in range(2):
            block = b0.at[x, give[n]] if first == "x" else b0.at[give[n], y]
            pending[k].append(remote(block, b3.at[n], 7 * k + 4 + n, where))

    hear(3)
    tell(4)
    for k, (src, b0, b1, b2, b3, b4, route) in chunks.items():
        arrive(k)
        first, kind = ROUTES[route]
        second = "y" if first == "x" else "x"
        keep, _, _, other, where = leg(second, kind)
        for n in range(2):
            at = (x, keep[n]) if first == "x" else (keep[n], y)
            b0[at] = b0[at] + b3[n]
        block = b0.at[x, other] if first == "x" else b0.at[other, y]
        pending[k] = [remote(block, b4, 7 * k + 6, where)]

    hear(4)
    everyone = tally[5]
    amount = jnp.broadcast_to(everyone[2:3, :], (8, TILE))
    spare = lax.broadcasted_iota(jnp.int32, (8, TILE), 0) == 4

    def plane_copy(k, source):
        return pltpu.make_async_remote_copy(
            src_ref=pack.at[k], dst_ref=got.at[source], send_sem=py_send.at[k], recv_sem=py_recv.at[source],
            device_id={"py": k}, device_id_type=MESH,
        )

    edge = []
    for k, (src, b0, b1, b2, b3, b4, route) in chunks.items():
        arrive(k)
        block = b0[x, y] + b4[...]
        if k >= 8:
            edge.append(block)
            if k == 9:
                edge = edge + [pltpu.roll(half, 64, 1) for half in edge] + [jnp.zeros((96, TILE), jnp.float32)]
                turned = jnp.transpose(jnp.concatenate(edge))
                for p in range(PLANES):
                    pack[p, RX:, :] = jnp.where(spare, amount, turned[8 * p : 8 * p + 8, :])
            continue
        pack[k, 0:RX, :] = block

        @pl.when(k != j)
        def _():
            plane_copy(k, j).start()

        @pl.when(k == j)
        def _():
            got[k] = pack[k]

    earlier = jnp.zeros((8, TILE), jnp.float32)
    for n, (_, lower) in enumerate(kin):
        earlier = earlier + jnp.where(lower, inbox[n], 0.0)
    spot = lax.broadcasted_iota(jnp.int32, (8, TILE), 1)
    running = everyone
    for shift in (1, 2, 4, 8, 16, 32, 64):
        running = running + jnp.where(spot >= shift, pltpu.roll(running, shift, 1), 0.0)
    begin = running - everyone + earlier
    whole = jnp.sum(everyone[0:1, :], axis=1, keepdims=True)
    begin_out[0:1, :] = begin[0:1, :]
    begin_out[1:2, :] = begin[1:2, :] + whole
    begin_out[2:8, :] = jnp.zeros((6, TILE), jnp.float32)

    for k in range(1, 8):
        peer = js[k]
        plane_copy(peer, j).wait_send()
        plane_copy(peer, peer).wait_recv()

    for copy in tables_in[1:]:
        copy.wait()
    lane = lax.broadcasted_iota(jnp.int32, (RX, TILE), 1)
    rims = jnp.concatenate([got[s, 32:40, :] for s in range(8)])
    rims = jnp.concatenate([rims, jnp.zeros((64, TILE), jnp.float32)])
    rims = jnp.transpose(rims)[:RX]
    mass_sum = got[0, 36:37, :]
    for s in range(1, 8):
        mass_sum = mass_sum + got[s, 36:37, :]
    inverse = float(PLANES * NX * NY) / jnp.sum(mass_sum, axis=1, keepdims=True)
    blocks = []
    for s in range(8):
        right = pltpu.roll(rims, (-8 * ((s + 7) % 8)) % TILE, 1)
        left = pltpu.roll(rims, (120 - 8 * ((s + 1) % 8)) % TILE, 1)
        value = got[s, 0:32, :] + jnp.where(lane < 4, right, 0.0) + jnp.where(lane >= 125, left, 0.0)
        blocks.append(value * inverse - 1.0)
    turned = []
    for k, (re, im) in enumerate(real_eighths(blocks)):
        tr, ti = twist_y[0, k : k + 1, :], twist_y[1, k : k + 1, :]
        turned.append(jnp.concatenate([re * tr - im * ti, re * ti + im * tr], axis=1))
    high, low = split_bf16(jnp.concatenate(turned))

    def times(a, b):
        return lax.dot_general(a, b, NT, preferred_element_type=jnp.float32)

    wave = times(y_high[...], low) + times(y_low[...], high) + times(y_high[...], high)
    for h in range(2):
        for k in range(TILE):
            waves[2 * k + h] = wave[2 * k : 2 * k + 2, TILE * h : TILE * h + TILE]

    columns[j * 32 + i] = waves[me]

    cs = [c, 1 - c]
    for a, b, d, e in FAR_FIRST:
        pltpu.make_async_remote_copy(
            src_ref=waves.at[((xs[a] * 4 + ys[b]) * 2 + cs[d]) * 8 + js[e]], dst_ref=columns.at[j * 32 + i],
            send_sem=wave_send, recv_sem=wave_recv,
            device_id={"px_0": xs[a], "px_1": ys[b], "px_2": cs[d], "py": js[e]}, device_id_type=MESH,
        ).start()
    for copy in (*sent, *told):
        copy.wait_send()
    for k, (src, b0, *_) in chunks.items():
        pltpu.make_async_copy(b0, b0, send.at[7 * k]).wait()
    others = columns.at[pl.ds(0, DEVICES - 1)]
    pltpu.make_async_copy(others, others, wave_recv).wait()
    pltpu.make_async_copy(others, others, wave_send).wait()


def transform(main, rim, total, counts, wave_tables):
    vmem = pl.BlockSpec(memory_space=pltpu.VMEM)
    f32 = jnp.float32

    def both(*lead):
        return [pltpu.VMEM((PLANES, *lead, RX, TILE), f32), pltpu.VMEM((2, *lead, 8, TILE), f32)]

    dma = pltpu.SemaphoreType.DMA
    return pl.pallas_call(
        transform_kernel,
        out_shape=(
            jax.ShapeDtypeStruct((DEVICES, 2, TILE), f32),
            jax.ShapeDtypeStruct((8, TILE), f32),
        ),
        in_specs=[vmem] * 3 + [pl.BlockSpec(memory_space=pltpu.HBM)] * 4,
        out_specs=(vmem, vmem),
        scratch_shapes=[
            pltpu.VMEM((1, 1, 2 * TILE), jnp.int32),
            pltpu.VMEM((2, 8, TILE), f32),
            pltpu.VMEM((2 * TILE, 2 * TILE), jnp.bfloat16),
            pltpu.VMEM((2 * TILE, 2 * TILE), jnp.bfloat16),
            dma((4,)),
            *both(4, 4), *both(2, 4), *both(4), *both(2), *both(),
            pltpu.VMEM((6, 8, TILE), f32),
            pltpu.VMEM((5, 8, TILE), f32),
            pltpu.VMEM((PLANES, RX + 8, TILE), f32),
            pltpu.VMEM((PLANES, RX + 8, TILE), f32),
            pltpu.VMEM((DEVICES, 2, TILE), f32),
            pltpu.SemaphoreType.REGULAR((3, 2)), dma((5,)), dma((5,)), dma((70,)), dma((70,)), dma((8,)), dma((8,)), dma, dma,
        ],
        compiler_params=pltpu.CompilerParams(
            collective_id=0, has_side_effects=True, vmem_limit_bytes=24 << 20
        ),
        name="transform",
    )(main, rim, total, *(pltpu.with_memory_space_constraint(a, pltpu.HBM) for a in (counts, *wave_tables)))


def finish_kernel(columns, begin_ref, x_both, x_low, twist_x, out_ref, start_ref):
    start_ref[0, :, 0:TILE] = begin_ref[0:1, :].astype(jnp.int32)
    start_ref[0, :, TILE:] = begin_ref[1:2, :].astype(jnp.int32)
    for g in range(4):
        pair = columns[64 * g : 64 * g + 64].reshape(TILE, TILE)
        high, low = split_bf16(jnp.transpose(pair))
        both = jnp.concatenate([high, low], axis=1)
        sums = jnp.dot(both, x_both[...], preferred_element_type=jnp.float32)
        sums = sums + jnp.dot(high, x_low[...], preferred_element_type=jnp.float32)
        parts = [[], []]
        for p in range(2):
            for w in range(4):
                re_sum = im_sum = None
                for q in range(4):
                    rows = slice(32 * w + 8 * q, 32 * w + 8 * q + 8)
                    re = sums[rows, 256 * p : 256 * p + 128]
                    im = sums[rows, 256 * p + 128 : 256 * p + 256]
                    tr, ti = twist_x[0, 8 * q : 8 * q + 8, :], twist_x[1, 8 * q : 8 * q + 8, :]
                    re_part, im_part = re * tr - im * ti, re * ti + im * tr
                    re_sum = re_part if q == 0 else re_sum + re_part
                    im_sum = im_part if q == 0 else im_sum + im_part
                parts[0].append(re_sum)
                parts[1].append(im_sum)
        re, im = (jnp.transpose(jnp.stack(part), (1, 0, 2)) for part in parts)
        for a, value in enumerate(eighths([(re[k], im[k]) for k in range(8)])):
            for n in range(2):
                for p in range(2):
                    out_ref[n, 2 * g + p, :, TILE * a : TILE * a + TILE] = value[n][4 * p : 4 * p + 4]


def finish(columns, begin, wave_tables):
    vmem = pl.BlockSpec(memory_space=pltpu.VMEM)
    return pl.pallas_call(
        finish_kernel,
        out_shape=(
            jax.ShapeDtypeStruct((2, PLANES, 4, NX), jnp.float32),
            jax.ShapeDtypeStruct((1, 1, 2 * TILE), jnp.int32),
        ),
        in_specs=[vmem] * 5,
        out_specs=(vmem, vmem),
        compiler_params=pltpu.CompilerParams(vmem_limit_bytes=24 << 20),
        name="finish",
    )(columns, begin, *wave_tables)


PX = ("px_0", "px_1", "px_2")
PX_PY = ("px_0", "px_1", "px_2", "py")


def local(cell_ids, offset_x, offset_y, mass, live, tile_owner, counts):
    main, rim, total = spread(tile_owner, cell_ids[0], offset_x[0], offset_y[0], mass[0], live[0])
    y_tables, x_tables = tables()
    columns, begin = transform(
        main.reshape(PLANES, BLOCKS // 2, 2, RX, TILE), rim.reshape(2, 4, 4, 2, 8, TILE), total, counts, y_tables
    )
    return finish(columns, begin, x_tables)


def solution(mesh):
    torus = Mesh(mesh.devices.reshape(4, 4, 2, mesh.shape["py"]), ("px_0", "px_1", "px_2", "py"))
    return jax.shard_map(
        local,
        mesh=torus,
        in_specs=(
            P(PX, "py", None),
            P(PX, "py", None),
            P(PX, "py", None),
            P(PX, "py", None),
            P(PX, "py", None),
            P(PX, "py"),
            P(PX, "py", None),
        ),
        out_specs=(P(None, None, PX_PY, None), P(PX, "py", None)),
        check_vma=False,
    )
```

```python
import functools
import math

import jax
import jax.numpy as jnp
import numpy as np
from jax import lax
from jax.experimental import pallas as pl
from jax.experimental.pallas import tpu as pltpu
from jax.sharding import Mesh
from jax.sharding import PartitionSpec as P

NX = 1024
NY = 1024
PLANES = 8
BETA = 18.4
OWNERS = 32
BLOCKS = OWNERS + 2
RX = 32
TILE = 128
NT = (((1,), (1,)), ((), ()))


def tap_values(step, fraction):
    z = (step.astype(jnp.float32) - fraction) * 0.25
    return jnp.exp(BETA * (jnp.sqrt(1.0 - z * z) - 1.0))


def spread_kernel(
    owner_hbm, cell_hbm, fx_hbm, fy_hbm, mass_hbm, live_hbm,
    main_ref, rim_ref, total_ref,
    owner_ref, cell_ref, fx_ref, fy_ref, mass_ref, live_ref, in_sem,
    rim_acc, lx_s, ly_s, fx_s, fy_s, w_s,
):
    tiles = cell_ref.shape[0]
    sources = (owner_hbm, cell_hbm, fx_hbm, fy_hbm, mass_hbm, live_hbm)
    homes = (owner_ref, cell_ref, fx_ref, fy_ref, mass_ref, live_ref)
    arrivals = [
        pltpu.make_async_copy(source, home, in_sem.at[k]) for k, (source, home) in enumerate(zip(sources, homes))
    ]
    for copy in arrivals:
        copy.start()
    zero = jnp.zeros((8, TILE), jnp.float32)

    def clear(i, _):
        for p in range(PLANES):
            for k in range(RX // 8):
                main_ref[i * PLANES + p, 8 * k : 8 * k + 8, :] = zero
        for k in range(RX // 8):
            rim_acc[i, 8 * k : 8 * k + 8, :] = zero
        return 0

    lax.fori_loop(0, BLOCKS, clear, 0)

    for copy in arrivals:
        copy.wait()

    def prepare(i, _):
        rows = pl.ds(pl.multiple_of(i * 16, 16), 16)
        cell = cell_ref[rows, :]
        ly_s[rows, :] = cell & 127
        lx_s[rows, :] = (cell >> 7) & 31
        fx_s[rows, :] = fx_ref[rows, :].astype(jnp.float32)
        fy_s[rows, :] = fy_ref[rows, :].astype(jnp.float32)
        w_s[rows, :] = jnp.where(live_ref[rows, :] == 1, mass_ref[rows, :].astype(jnp.float32), 0.0)
        return 0

    lax.fori_loop(0, tiles // 16, prepare, 0, unroll=8)

    sub = lax.broadcasted_iota(jnp.int32, (8, TILE), 0)

    def row(ref, t):
        return jnp.broadcast_to(ref[pl.ds(t, 1), :], (8, TILE))

    def one_tile(t):
        lx, ly = row(lx_s, t), row(ly_s, t)
        jx = (sub - lx + 3) & 7
        jy = (sub - ly + 3) & 7
        tx = tap_values(jx - 3, row(fx_s, t))
        ty = tap_values(jy - 3, row(fy_s, t)) * row(w_s, t)
        gx = (lx + jx + 5) >> 3
        gy = (ly + jy - 3) >> 3
        gy = jnp.where(gy < 0, 16, gy)
        wx = jnp.concatenate([jnp.where(gx == g, tx, 0.0) for g in range(6)]).astype(jnp.bfloat16)
        wy = jnp.concatenate([*(jnp.where(gy == g, ty, 0.0) for g in range(17)), zero]).astype(jnp.bfloat16)
        return lax.dot_general(wx, wy, NT, preferred_element_type=jnp.float32)

    blank = jnp.zeros((48, TILE - 8), jnp.float32)

    unroll = 320

    def add_tiles(i, _):
        results = [one_tile(i * unroll + k) for k in range(unroll)]
        for k in range(unroll):
            owner = owner_ref[0, i * unroll + k]
            plane = cell_ref[pl.ds(i * unroll + k, 1), :][0, 0] >> 12
            main, rim = results[k][:, :TILE], results[k][:, TILE : TILE + 8]
            rim = pltpu.roll(jnp.concatenate([rim, blank], axis=1), 8 * plane, 1)
            for blocks, spot, part in ((main_ref, plane * BLOCKS + owner, main), (rim_acc, owner, rim)):
                blocks[spot, 24:32, :] = blocks[spot, 24:32, :] + part[:8]
                blocks[spot + 1] = blocks[spot + 1] + part[8:40]
                blocks[spot + 2, 0:8, :] = blocks[spot + 2, 0:8, :] + part[40:]
        return 0

    lax.fori_loop(0, tiles // unroll, add_tiles, 0)

    for blocks, start in ((rim_acc, 0), *((main_ref, p * BLOCKS) for p in range(PLANES))):
        first, last = start, start + OWNERS
        blocks[last, 24:32, :] = blocks[last, 24:32, :] + blocks[first, 24:32, :]
        blocks[first + 1, 0:8, :] = blocks[first + 1, 0:8, :] + blocks[last + 1, 0:8, :]

    def write_out(i, total):
        parts = [main_ref[p * BLOCKS + i + 1, 8 * k : 8 * k + 8, :] for p in range(PLANES) for k in range(RX // 8)]
        while len(parts) > 1:
            parts = [one + two for one, two in zip(parts[::2], parts[1::2])]
        total = total + parts[0]
        for q in range(2):
            near_rows, far_rows = rim_acc[i + 1, 8 * q : 8 * q + 8, :], rim_acc[i + 1, 8 * q + 16 : 8 * q + 24, :]
            out = near_rows + pltpu.roll(far_rows, 64, 1)
            rim_ref[q, i // 2, i % 2] = out
            total = total + out
        return total

    total_ref[...] = lax.fori_loop(0, OWNERS, write_out, zero, unroll=8)


def spread(owners, cells, fx, fy, mass, live):
    tiles = cells.shape[0]
    vmem = pl.BlockSpec(memory_space=pltpu.VMEM)
    return pl.pallas_call(
        spread_kernel,
        out_shape=(
            jax.ShapeDtypeStruct((PLANES * BLOCKS, RX, TILE), jnp.float32),
            jax.ShapeDtypeStruct((2, 16, 2, 8, TILE), jnp.float32),
            jax.ShapeDtypeStruct((8, TILE), jnp.float32),
        ),
        in_specs=[pl.BlockSpec(memory_space=pltpu.HBM)] * 6,
        out_specs=(vmem, vmem, vmem),
        scratch_shapes=[
            pltpu.SMEM((1, tiles), jnp.int32),
            pltpu.VMEM((tiles, TILE), jnp.int32),
            pltpu.VMEM((tiles, TILE), jnp.bfloat16),
            pltpu.VMEM((tiles, TILE), jnp.bfloat16),
            pltpu.VMEM((tiles, TILE), jnp.bfloat16),
            pltpu.VMEM((tiles, TILE), jnp.int32),
            pltpu.SemaphoreType.DMA((6,)),
            pltpu.VMEM((BLOCKS, RX, TILE), jnp.float32),
            pltpu.VMEM((tiles, TILE), jnp.int32),
            pltpu.VMEM((tiles, TILE), jnp.int32),
            pltpu.VMEM((tiles, TILE), jnp.float32),
            pltpu.VMEM((tiles, TILE), jnp.float32),
            pltpu.VMEM((tiles, TILE), jnp.float32),
        ],
        compiler_params=pltpu.CompilerParams(vmem_limit_bytes=24 << 20),
        name="spread",
    )(*(pltpu.with_memory_space_constraint(a, pltpu.HBM) for a in (owners, cells, fx, fy, mass, live)))


COORDS = ("px_0", "px_1", "px_2")
DEVICES = 256


def split_bf16(value):
    high = value.astype(jnp.bfloat16)
    return high, (value - high.astype(jnp.float32)).astype(jnp.bfloat16)


def np_split(value):
    high = np.asarray(value, np.float32).astype(jnp.bfloat16)
    low = (np.asarray(value, np.float64) - high.astype(np.float64)).astype(jnp.bfloat16)
    return high, low


def tables():
    k = np.arange(TILE)
    turn_y = 2 * np.pi / NY * (np.arange(8)[:, None] * k[None, :])
    twist_y = np.stack([np.cos(turn_y), -np.sin(turn_y)]).astype(np.float32)
    theta = 2 * np.pi / TILE * (k[:, None] * k[None, :] % TILE)
    wave_y = np.zeros((TILE, 2, 2, TILE))
    wave_y[:, 0, 0], wave_y[:, 0, 1] = np.cos(theta), np.sin(theta)
    wave_y[:, 1, 0], wave_y[:, 1, 1] = -np.sin(theta), np.cos(theta)
    y_high, y_low = np_split(wave_y.reshape(2 * TILE, 2 * TILE))
    phase = 2 * np.pi / OWNERS * (np.arange(OWNERS)[:, None] * k[None, :] % OWNERS)
    block = np.zeros((OWNERS, 2, 2, TILE))
    block[:, 0, 0], block[:, 1, 0] = np.cos(phase), np.sin(phase)
    block[:, 0, 1], block[:, 1, 1] = -np.sin(phase), np.cos(phase)
    wave_x = np.kron(np.eye(2), block.reshape(2 * OWNERS, 2 * TILE))
    x_high, x_low = np_split(wave_x)
    turn_x = 2 * np.pi / NX * (np.arange(RX)[:, None] * k[None, :])
    scale = 1.0 / math.sqrt(NX * NY)
    twist_x = (scale * np.stack([np.cos(turn_x), -np.sin(turn_x)])).astype(np.float32)
    return (twist_y, y_high, y_low), (np.concatenate([x_high, x_high]), x_low, twist_x)


HALF = math.sqrt(0.5)


def real_eighths(d):
    s = [d[k] + d[k + 4] for k in range(4)]
    e = [d[k] - d[k + 4] for k in range(4)]
    near_sum, far_sum = s[0] + s[2], s[1] + s[3]
    a0, a4 = near_sum + far_sum, near_sum - far_sum
    re2, im2 = s[0] - s[2], s[3] - s[1]
    tilt, lean = (e[1] - e[3]) * HALF, (e[1] + e[3]) * HALF
    re1, im1 = e[0] + tilt, -e[2] - lean
    re3, im3 = e[0] - tilt, e[2] - lean
    zero = jnp.zeros_like(a0)
    return [(a0, zero), (re1, im1), (re2, im2), (re3, im3), (a4, zero), (re3, -im3), (re2, -im2), (re1, -im1)]


def fourths(t):
    def add(p, q):
        return p[0] + q[0], p[1] + q[1]

    def less(p, q):
        return p[0] - q[0], p[1] - q[1]

    e0, e1 = add(t[0], t[2]), less(t[0], t[2])
    f0, g = add(t[1], t[3]), less(t[1], t[3])
    f1 = (g[1], -g[0])
    return [add(e0, f0), add(e1, f1), less(e0, f0), less(e1, f1)]


def eighths(z):
    s = [(z[k][0] + z[k + 4][0], z[k][1] + z[k + 4][1]) for k in range(4)]
    d = [(z[k][0] - z[k + 4][0], z[k][1] - z[k + 4][1]) for k in range(4)]
    turned = [
        d[0],
        ((d[1][0] + d[1][1]) * HALF, (d[1][1] - d[1][0]) * HALF),
        (d[2][1], -d[2][0]),
        ((d[3][1] - d[3][0]) * HALF, -(d[3][0] + d[3][1]) * HALF),
    ]
    even, odd = fourths(s), fourths(turned)
    return [even[0], odd[0], even[1], odd[1], even[2], odd[2], even[3], odd[3]]


def near(v):
    return v + 1 - 2 * lax.rem(v, 2)


def far(v):
    return 3 - v


ROUTES = (("x", "near"), ("x", "far"), ("y", "near"), ("y", "far"))
MESH = pl.DeviceIdType.MESH


def hops(offset):
    a, b, d, e = offset
    return min(a, 4 - a) + min(b, 4 - b) + min(e, 8 - e)


FAR_FIRST = sorted(
    ((a, b, d, e) for a in range(4) for b in range(4) for e in range(8) for d in range(2) if (a, b, d, e) != (0, 0, 0, 0)),
    key=lambda o: (-hops(o), (7 * o[0] + 3 * o[1] + 5 * o[3]) % 11),
)


def transform_kernel(
    main_ref, rim_ref, total_ref, counts_hbm, twist_hbm, y_high_hbm, y_low_hbm,
    columns, begin_out,
    counts_ref, twist_y, y_high, y_low, table_sem,
    main0, rim0, main1, rim1, main2, rim2, main3, rim3, main4, rim4,
    tally, inbox, pack, got, waves,
    z_sem, note_send, note_recv, send, recv, py_send, py_recv, wave_send, wave_recv,
):
    x, y, c = (lax.axis_index(a) for a in COORDS)
    j = lax.axis_index("py")
    i = (x * 4 + y) * 2 + c
    me = i * 8 + j
    barrier = pltpu.get_barrier_semaphore()

    def device(x, y, c):
        return {"px_0": x, "px_1": y, "px_2": c}

    tables_in = [
        pltpu.make_async_copy(table, spot, table_sem.at[k])
        for k, (table, spot) in enumerate(
            ((counts_hbm, counts_ref), (twist_hbm, twist_y), (y_high_hbm, y_high), (y_low_hbm, y_low))
        )
    ]
    for copy in tables_in:
        copy.start()
    xs = [x] + [lax.rem(x + k, 4) for k in range(1, 4)]
    ys = [y] + [lax.rem(y + k, 4) for k in range(1, 4)]
    js = [j] + [lax.rem(j + k, 8) for k in range(1, 8)]
    kin = [
        (device(x, y, 1 - c), c == 1),
        (device(x, near(y), c), lax.rem(y, 2) == 1),
        (device(x, far(y), c), y >= 2),
        (device(near(x), y, c), lax.rem(x, 2) == 1),
        (device(far(x), y, c), x >= 2),
    ]
    above, below = {"py": js[1]}, {"py": js[7]}
    for peer in (*(peer for peer, _ in kin), above, below):
        pl.semaphore_signal(barrier, inc=1, device_id=peer, device_id_type=MESH)
    tables_in[0].wait()
    tally[0, 0:1, :] = counts_ref[0, :, 0:TILE].astype(jnp.float32)
    tally[0, 1:2, :] = counts_ref[0, :, TILE:].astype(jnp.float32)
    tally[0, 2:3, :] = jnp.sum(total_ref[...], axis=0, keepdims=True)
    tally[0, 3:8, :] = jnp.zeros((5, TILE), jnp.float32)
    pl.semaphore_wait(barrier, 7)

    def tell(n):
        if n < 3:
            pl.semaphore_signal(z_sem.at[n, 0], inc=1, device_id=above, device_id_type=MESH)
            pl.semaphore_signal(z_sem.at[n, 1], inc=1, device_id=below, device_id_type=MESH)
        copy = pltpu.make_async_remote_copy(
            src_ref=tally.at[n], dst_ref=inbox.at[n], send_sem=note_send.at[n], recv_sem=note_recv.at[n],
            device_id=kin[n][0], device_id_type=MESH,
        )
        copy.start()
        told.append(copy)

    def hear(n):
        if n < 3:
            pl.semaphore_wait(z_sem.at[n, 0], 1)
            pl.semaphore_wait(z_sem.at[n, 1], 1)
        told[n].wait_recv()
        tally[n + 1] = tally[n] + inbox[n]

    sent, told = [], []
    tell(0)

    def remote(src, dst, slot, where):
        copy = pltpu.make_async_remote_copy(
            src_ref=src, dst_ref=dst, send_sem=send.at[slot], recv_sem=recv.at[slot],
            device_id=where, device_id_type=MESH,
        )
        copy.start()
        return copy

    chunks = {}
    for k in (8, 9, *range(8)):
        if k < 8:
            refs = (main_ref.at[k], *(r.at[k] for r in (main0, main1, main2, main3, main4)))
        else:
            refs = (rim_ref.at[k - 8], *(r.at[k - 8] for r in (rim0, rim1, rim2, rim3, rim4)))
        chunks[k] = (*refs, k % 4 if k < 8 else 2 * (k - 8))

    def leg(first, kind):
        v = x if first == "x" else y
        if kind == "near":
            low = lax.rem((v + 1) // 2, 2)
            keep, give = (low, 3 - low), (1 - low, 2 + low)
            partner, other = near(v), far(v)
        else:
            low = 2 * (v // 2)
            keep, give = (low, low + 1), (2 - low, 3 - low)
            partner, other = far(v), near(v)
        if first == "x":
            return keep, give, device(partner, y, c), other, device(other, y, c)
        return keep, give, device(x, partner, c), other, device(x, other, c)

    def core_copy(k, src, b0):
        where = device(x, y, 1 - c)
        if k >= 8:
            parts = [(src.at[:, :, 1 - c], b0)]
        else:
            parts = [(src.at[pl.ds(1 - c + 4 * n, 4), c], b0.at[n]) for n in range(4)]
        for one, two in parts:
            pltpu.make_async_remote_copy(
                src_ref=one, dst_ref=two, send_sem=send.at[7 * k], recv_sem=recv.at[7 * k],
                device_id=where, device_id_type=MESH,
            ).start()

    for k, (src, b0, *_) in chunks.items():
        core_copy(k, src, b0)
    pending = {}

    hear(0)
    tell(1)

    def arrive(k):
        for copy in pending[k]:
            copy.wait_recv()
        sent.extend(pending[k])

    for k, (src, b0, b1, b2, b3, b4, route) in chunks.items():
        pltpu.make_async_copy(b0, b0, recv.at[7 * k]).wait()

        def add0(n, _, src=src, b0=b0, k=k):
            for m in range(4):
                own = src[c + 4 * n + m, 1 - c] if k < 8 else src[n, m, c]
                b0[n, m] = b0[n, m] + own
            return 0

        lax.fori_loop(0, 4, add0, 0)
        first, kind = ROUTES[route]
        _, give, where, _, _ = leg(first, kind)
        pending[k] = []
        for n in range(2):
            block = b0.at[give[n]] if first == "x" else b0.at[:, give[n]]
            pending[k].append(remote(block, b1.at[n], 7 * k + 1 + n, where))

    hear(1)
    tell(2)
    for k, (src, b0, b1, b2, b3, b4, route) in chunks.items():
        arrive(k)
        first, kind = ROUTES[route]
        keep, _, _, other, where = leg(first, kind)
        for n in range(2):
            for m in range(4):
                at = (keep[n], m) if first == "x" else (m, keep[n])
                b0[at] = b0[at] + b1[n, m]
        block = b0.at[other] if first == "x" else b0.at[:, other]
        pending[k] = [remote(block, b2, 7 * k + 3, where)]

    hear(2)
    tell(3)
    for k, (src, b0, b1, b2, b3, b4, route) in chunks.items():
        arrive(k)
        first, kind = ROUTES[route]
        for m in range(4):
            at = (x, m) if first == "x" else (m, y)
            b0[at] = b0[at] + b2[m]
        second = "y" if first == "x" else "x"
        _, give, where, _, _ = leg(second, kind)
        pending[k] = []
        for n in range(2):
            block = b0.at[x, give[n]] if first == "x" else b0.at[give[n], y]
            pending[k].append(remote(block, b3.at[n], 7 * k + 4 + n, where))

    hear(3)
    tell(4)
    for k, (src, b0, b1, b2, b3, b4, route) in chunks.items():
        arrive(k)
        first, kind = ROUTES[route]
        second = "y" if first == "x" else "x"
        keep, _, _, other, where = leg(second, kind)
        for n in range(2):
            at = (x, keep[n]) if first == "x" else (keep[n], y)
            b0[at] = b0[at] + b3[n]
        block = b0.at[x, other] if first == "x" else b0.at[other, y]
        pending[k] = [remote(block, b4, 7 * k + 6, where)]

    hear(4)
    everyone = tally[5]
    amount = jnp.broadcast_to(everyone[2:3, :], (8, TILE))
    spare = lax.broadcasted_iota(jnp.int32, (8, TILE), 0) == 4

    def plane_copy(k, source):
        return pltpu.make_async_remote_copy(
            src_ref=pack.at[k], dst_ref=got.at[source], send_sem=py_send.at[k], recv_sem=py_recv.at[source],
            device_id={"py": k}, device_id_type=MESH,
        )

    edge = []
    for k in (8, 9):
        arrive(k)
        edge.append(rim0[k - 8, x, y] + rim4[k - 8])
    edge = edge + [pltpu.roll(half, 64, 1) for half in edge] + [jnp.zeros((96, TILE), jnp.float32)]
    turned = jnp.transpose(jnp.concatenate(edge))
    for p in range(PLANES):
        pack[p, RX:, :] = jnp.where(spare, amount, turned[8 * p : 8 * p + 8, :])
    for n in (4, 3, 5, 2, 6, 1, 7, 0):
        k = js[n]
        pltpu.make_async_copy(main4.at[k], main4.at[k], recv.at[7 * k + 6]).wait()
        pack[k, 0:RX, :] = main0[k, x, y] + main4[k]
        if n:
            plane_copy(k, j).start()
    got[j] = pack[j]
    for k in range(PLANES):
        sent.extend(pending[k])

    earlier = jnp.zeros((8, TILE), jnp.float32)
    for n, (_, lower) in enumerate(kin):
        earlier = earlier + jnp.where(lower, inbox[n], 0.0)
    spot = lax.broadcasted_iota(jnp.int32, (8, TILE), 1)
    running = everyone
    for shift in (1, 2, 4, 8, 16, 32, 64):
        running = running + jnp.where(spot >= shift, pltpu.roll(running, shift, 1), 0.0)
    begin = running - everyone + earlier
    whole = jnp.sum(everyone[0:1, :], axis=1, keepdims=True)
    begin_out[0:1, :] = begin[0:1, :]
    begin_out[1:2, :] = begin[1:2, :] + whole
    begin_out[2:8, :] = jnp.zeros((6, TILE), jnp.float32)

    for k in range(1, 8):
        peer = js[k]
        plane_copy(peer, j).wait_send()
        plane_copy(peer, peer).wait_recv()

    for copy in tables_in[1:]:
        copy.wait()
    lane = lax.broadcasted_iota(jnp.int32, (RX, TILE), 1)
    rims = jnp.concatenate([got[s, 32:40, :] for s in range(8)])
    rims = jnp.concatenate([rims, jnp.zeros((64, TILE), jnp.float32)])
    rims = jnp.transpose(rims)[:RX]
    mass_sum = got[0, 36:37, :]
    for s in range(1, 8):
        mass_sum = mass_sum + got[s, 36:37, :]
    inverse = float(PLANES * NX * NY) / jnp.sum(mass_sum, axis=1, keepdims=True)
    blocks = []
    for s in range(8):
        right = pltpu.roll(rims, (-8 * ((s + 7) % 8)) % TILE, 1)
        left = pltpu.roll(rims, (120 - 8 * ((s + 1) % 8)) % TILE, 1)
        value = got[s, 0:32, :] + jnp.where(lane < 4, right, 0.0) + jnp.where(lane >= 125, left, 0.0)
        blocks.append(value * inverse - 1.0)
    turned = []
    for k, (re, im) in enumerate(real_eighths(blocks)):
        tr, ti = twist_y[0, k : k + 1, :], twist_y[1, k : k + 1, :]
        turned.append(jnp.concatenate([re * tr - im * ti, re * ti + im * tr], axis=1))
    high, low = split_bf16(jnp.concatenate(turned))

    def times(a, b):
        return lax.dot_general(a, b, NT, preferred_element_type=jnp.float32)

    wave = times(y_high[...], low) + times(y_low[...], high) + times(y_high[...], high)
    for h in range(2):
        for k in range(TILE):
            waves[2 * k + h] = wave[2 * k : 2 * k + 2, TILE * h : TILE * h + TILE]

    columns[j * 32 + i] = waves[me]

    cs = [c, 1 - c]
    for a, b, d, e in FAR_FIRST:
        pltpu.make_async_remote_copy(
            src_ref=waves.at[((xs[a] * 4 + ys[b]) * 2 + cs[d]) * 8 + js[e]], dst_ref=columns.at[j * 32 + i],
            send_sem=wave_send, recv_sem=wave_recv,
            device_id={"px_0": xs[a], "px_1": ys[b], "px_2": cs[d], "py": js[e]}, device_id_type=MESH,
        ).start()
    for copy in (*sent, *told):
        copy.wait_send()
    for k, (src, b0, *_) in chunks.items():
        pltpu.make_async_copy(b0, b0, send.at[7 * k]).wait()
    others = columns.at[pl.ds(0, DEVICES - 1)]
    pltpu.make_async_copy(others, others, wave_recv).wait()
    pltpu.make_async_copy(others, others, wave_send).wait()


def transform(main, rim, total, counts, wave_tables):
    vmem = pl.BlockSpec(memory_space=pltpu.VMEM)
    f32 = jnp.float32

    def both(*lead):
        return [pltpu.VMEM((PLANES, *lead, RX, TILE), f32), pltpu.VMEM((2, *lead, 8, TILE), f32)]

    dma = pltpu.SemaphoreType.DMA
    return pl.pallas_call(
        transform_kernel,
        out_shape=(
            jax.ShapeDtypeStruct((DEVICES, 2, TILE), f32),
            jax.ShapeDtypeStruct((8, TILE), f32),
        ),
        in_specs=[vmem] * 3 + [pl.BlockSpec(memory_space=pltpu.HBM)] * 4,
        out_specs=(vmem, vmem),
        scratch_shapes=[
            pltpu.VMEM((1, 1, 2 * TILE), jnp.int32),
            pltpu.VMEM((2, 8, TILE), f32),
            pltpu.VMEM((2 * TILE, 2 * TILE), jnp.bfloat16),
            pltpu.VMEM((2 * TILE, 2 * TILE), jnp.bfloat16),
            dma((4,)),
            *both(4, 4), *both(2, 4), *both(4), *both(2), *both(),
            pltpu.VMEM((6, 8, TILE), f32),
            pltpu.VMEM((5, 8, TILE), f32),
            pltpu.VMEM((PLANES, RX + 8, TILE), f32),
            pltpu.VMEM((PLANES, RX + 8, TILE), f32),
            pltpu.VMEM((DEVICES, 2, TILE), f32),
            pltpu.SemaphoreType.REGULAR((3, 2)), dma((5,)), dma((5,)), dma((70,)), dma((70,)), dma((8,)), dma((8,)), dma, dma,
        ],
        compiler_params=pltpu.CompilerParams(
            collective_id=0, has_side_effects=True, vmem_limit_bytes=24 << 20
        ),
        name="transform",
    )(main, rim, total, *(pltpu.with_memory_space_constraint(a, pltpu.HBM) for a in (counts, *wave_tables)))


def finish_kernel(columns, begin_ref, x_both, x_low, twist_x, out_ref, start_ref):
    start_ref[0, :, 0:TILE] = begin_ref[0:1, :].astype(jnp.int32)
    start_ref[0, :, TILE:] = begin_ref[1:2, :].astype(jnp.int32)
    for g in range(4):
        pair = columns[64 * g : 64 * g + 64].reshape(TILE, TILE)
        high, low = split_bf16(jnp.transpose(pair))
        both = jnp.concatenate([high, low], axis=1)
        sums = jnp.dot(both, x_both[...], preferred_element_type=jnp.float32)
        sums = sums + jnp.dot(high, x_low[...], preferred_element_type=jnp.float32)
        parts = [[], []]
        for p in range(2):
            for w in range(4):
                re_sum = im_sum = None
                for q in range(4):
                    rows = slice(32 * w + 8 * q, 32 * w + 8 * q + 8)
                    re = sums[rows, 256 * p : 256 * p + 128]
                    im = sums[rows, 256 * p + 128 : 256 * p + 256]
                    tr, ti = twist_x[0, 8 * q : 8 * q + 8, :], twist_x[1, 8 * q : 8 * q + 8, :]
                    re_part, im_part = re * tr - im * ti, re * ti + im * tr
                    re_sum = re_part if q == 0 else re_sum + re_part
                    im_sum = im_part if q == 0 else im_sum + im_part
                parts[0].append(re_sum)
                parts[1].append(im_sum)
        re, im = (jnp.transpose(jnp.stack(part), (1, 0, 2)) for part in parts)
        for a, value in enumerate(eighths([(re[k], im[k]) for k in range(8)])):
            for n in range(2):
                for p in range(2):
                    out_ref[n, 2 * g + p, :, TILE * a : TILE * a + TILE] = value[n][4 * p : 4 * p + 4]


def finish(columns, begin, wave_tables):
    vmem = pl.BlockSpec(memory_space=pltpu.VMEM)
    return pl.pallas_call(
        finish_kernel,
        out_shape=(
            jax.ShapeDtypeStruct((2, PLANES, 4, NX), jnp.float32),
            jax.ShapeDtypeStruct((1, 1, 2 * TILE), jnp.int32),
        ),
        in_specs=[vmem] * 5,
        out_specs=(vmem, vmem),
        compiler_params=pltpu.CompilerParams(vmem_limit_bytes=24 << 20),
        name="finish",
    )(columns, begin, *wave_tables)


PX = ("px_0", "px_1", "px_2")
PX_PY = ("px_0", "px_1", "px_2", "py")


def local(cell_ids, offset_x, offset_y, mass, live, tile_owner, counts):
    main, rim, total = spread(tile_owner, cell_ids[0], offset_x[0], offset_y[0], mass[0], live[0])
    y_tables, x_tables = tables()
    columns, begin = transform(
        main.reshape(PLANES, BLOCKS // 2, 2, RX, TILE), rim.reshape(2, 4, 4, 2, 8, TILE), total, counts, y_tables
    )
    return finish(columns, begin, x_tables)


def solution(mesh):
    torus = Mesh(mesh.devices.reshape(4, 4, 2, mesh.shape["py"]), ("px_0", "px_1", "px_2", "py"))
    return jax.shard_map(
        local,
        mesh=torus,
        in_specs=(
            P(PX, "py", None),
            P(PX, "py", None),
            P(PX, "py", None),
            P(PX, "py", None),
            P(PX, "py", None),
            P(PX, "py"),
            P(PX, "py", None),
        ),
        out_specs=(P(None, None, PX_PY, None), P(PX, "py", None)),
        check_vma=False,
    )
```
